32 devices in a mesh: mem: 16 (over z, y, core), band: 2 (over x).
Axes of the slice: x: 2, y: 2, z: 4, core: 2. Of those that a mesh axis runs over, the one named last changes fastest.
Arguments:
- ensemble: bfloat16 [16, 12, 32, 128], P('mem', None, 'band'), may hold values from -6 to 6
- alpha: float32 [16, 12, 32, 128], P('mem', None, 'band'), may hold values from -6 to 6
- lat_lower: int32 [96], P('band'), may hold values from -1 to 15, as said below
- lat_weight: float32 [96], P('band'), may hold values from 0 to 1
- background: float32 [12, 32, 1152], P(None, ('band', 'mem')), may hold values from -6 to 6
- obs_cell: int32 [32, 256], P(('band', 'mem')), may hold values from 0 to 1151
- obs_value: float32 [12, 32, 256], P(None, ('band', 'mem')), may hold values from -6 to 6
- obs_precision: float32 [32, 256], P(('band', 'mem')), may hold values from 1 to 10
Outputs:
- advected: float32 [12, 32, 1152], P(None, ('band', 'mem'))
- gradient: float32 [16, 12, 32, 128], P('mem', None, 'band')
The draws below stay inside these ranges and needn't reach their ends.
Inputs may be any that keep to these rules, and one draw needn't show every extreme that they name: `lat_lower`: fine rows of the first band use lower rows from 0, those of the last band up to 14 of their band, so that their upper row reaches 15; other bands reach -1 and 15. `obs_cell`: the cell is r * 24 + c for fine row r and column c within the tile.
All inputs are finite; a program needn't handle non-finite values.
Results may differ from the reference program's by a relative error of at most 0.0004.
Values sent between devices are 32-bit elements; how exact they have to be, the bound alone decides.
A program may use at most 64 MiB of HBM per device.

```python
import math
import jax
import jax.numpy as jnp
from jax import lax

LEV = 12
CLAT_B = 16
NOBS = 256
MEMBERS = 16
CLAT = 32
CLON = 128
FLAT_B = 48
FLON_T = 24
FLAT = 96
FLON = 384
TILES = 32
TILE_CELLS = 1152
N_MEM = 16
N_BAND = 2


def draw_lat_lower(key, part):
    fine_index = jnp.arange(FLAT, dtype=jnp.int32)
    inner = fine_index % FLAT_B
    band_index = fine_index // FLAT_B
    jitter = jax.random.randint(key, (FLAT,), 0, 2, dtype=jnp.int32)
    jitter = jnp.where(inner == 0, 0, jnp.where(inner == FLAT_B - 1, 1, jitter))
    lower_row = inner * CLAT_B // FLAT_B - 1 + jitter
    lower_row = jnp.where(band_index == 0, jnp.maximum(lower_row, 0), lower_row)
    lower_row = jnp.where(band_index == FLAT // FLAT_B - 1, jnp.minimum(lower_row, CLAT_B - 2), lower_row)
    return lower_row.astype(jnp.int32)


def touch_ends(values, stream_key, smallest, high):
    longest = values.shape.index(max(values.shape))
    spots = []
    for shift in (0, 1):
        where = [jax.random.randint(jax.random.fold_in(stream_key, axis), (), 0, length) for axis, length in enumerate(values.shape)]
        where[longest] = (where[longest] + shift) % values.shape[longest]
        spots.append(tuple(where))
    return values.at[spots[0]].set(smallest).at[spots[1]].set(high)


def level_of(key, extent, shards, least, largest):
    def one(axis_at, parts):
        steps = jax.random.uniform(jax.random.fold_in(jax.random.fold_in(key, 6), axis_at), (parts,), jnp.float32, least / len(shards), largest / len(shards))
        return jnp.repeat(jnp.exp(steps), extent[axis_at] // parts).reshape((-1,) + (1,) * (len(extent) - axis_at - 1))

    level = one(*shards[0])
    for cut in shards[1:]:
        level = level * one(*cut)
    return level


def centred(stream_key, shape, scale, most, cuts=(), kind=jnp.bfloat16):
    result = scale * jax.random.normal(stream_key, shape, jnp.float32)
    if cuts:
        result = result * level_of(stream_key, shape, cuts, -0.22, 0.18)
    return jnp.clip(result, -most, most).astype(kind)


def setup_inputs(seed: int = 0) -> dict:
    key_of = jax.random.split(jax.random.key(seed), 9)
    ensemble = centred(key_of[0], (MEMBERS, LEV, CLAT, CLON), 1.0, 6.0, ((0, 16), (2, 2)))
    alpha = centred(key_of[1], (MEMBERS, LEV, CLAT, CLON), 1.0, 6.0, ((0, 16), (2, 2)), jnp.float32)
    lat_lower = draw_lat_lower(jax.random.fold_in(key_of[8], 71), 0)
    lat_weight = jnp.clip(1.0 * jax.random.uniform(key_of[3], (FLAT,), jnp.float32) ** level_of(key_of[3], (FLAT,), ((0, 2),), -0.2, 0.2), 0.0, 1.0)
    background = centred(key_of[4], (LEV, TILES, TILE_CELLS), 1.0, 6.0, ((1, 32),), jnp.float32)
    obs_cell = touch_ends(jax.random.randint(key_of[5], (TILES, NOBS), 0, TILE_CELLS), jax.random.fold_in(key_of[5], 1), 0, TILE_CELLS - 1).astype(jnp.int32)
    obs_value = centred(key_of[6], (LEV, TILES, NOBS), 1.0, 6.0, ((1, 32),), jnp.float32)
    obs_precision = jnp.clip(jnp.exp(math.log(10.0) - 2.3025851 * jax.random.uniform(key_of[7], (TILES, NOBS), jnp.float32) ** level_of(key_of[7], (TILES, NOBS), ((0, 32),), -0.2, 0.2)), 1.0, 10.0)
    return {"ensemble": ensemble, "alpha": alpha, "lat_lower": lat_lower, "lat_weight": lat_weight, "background": background, "obs_cell": obs_cell, "obs_value": obs_value, "obs_precision": obs_precision}


advect_rate = 0.25
highest = lax.Precision.HIGHEST

def smooth_field(grid_field):
    padded = jnp.pad(grid_field, ((0, 0), (0, 0), (1, 1), (0, 0)))
    grid_field = 0.25 * padded[:, :, :-2] + 0.5 * padded[:, :, 1:-1] + 0.25 * padded[:, :, 2:]
    return 0.25 * jnp.roll(grid_field, 1, 3) + 0.5 * grid_field + 0.25 * jnp.roll(grid_field, -1, 3)

def latitude_table(lat_lower, lat_weight):
    fine_index = jnp.arange(FLAT, dtype=jnp.int32)
    lower_row = fine_index // FLAT_B * CLAT_B + lat_lower
    coarse = jnp.arange(CLAT, dtype=jnp.int32)
    weight = lat_weight[:, None]
    return (1.0 - weight) * (coarse[None, :] == lower_row[:, None]) + weight * (coarse[None, :] == lower_row[:, None] + 1)

def longitude_table(coarse_cols, fine_cols):
    fine_ratio = fine_cols // coarse_cols
    fine_index = jnp.arange(fine_cols, dtype=jnp.int32)
    numerator = 2 * fine_index + 1 + fine_ratio
    upper_col = numerator // (2 * fine_ratio)
    fraction = (numerator % (2 * fine_ratio)).astype(jnp.float32) / (2 * fine_ratio)
    coarse = jnp.arange(coarse_cols, dtype=jnp.int32)[:, None]
    low_col = (upper_col - 1) % coarse_cols
    high_col = upper_col % coarse_cols
    return (1.0 - fraction)[None, :] * (coarse == low_col[None, :]) + fraction[None, :] * (coarse == high_col[None, :])

def reference(ensemble, alpha, lat_lower, lat_weight, background, obs_cell, obs_value, obs_precision):
    member_scale = 1.0 / math.sqrt(MEMBERS - 1)
    members_f = ensemble.astype(jnp.float32)
    increment = lax.optimization_barrier(jnp.sum(smooth_field(alpha) * members_f, axis=0)) * member_scale
    lat_table = latitude_table(lat_lower, lat_weight)
    lon_table = longitude_table(CLON, FLON)
    fine_grid = background.reshape(LEV, N_BAND, N_MEM, FLAT_B, FLON_T).transpose(0, 1, 3, 2, 4).reshape(LEV, FLAT, FLON)
    indices = jnp.broadcast_to(obs_cell[None], (LEV, TILES, NOBS))

    def fine_model(incr):
        lat_rows = jnp.einsum('ik,lkc->lic', lat_table, incr, precision=highest)
        fine_incr = jnp.einsum('lic,cj->lij', lat_rows, lon_table, precision=highest)
        fine_state = fine_grid + fine_incr
        lon_slope = 0.5 * (jnp.roll(fine_state, -1, 2) - jnp.roll(fine_state, 1, 2))
        moved = fine_state - advect_rate * fine_state * lon_slope
        return moved.reshape(LEV, N_BAND, FLAT_B, N_MEM, FLON_T).transpose(0, 1, 3, 2, 4).reshape(LEV, TILES, TILE_CELLS)

    def observed_of(incr):
        return jnp.take_along_axis(fine_model(incr), indices, axis=2)
    advected = fine_model(increment)
    observed, pullback = jax.vjp(observed_of, increment)
    weighted = obs_precision[None] * (observed - obs_value)
    coarse_gradient = pullback(weighted)[0]
    gradient = smooth_field(members_f * coarse_gradient[None] * member_scale)
    return (advected, gradient)
```

```python
import functools
import math

import jax
import jax.numpy as jnp
from jax import lax
from jax.experimental import pallas as pl
from jax.experimental.pallas import tpu as pltpu
from jax.sharding import PartitionSpec as P

advect_rate = 0.25
LANES = 128
SUB = 8
RG = 16
f32 = jnp.float32
bf16 = jnp.bfloat16


def split2(x):
    hi = x.astype(bf16)
    lo = (x - hi.astype(f32)).astype(bf16)
    return hi, lo


def split2f(x):
    hi = x.astype(bf16).astype(f32)
    return hi, x - hi


def dims(a, b, ca, cb):
    return lax.dot_general(a, b, (((ca,), (cb,)), ((), ())), preferred_element_type=f32)


def iota(shape, d):
    return lax.broadcasted_iota(jnp.int32, shape, d)


def smooth_lon(x):
    n = x.shape[1]
    return 0.25 * pltpu.roll(x, 1, 1) + 0.5 * x + 0.25 * pltpu.roll(x, n - 1, 1)


def lon_weights(ratio):
    def parts(shift):
        num = 2 * shift + 1 + ratio
        return num // (2 * ratio), (num % (2 * ratio)) / (2 * ratio)

    def taps(shift):
        q, f = parts(shift)
        w = [0.0, 0.0, 0.0]
        for at, v in ((q, 1.0 - f), (q + 1, f)):
            if v:
                w[at] += v
        return w

    value = [taps(b) for b in range(ratio)]
    slope = [[0.5 * (p - m) for p, m in zip(taps(b + 1), taps(b - 1))] for b in range(ratio)]
    return value, slope


def combine(weights, parts):
    out = None
    for w, p in zip(weights, parts):
        if w == 0.0:
            continue
        term = p if w == 1.0 else w * p
        out = term if out is None else out + term
    return out


def kernel(
    cfg,
    ens_hbm,
    alpha_hbm,
    low_hbm,
    wt_hbm,
    bg_hbm,
    cell_hbm,
    val_hbm,
    prec_hbm,
    adv_ref,
    grad_ref,
    ens_in,
    alpha,
    low,
    wt,
    bg,
    cell,
    val,
    prec,
    ensf,
    plain,
    part,
    edge_send,
    edge_recv,
    send1,
    recv1,
    table_hi,
    table_lo,
    zbuf,
    rbuf,
    abuf,
    fine_bg,
    obs_a,
    obs_b,
    fe_send,
    fe_recv,
    lbuf,
    gbuf,
    advbuf,
    send2,
    recv2,
    recvx,
    merged,
    in_sem,
    edge_ss,
    edge_rs,
    ss1,
    rs1,
    fe_ss,
    fe_rs,
    ss2,
    rs2,
    ssx,
    rsx,
):
    n, nb, lev, rows, lon, fine_rows, fine_cols, scale = cfg
    block = lon // n
    frame = block + 2
    ratio = fine_cols // block
    main = lev * rows
    tiles = lon // LANES
    ng = fine_rows // RG
    gcells = RG * fine_cols
    gl = RG * RG
    levp = RG
    xs = recvx.shape[0]
    me = lax.axis_index("mem")
    band = lax.axis_index("band")
    has_up = band > 0
    has_down = band < nb - 1
    has = (has_up, has_down)
    wv, ws = lon_weights(ratio)

    barrier = pltpu.get_barrier_semaphore()

    def greet(o, c):
        pl.semaphore_signal(barrier, inc=1, device_id={"mem": lax.rem(me + o, n)})
        return c

    lax.fori_loop(1, n, greet, 0)

    @pl.when(has_up)
    def _():
        pl.semaphore_signal(barrier, inc=1, device_id={"band": band - 1})

    @pl.when(has_down)
    def _():
        pl.semaphore_signal(barrier, inc=1, device_id={"band": band + 1})

    loads = [
        pltpu.make_async_copy(src, dst, in_sem.at[i])
        for i, (src, dst) in enumerate(
            (
                (alpha_hbm, alpha),
                (ens_hbm, ens_in),
                (bg_hbm, bg),
                (low_hbm, low),
                (wt_hbm, wt),
                (cell_hbm, cell),
                (val_hbm, val),
                (prec_hbm, prec),
            )
        )
    ]
    for c in loads:
        c.start()

    for ref in (recv1, recv2, recvx):
        ref[:, :, frame:, :] = jnp.zeros(ref.shape[:2] + (ref.shape[2] - frame, LANES), f32)
    part[main:, :] = jnp.zeros((part.shape[0] - main, lon), f32)
    edge_send[...] = jnp.zeros(edge_send.shape, f32)
    fe_send[...] = jnp.zeros(fe_send.shape, f32)

    loads[0].wait()
    loads[1].wait()

    def whole(ref):
        parts = [ref[t] for t in range(tiles)]
        return parts[0] if tiles == 1 else jnp.concatenate(parts, axis=1)

    def row(ref, k):
        parts = [ref.at[t][pl.ds(k, lev, stride=rows), :] for t in range(tiles)]
        return parts[0] if tiles == 1 else jnp.concatenate(parts, axis=1)

    for t in range(tiles):
        ensf[t] = ens_in[t].astype(f32)
    al = whole(alpha)
    en = whole(ensf)
    kk = iota((main, lon), 0) % rows
    a_up = jnp.where(kk == 0, 0.0, pltpu.roll(al, 1, 0))
    a_dn = jnp.where(kk == rows - 1, 0.0, pltpu.roll(al, main - 1, 0))
    z = smooth_lon(0.25 * (a_up + a_dn) + 0.5 * al) * en * scale
    for t in range(tiles):
        plain[t] = z[:, t * LANES : (t + 1) * LANES]
    part[0:main, :] = z
    mine = []
    for side, k in ((0, 0), (1, rows - 1)):
        a_edge = smooth_lon(row(alpha, k)) * (0.25 * scale)
        e_edge = row(ensf, k)
        mine.append((a_edge, e_edge))
        edge_send[side, 0, 0:lev, :] = a_edge
        edge_send[side, 1, 0:lev, :] = e_edge
        edge_send[side, 2, 0:lev, :] = row(plain, k)

    def lay(g):
        block_rows = part[g * LANES : (g + 1) * LANES, :]
        block_rows = pltpu.roll(block_rows, 1, 1)
        for t in range(tiles):
            send1[g, t * LANES : (t + 1) * LANES, :] = block_rows[:, t * LANES : (t + 1) * LANES].T
        send1[g, lon : lon + SUB, :] = send1[g, 0:SUB, :]

    lay(0)

    if nb == 2:
        pl.semaphore_wait(barrier, n)
    else:
        pl.semaphore_wait(barrier, n - 1 + has_up.astype(jnp.int32) + has_down.astype(jnp.int32))

    def edge_copy(side):
        return pltpu.make_async_remote_copy(
            src_ref=edge_send.at[side],
            dst_ref=edge_recv.at[1 - side],
            send_sem=edge_ss.at[side],
            recv_sem=edge_rs.at[1 - side],
            device_id={"band": band - 1 if side == 0 else band + 1},
        )

    for side in (0, 1):

        @pl.when(has[side])
        def _():
            edge_copy(side).start()

        @pl.when(jnp.logical_not(has[side]))
        def _():
            edge_recv[side] = jnp.zeros(edge_recv.shape[1:], f32)
            if xs > 1:
                recvx[side, :, 0:frame, :] = jnp.zeros((n, frame, LANES), f32)

    def copy1(g, dst):
        return pltpu.make_async_remote_copy(
            src_ref=send1.at[g, pl.ds(pl.multiple_of(dst * block, block), frame), :],
            dst_ref=recv1.at[g, me, pl.ds(0, frame), :],
            send_sem=ss1.at[g, dst],
            recv_sem=rs1.at[g, me],
            device_id={"mem": dst},
        )

    def others(go):
        def step(o, c):
            go(lax.rem(me + o, n))
            return c

        lax.fori_loop(1, n, step, 0)

    def arrive1(g, src):
        got = recv1.at[g, src, pl.ds(0, frame), :]
        pltpu.make_async_copy(got, got, rs1.at[g, src]).wait()

    others(lambda d: copy1(0, d).start())

    loads[2].wait()
    row32 = iota((4 * SUB, gcells), 0)
    col_of = jnp.where(row32 < ratio * SUB, (row32 % SUB) * ratio + row32 // SUB, -1)
    pick = (iota((4 * SUB, gcells), 1) % fine_cols == col_of).astype(f32).astype(bf16)
    pick2 = jnp.concatenate([pick, pick], axis=1)
    in_row = iota((RG, gcells), 1) // fine_cols == iota((RG, gcells), 0)
    zbuf[main:, :] = jnp.zeros((gl - main, 2 * gcells), bf16)
    back = bg[:, 0, :]
    for g in range(ng):
        hi, lo = split2f(back[:, g * gcells : (g + 1) * gcells])
        for l in range(lev):
            at = slice(l * RG, (l + 1) * RG)
            zbuf[at, 0:gcells] = jnp.where(in_row, jnp.broadcast_to(hi[l : l + 1], (RG, gcells)), 0.0).astype(bf16)
            zbuf[at, gcells : 2 * gcells] = jnp.where(in_row, jnp.broadcast_to(lo[l : l + 1], (RG, gcells)), 0.0).astype(bf16)
        fine_bg[:, g * gl : (g + 1) * gl] = dims(pick2, zbuf[...], 1, 1)
    first = fine_bg[0:1, :]
    last = fine_bg[ratio * SUB - 1 : ratio * SUB, :]
    for t in range(ng * gl // LANES):
        fe_send[0, t : t + 1, :] = first[:, t * LANES : (t + 1) * LANES]
        fe_send[1, t : t + 1, :] = last[:, t * LANES : (t + 1) * LANES]

    def fe_copy(side):
        return pltpu.make_async_remote_copy(
            src_ref=fe_send.at[side],
            dst_ref=fe_recv.at[1 - side],
            send_sem=fe_ss.at[side],
            recv_sem=fe_rs.at[1 - side],
            device_id={"mem": lax.rem(me + (n - 1 if side == 0 else 1), n)},
        )

    fe_copy(0).start()
    fe_copy(1).start()

    for side in (0, 1):

        @pl.when(has[side])
        def _():
            pltpu.make_async_copy(edge_recv.at[side], edge_recv.at[side], edge_rs.at[side]).wait()

        a_edge, e_edge = mine[side]
        at = main + side * 2 * levp
        part[at : at + lev, :] = edge_recv[side, 2, 0:lev, :] + edge_recv[side, 1, 0:lev, :] * a_edge
        part[at + levp : at + levp + lev, :] = edge_recv[side, 0, 0:lev, :] * e_edge
    lay(1)
    others(lambda d: copy1(1, d).start())
    for g in (0, 1):
        recv1[g, me] = send1[g, pl.ds(pl.multiple_of(me * block, block), 2 * SUB), :]

    loads[3].wait()
    loads[4].wait()
    lane = iota((SUB, LANES), 1)

    def per_row(v):
        v = jnp.concatenate([v, jnp.zeros((1, LANES - fine_rows), f32)], axis=1)
        v = jnp.broadcast_to(v, (SUB, LANES))
        out = []
        for g in range(ng):
            r = v if g == 0 else pltpu.roll(v, LANES - g * RG, 1)
            r = jnp.where(lane < RG, r, 0.0)
            for s in (RG, 2 * RG, 4 * RG):
                r = r + pltpu.roll(r, s, 1)
            out += [r] * (gl // LANES)
        return jnp.concatenate(out, axis=1)[0:1]

    wide = ng * gl
    wl = per_row(wt[...])
    jl = iota((1, wide), 1) % gl
    key0 = per_row(low[...].astype(f32)) + ((jl // RG) * 64 + 1).astype(f32)
    key1 = key0 + 1.0
    w_hi, w_lo = split2f(wl)
    o_hi, o_lo = split2f(1.0 - wl)
    chunk = 2 * RG

    def table_step(i, c):
        kap = iota((chunk, 1), 0) + i * chunk
        e = kap - main
        es = e // levp
        ek = jnp.where(es == 0, -1, jnp.where(es == 1, 0, jnp.where(es == 2, rows, rows - 1)))
        l = jnp.where(e < 0, kap // rows, e % levp)
        k = jnp.where(e < 0, kap % rows, ek)
        key = jnp.where(l < lev, l * 64 + k + 1, -1).astype(f32)
        m0 = key == key0
        m1 = key == key1
        at = pl.ds(pl.multiple_of(i * chunk, chunk), chunk)
        table_hi[at, :] = jnp.where(m0, o_hi, jnp.where(m1, w_hi, 0.0)).astype(bf16)
        table_lo[at, :] = jnp.where(m0, o_lo, jnp.where(m1, w_lo, 0.0)).astype(bf16)
        return c

    lax.fori_loop(0, table_hi.shape[0] // chunk, table_step, 0)

    for i in (5, 6, 7):
        loads[i].wait()
    nobs = cell.shape[1]
    crow = cell[...] // fine_cols
    ccol = cell[...] % fine_cols
    r32 = iota((4 * SUB, nobs), 0)
    col_o = jnp.where(r32 < ratio * SUB, (r32 % SUB) * ratio + r32 // SUB, -1)
    hot = (col_o == ccol).astype(f32).astype(bf16)
    hot2 = jnp.concatenate([hot, hot], axis=1)
    pr = prec[...]
    p_hi, p_lo = split2f(pr)
    v_hi, v_lo = split2f(val[:, 0, :] * pr)
    rbuf[main:, :] = jnp.zeros((gl - main, 2 * nobs), bf16)
    for g in range(ng):
        at_row = iota((RG, nobs), 0) + g * RG == crow
        for l in range(lev):
            at = slice(l * RG, (l + 1) * RG)
            rbuf[at, 0:nobs] = jnp.where(at_row, jnp.broadcast_to(v_hi[l : l + 1], (RG, nobs)), 0.0).astype(bf16)
            rbuf[at, nobs : 2 * nobs] = jnp.where(at_row, jnp.broadcast_to(v_lo[l : l + 1], (RG, nobs)), 0.0).astype(bf16)
        obs_b[:, g * gl : (g + 1) * gl] = dims(hot2, rbuf[...], 1, 1)
        ph = jnp.where(at_row, jnp.broadcast_to(p_hi, (RG, nobs)), 0.0).astype(bf16)
        plo = jnp.where(at_row, jnp.broadcast_to(p_lo, (RG, nobs)), 0.0).astype(bf16)
        for j in range(LANES // RG):
            abuf[j * RG : (j + 1) * RG, 0:nobs] = ph
            abuf[j * RG : (j + 1) * RG, nobs : 2 * nobs] = plo
        oa = dims(hot2, abuf[...], 1, 1)
        for j in range(gl // LANES):
            obs_a[:, g * gl + j * LANES : g * gl + (j + 1) * LANES] = oa

    for side in (0, 1):
        pltpu.make_async_copy(fe_recv.at[side], fe_recv.at[side], fe_rs.at[side]).wait()
    nt = wide // LANES
    left = jnp.concatenate([fe_recv[0, t : t + 1, :] for t in range(nt)], axis=1)
    right = jnp.concatenate([fe_recv[1, t : t + 1, :] for t in range(nt)], axis=1)
    fb = [fine_bg[b * SUB : (b + 1) * SUB, :] for b in range(ratio)]
    arow = iota((SUB, wide), 0)
    before0 = jnp.where(arow == 0, left, pltpu.roll(fb[ratio - 1], 1, 0))
    after_last = jnp.where(arow == SUB - 1, right, pltpu.roll(fb[0], SUB - 1, 0))
    chain = [before0] + fb + [after_last]
    slope_bg = [0.5 * (chain[b + 2] - chain[b]) for b in range(ratio)]

    others(lambda s: arrive1(0, s))
    others(lambda s: arrive1(1, s))
    xg = []
    for g in (0, 1):
        total = recv1[g, 0]
        for s in range(1, n):
            total = total + recv1[g, s]
        xg.append(total)
    x = jnp.concatenate(xg, axis=1)
    x_hi, x_lo = split2f(x)
    x2 = jnp.concatenate([x_hi, x_lo], axis=0).astype(bf16)
    y = dims(x2, table_hi[...], 1, 0)
    y = y[0:16] + y[16:32] + dims(x_hi.astype(bf16), table_lo[...], 1, 0)
    lbuf[...] = y
    taps = [lbuf[d : d + SUB, :] for d in range(3)]

    us, vs, moved = [], [], []
    for b in range(ratio):
        state = fb[b] + combine(wv[b], taps)
        slope = slope_bg[b] + combine(ws[b], taps)
        factor = 1.0 - advect_rate * slope
        mv = state * factor
        at = slice(b * SUB, (b + 1) * SUB)
        cot = obs_a[at, :] * mv - obs_b[at, :]
        us.append(cot * factor)
        vs.append((-advect_rate) * (state * cot))
        moved.append(mv)
    gbuf[...] = jnp.zeros(gbuf.shape, f32)
    for d in range(3):
        t = combine([wv[b][d] for b in range(ratio)] + [ws[b][d] for b in range(ratio)], us + vs)
        gbuf[d : d + SUB, :] += t
    gl_v = gbuf[...]
    g_hi, g_lo = split2f(gl_v)
    g2 = jnp.concatenate([g_hi, g_lo], axis=0).astype(bf16)
    gr = dims(g2, table_hi[...], 1, 1)
    gr = gr[0:16] + gr[16:32] + dims(g_hi.astype(bf16), table_lo[...], 1, 1)
    for g in (0, 1):
        send2[g] = gr[:, g * LANES : (g + 1) * LANES]

    def copyx(side, dst):
        return pltpu.make_async_remote_copy(
            src_ref=send2.at[1, pl.ds(0, frame), :],
            dst_ref=recvx.at[0 if xs == 1 else 1 - side, me, pl.ds(0, frame), :],
            send_sem=ssx.at[side, dst],
            recv_sem=rsx.at[0 if xs == 1 else 1 - side, me],
            device_id={"mem": dst, "band": band - 1 if side == 0 else band + 1},
        )

    def copy2(g, dst):
        return pltpu.make_async_remote_copy(
            src_ref=send2.at[g, pl.ds(0, frame), :],
            dst_ref=recv2.at[g, me, pl.ds(0, frame), :],
            send_sem=ss2.at[g, dst],
            recv_sem=rs2.at[g, me],
            device_id={"mem": dst},
        )

    def everyone(go):
        def step(o, c):
            go(lax.rem(me + o, n))
            return c

        lax.fori_loop(0, n, step, 0)

    for side in (0, 1):

        @pl.when(has[side])
        def _():
            everyone(lambda d: copyx(side, d).start())

    def both(d):
        copy2(0, d).start()
        copy2(1, d).start()

    others(both)
    for g in (0, 1):
        recv2[g, me] = send2[g]

    advbuf[...] = jnp.concatenate(moved + [jnp.zeros((SUB, wide), f32)], axis=0)
    pickt = jnp.concatenate([pick, pick], axis=0)
    for g in range(ng):
        hi, lo = split2(advbuf[:, g * gl : g * gl + main])
        e = dims(jnp.concatenate([hi, lo], axis=0), pickt, 0, 0)
        for l in range(lev):
            v = jnp.where(in_row, e[l * RG : (l + 1) * RG], 0.0)
            adv_ref[l, :, g * gcells : (g + 1) * gcells] = jnp.sum(v, axis=0, keepdims=True)

    def arrive2(s):
        for g in (0, 1):
            got = recv2.at[g, s, pl.ds(0, frame), :]
            pltpu.make_async_copy(got, got, rs2.at[g, s]).wait()

    others(arrive2)
    for side in (0, 1):

        @pl.when(has[side])
        def _():
            def step(s):
                i = 0 if xs == 1 else side
                got = recvx.at[i, s, pl.ds(0, frame), :]
                pltpu.make_async_copy(got, got, rsx.at[i, s]).wait()

            everyone(step)

    over = iota((SUB, LANES), 0) < frame - block

    def gather(ref):
        for d in range(n):
            tail = jnp.where(over, ref[(d - 1) % n, SUB : 2 * SUB, :], 0.0)
            merged[d * SUB : (d + 1) * SUB, :] = ref[d, 0:SUB, :] + tail
        cols = [merged[t * LANES : (t + 1) * LANES, :].T for t in range(tiles)]
        cols = cols[0] if tiles == 1 else jnp.concatenate(cols, axis=1)
        return pltpu.roll(cols, lon - 1, 1)

    c0 = gather(recv2.at[0])
    c1 = gather(recv2.at[1])
    cx = [gather(recvx.at[i]) for i in range(xs)]
    cu, cd = cx[0], cx[-1]
    e0 = main - LANES
    coarse = jnp.concatenate([c0, c1[0:e0]], axis=0)
    en = whole(ensf)
    wm = en * coarse * scale
    w_up = jnp.where(kk == 0, 0.0, pltpu.roll(wm, 1, 0))
    w_dn = jnp.where(kk == rows - 1, 0.0, pltpu.roll(wm, main - 1, 0))
    zz = smooth_lon(0.25 * (w_up + w_dn) + 0.5 * wm)
    for t in range(tiles):
        grad_ref[t] = zz[:, t * LANES : (t + 1) * LANES]
    for side, k, k_in in ((0, 0, 1), (1, rows - 1, rows - 2)):
        src = (cu, cd)[side]
        mine_at = e0 + side * 2 * levp
        edge_at = e0 + (1 - side) * 2 * levp
        extra = jnp.where(has[side], src[edge_at : edge_at + lev], 0.0)
        halo = c1[mine_at : mine_at + lev] + jnp.where(has[side], src[edge_at + levp : edge_at + levp + lev], 0.0)
        we = row(ensf, k) * extra * scale
        wh = edge_recv[side, 1, 0:lev, :] * halo * scale
        z_edge = smooth_lon(0.5 * we + 0.25 * wh)
        z_in = smooth_lon(0.25 * we)
        for t in range(tiles):
            cut = slice(t * LANES, (t + 1) * LANES)
            grad_ref.at[t][pl.ds(k, lev, stride=rows), :] += z_edge[:, cut]
            grad_ref.at[t][pl.ds(k_in, lev, stride=rows), :] += z_in[:, cut]

    for side in (0, 1):
        fe_copy(side).wait_send()

        @pl.when(has[side])
        def _():
            edge_copy(side).wait_send()
            everyone(lambda d: copyx(side, d).wait_send())

    def sent(d):
        for g in (0, 1):
            copy1(g, d).wait_send()
            copy2(g, d).wait_send()

    others(sent)


def up_to(x, m):
    return -(-x // m) * m


def to_tiles(x):
    return x.reshape(-1, x.shape[3] // LANES, LANES).swapaxes(0, 1)


def shards(ensemble, alpha, lat_lower, lat_weight, background, obs_cell, obs_value, obs_precision):
    n, nb = lax.axis_size("mem"), lax.axis_size("band")
    members, lev, rows, lon = ensemble.shape
    fine_rows = lat_lower.shape[0]
    cells = background.shape[2]
    nobs = obs_cell.shape[1]
    fine_cols = cells // fine_rows
    scale = 1.0 / math.sqrt(members * n - 1)
    block = lon // n
    main = lev * rows
    kaps = main + 4 * RG
    assert members == 1 and block == SUB and rows == RG and lev <= RG and kaps == 2 * LANES
    assert fine_rows % RG == 0 and fine_cols % block == 0 and fine_cols // block == 3
    cfg = (n, nb, lev, rows, lon, fine_rows, fine_cols, scale)
    tiles = lon // LANES
    ng = fine_rows // RG
    gl = RG * RG
    wide = ng * gl
    gcells = RG * fine_cols
    xs = 1 if nb == 2 else 2
    dma = pltpu.SemaphoreType.DMA
    vm = pl.BlockSpec(memory_space=pltpu.VMEM)
    hbm = pl.BlockSpec(memory_space=pltpu.HBM)
    fr = 2 * SUB
    advected, gradient = pl.pallas_call(
        functools.partial(kernel, cfg),
        out_shape=(
            jax.ShapeDtypeStruct(background.shape, f32),
            jax.ShapeDtypeStruct((tiles, main, LANES), f32),
        ),
        in_specs=[hbm] * 8,
        out_specs=(vm, vm),
        scratch_shapes=[
            pltpu.VMEM((tiles, main, LANES), bf16),
            pltpu.VMEM((tiles, main, LANES), f32),
            pltpu.VMEM((1, fine_rows), jnp.int32),
            pltpu.VMEM((1, fine_rows), f32),
            pltpu.VMEM(background.shape, f32),
            pltpu.VMEM((1, nobs), jnp.int32),
            pltpu.VMEM(obs_value.shape, f32),
            pltpu.VMEM((1, nobs), f32),
            pltpu.VMEM((tiles, main, LANES), f32),
            pltpu.VMEM((tiles, main, LANES), f32),
            pltpu.VMEM((kaps, lon), f32),
            pltpu.VMEM((2, 3, RG, lon), f32),
            pltpu.VMEM((2, 3, RG, lon), f32),
            pltpu.VMEM((2, lon + SUB, LANES), f32),
            pltpu.VMEM((2, n, fr, LANES), f32),
            pltpu.VMEM((kaps, wide), bf16),
            pltpu.VMEM((kaps, wide), bf16),
            pltpu.VMEM((gl, 2 * gcells), bf16),
            pltpu.VMEM((gl, 2 * nobs), bf16),
            pltpu.VMEM((LANES, 2 * nobs), bf16),
            pltpu.VMEM((4 * SUB, wide), f32),
            pltpu.VMEM((4 * SUB, wide), f32),
            pltpu.VMEM((4 * SUB, wide), f32),
            pltpu.VMEM((2, SUB, LANES), f32),
            pltpu.VMEM((2, SUB, LANES), f32),
            pltpu.VMEM((fr, wide), f32),
            pltpu.VMEM((fr, wide), f32),
            pltpu.VMEM((4 * SUB, wide), f32),
            pltpu.VMEM((2, fr, LANES), f32),
            pltpu.VMEM((2, n, fr, LANES), f32),
            pltpu.VMEM((xs, n, fr, LANES), f32),
            pltpu.VMEM((lon, LANES), f32),
            dma((8,)),
            dma((2,)),
            dma((2,)),
            dma((2, n)),
            dma((2, n)),
            dma((2,)),
            dma((2,)),
            dma((2, n)),
            dma((2, n)),
            dma((2, n)),
            dma((xs, n)),
        ],
        compiler_params=pltpu.CompilerParams(collective_id=0, has_side_effects=True, vmem_limit_bytes=48 * 2**20),
    )(
        to_tiles(ensemble),
        to_tiles(alpha),
        lat_lower.reshape(1, fine_rows),
        lat_weight.reshape(1, fine_rows),
        background,
        obs_cell,
        obs_value,
        obs_precision,
    )
    return advected, gradient.swapaxes(0, 1).reshape(members, lev, rows, lon)


def solution(mesh):
    return jax.shard_map(
        shards,
        mesh=mesh,
        in_specs=(
            P("mem", None, "band", None),
            P("mem", None, "band", None),
            P("band"),
            P("band"),
            P(None, ("band", "mem"), None),
            P(("band", "mem"), None),
            P(None, ("band", "mem"), None),
            P(("band", "mem"), None),
        ),
        out_specs=(P(None, ("band", "mem"), None), P("mem", None, "band", None)),
        check_vma=False,
    )
```

```python
import functools
import math

import jax
import jax.numpy as jnp
from jax import lax
from jax.experimental import pallas as pl
from jax.experimental.pallas import tpu as pltpu
from jax.sharding import PartitionSpec as P

advect_rate = 0.25
LANES = 128
SUB = 8
RG = 16
f32 = jnp.float32
bf16 = jnp.bfloat16


def split2(x):
    hi = x.astype(bf16)
    lo = (x - hi.astype(f32)).astype(bf16)
    return hi, lo


def split2f(x):
    hi = x.astype(bf16).astype(f32)
    return hi, x - hi


def dims(a, b, ca, cb):
    return lax.dot_general(a, b, (((ca,), (cb,)), ((), ())), preferred_element_type=f32)


def iota(shape, d):
    return lax.broadcasted_iota(jnp.int32, shape, d)


def smooth_lon(x):
    n = x.shape[1]
    return 0.25 * pltpu.roll(x, 1, 1) + 0.5 * x + 0.25 * pltpu.roll(x, n - 1, 1)


def lon_weights(ratio):
    def parts(shift):
        num = 2 * shift + 1 + ratio
        return num // (2 * ratio), (num % (2 * ratio)) / (2 * ratio)

    def taps(shift):
        q, f = parts(shift)
        w = [0.0, 0.0, 0.0]
        for at, v in ((q, 1.0 - f), (q + 1, f)):
            if v:
                w[at] += v
        return w

    value = [taps(b) for b in range(ratio)]
    slope = [[0.5 * (p - m) for p, m in zip(taps(b + 1), taps(b - 1))] for b in range(ratio)]
    return value, slope


def combine(weights, parts):
    out = None
    for w, p in zip(weights, parts):
        if w == 0.0:
            continue
        term = p if w == 1.0 else w * p
        out = term if out is None else out + term
    return out


def kernel(
    cfg,
    ens_hbm,
    alpha_hbm,
    low_hbm,
    wt_hbm,
    bg_hbm,
    cell_hbm,
    val_hbm,
    prec_hbm,
    adv_ref,
    grad_ref,
    ens_in,
    alpha,
    low,
    wt,
    bg,
    cell,
    val,
    prec,
    ensf,
    plain,
    part,
    edge_send,
    edge_recv,
    send1,
    recv1,
    table_hi,
    table_lo,
    zbuf,
    rbuf,
    abuf,
    fine_bg,
    obs_a,
    obs_b,
    fe_send,
    fe_recv,
    lbuf,
    gbuf,
    advbuf,
    send2,
    recv2,
    recvx,
    merged,
    in_sem,
    edge_ss,
    edge_rs,
    ss1,
    rs1,
    fe_ss,
    fe_rs,
    ss2,
    rs2,
    ssx,
    rsx,
):
    n, nb, lev, rows, lon, fine_rows, fine_cols, scale = cfg
    block = lon // n
    frame = block + 2
    ratio = fine_cols // block
    main = lev * rows
    tiles = lon // LANES
    ng = fine_rows // RG
    gcells = RG * fine_cols
    gl = RG * RG
    levp = RG
    xs = recvx.shape[0]
    me = lax.axis_index("mem")
    band = lax.axis_index("band")
    has_up = band > 0
    has_down = band < nb - 1
    has = (has_up, has_down)
    wv, ws = lon_weights(ratio)

    barrier = pltpu.get_barrier_semaphore()

    for o in sorted(range(1, n), key=lambda o: -min(o, n - o)):
        pl.semaphore_signal(barrier, inc=1, device_id={"mem": lax.rem(me + o, n)})

    @pl.when(has_up)
    def _():
        pl.semaphore_signal(barrier, inc=1, device_id={"band": band - 1})

    @pl.when(has_down)
    def _():
        pl.semaphore_signal(barrier, inc=1, device_id={"band": band + 1})

    loads = [
        pltpu.make_async_copy(src, dst, in_sem.at[i])
        for i, (src, dst) in enumerate(
            (
                (alpha_hbm, alpha),
                (ens_hbm, ens_in),
                (bg_hbm, bg),
                (low_hbm, low),
                (wt_hbm, wt),
                (cell_hbm, cell),
                (val_hbm, val),
                (prec_hbm, prec),
            )
        )
    ]
    for c in loads:
        c.start()

    for ref in (recv1, recv2, recvx):
        ref[:, :, frame:, :] = jnp.zeros(ref.shape[:2] + (ref.shape[2] - frame, LANES), f32)
    part[main:, :] = jnp.zeros((part.shape[0] - main, lon), f32)
    edge_send[...] = jnp.zeros(edge_send.shape, f32)
    fe_send[...] = jnp.zeros(fe_send.shape, f32)

    loads[0].wait()
    loads[1].wait()

    def whole(ref):
        parts = [ref[t] for t in range(tiles)]
        return parts[0] if tiles == 1 else jnp.concatenate(parts, axis=1)

    def row(ref, k):
        parts = [ref.at[t][pl.ds(k, lev, stride=rows), :] for t in range(tiles)]
        return parts[0] if tiles == 1 else jnp.concatenate(parts, axis=1)

    for t in range(tiles):
        ensf[t] = ens_in[t].astype(f32)
    al = whole(alpha)
    en = whole(ensf)
    kk = iota((main, lon), 0) % rows
    a_up = jnp.where(kk == 0, 0.0, pltpu.roll(al, 1, 0))
    a_dn = jnp.where(kk == rows - 1, 0.0, pltpu.roll(al, main - 1, 0))
    z = smooth_lon(0.25 * (a_up + a_dn) + 0.5 * al) * en * scale
    for t in range(tiles):
        plain[t] = z[:, t * LANES : (t + 1) * LANES]
    part[0:main, :] = z
    mine = []
    for side, k in ((0, 0), (1, rows - 1)):
        a_edge = smooth_lon(row(alpha, k)) * (0.25 * scale)
        e_edge = row(ensf, k)
        mine.append((a_edge, e_edge))
        edge_send[side, 0, 0:lev, :] = a_edge
        edge_send[side, 1, 0:lev, :] = e_edge
        edge_send[side, 2, 0:lev, :] = row(plain, k)

    def lay(g):
        block_rows = part[g * LANES : (g + 1) * LANES, :]
        block_rows = pltpu.roll(block_rows, 1, 1)
        for t in range(tiles):
            send1[g, t * LANES : (t + 1) * LANES, :] = block_rows[:, t * LANES : (t + 1) * LANES].T
        send1[g, lon : lon + SUB, :] = send1[g, 0:SUB, :]

    lay(0)

    if nb == 2:
        pl.semaphore_wait(barrier, n)
    else:
        pl.semaphore_wait(barrier, n - 1 + has_up.astype(jnp.int32) + has_down.astype(jnp.int32))

    def edge_copy(side):
        return pltpu.make_async_remote_copy(
            src_ref=edge_send.at[side],
            dst_ref=edge_recv.at[1 - side],
            send_sem=edge_ss.at[side],
            recv_sem=edge_rs.at[1 - side],
            device_id={"band": band - 1 if side == 0 else band + 1},
        )

    for side in (0, 1):

        @pl.when(has[side])
        def _():
            edge_copy(side).start()

        @pl.when(jnp.logical_not(has[side]))
        def _():
            edge_recv[side] = jnp.zeros(edge_recv.shape[1:], f32)
            if xs > 1:
                recvx[side, :, 0:frame, :] = jnp.zeros((n, frame, LANES), f32)

    def copy1(g, dst):
        return pltpu.make_async_remote_copy(
            src_ref=send1.at[g, pl.ds(pl.multiple_of(dst * block, block), frame), :],
            dst_ref=recv1.at[g, me, pl.ds(0, frame), :],
            send_sem=ss1.at[g],
            recv_sem=rs1.at[g],
            device_id={"mem": dst},
        )

    def others(go):
        def step(o, c):
            go(lax.rem(me + o, n))
            return c

        lax.fori_loop(1, n, step, 0)

    def all_of(ref, count, sem):
        whole_ref = ref.at[pl.ds(0, count), pl.ds(0, frame), :]
        pltpu.make_async_copy(whole_ref, whole_ref, sem).wait()

    others(lambda d: copy1(0, d).start())

    loads[2].wait()
    row32 = iota((4 * SUB, gcells), 0)
    col_of = jnp.where(row32 < ratio * SUB, (row32 % SUB) * ratio + row32 // SUB, -1)
    pick = (iota((4 * SUB, gcells), 1) % fine_cols == col_of).astype(f32).astype(bf16)
    pick2 = jnp.concatenate([pick, pick], axis=1)
    in_row = iota((RG, gcells), 1) // fine_cols == iota((RG, gcells), 0)
    zbuf[main:, :] = jnp.zeros((gl - main, 2 * gcells), bf16)
    back = bg[:, 0, :]
    for g in range(ng):
        hi, lo = split2f(back[:, g * gcells : (g + 1) * gcells])
        for l in range(lev):
            at = slice(l * RG, (l + 1) * RG)
            zbuf[at, 0:gcells] = jnp.where(in_row, jnp.broadcast_to(hi[l : l + 1], (RG, gcells)), 0.0).astype(bf16)
            zbuf[at, gcells : 2 * gcells] = jnp.where(in_row, jnp.broadcast_to(lo[l : l + 1], (RG, gcells)), 0.0).astype(bf16)
        fine_bg[:, g * gl : (g + 1) * gl] = dims(pick2, zbuf[...], 1, 1)
    first = fine_bg[0:1, :]
    last = fine_bg[ratio * SUB - 1 : ratio * SUB, :]
    for t in range(ng * gl // LANES):
        fe_send[0, t : t + 1, :] = first[:, t * LANES : (t + 1) * LANES]
        fe_send[1, t : t + 1, :] = last[:, t * LANES : (t + 1) * LANES]

    def fe_copy(side):
        return pltpu.make_async_remote_copy(
            src_ref=fe_send.at[side],
            dst_ref=fe_recv.at[1 - side],
            send_sem=fe_ss.at[side],
            recv_sem=fe_rs.at[1 - side],
            device_id={"mem": lax.rem(me + (n - 1 if side == 0 else 1), n)},
        )

    fe_copy(0).start()
    fe_copy(1).start()

    for side in (0, 1):

        @pl.when(has[side])
        def _():
            pltpu.make_async_copy(edge_recv.at[side], edge_recv.at[side], edge_rs.at[side]).wait()

        a_edge, e_edge = mine[side]
        at = main + side * 2 * levp
        part[at : at + lev, :] = edge_recv[side, 2, 0:lev, :] + edge_recv[side, 1, 0:lev, :] * a_edge
        part[at + levp : at + levp + lev, :] = edge_recv[side, 0, 0:lev, :] * e_edge
    lay(1)
    others(lambda d: copy1(1, d).start())
    for g in (0, 1):
        recv1[g, me] = send1[g, pl.ds(pl.multiple_of(me * block, block), 2 * SUB), :]

    loads[3].wait()
    loads[4].wait()
    lane = iota((SUB, LANES), 1)

    def per_row(v):
        v = jnp.concatenate([v, jnp.zeros((1, LANES - fine_rows), f32)], axis=1)
        v = jnp.broadcast_to(v, (SUB, LANES))
        out = []
        for g in range(ng):
            r = v if g == 0 else pltpu.roll(v, LANES - g * RG, 1)
            r = jnp.where(lane < RG, r, 0.0)
            for s in (RG, 2 * RG, 4 * RG):
                r = r + pltpu.roll(r, s, 1)
            out += [r] * (gl // LANES)
        return jnp.concatenate(out, axis=1)[0:1]

    wide = ng * gl
    wl = per_row(wt[...])
    jl = iota((1, wide), 1) % gl
    key0 = per_row(low[...].astype(f32)) + ((jl // RG) * 64 + 1).astype(f32)
    key1 = key0 + 1.0
    w_hi, w_lo = split2f(wl)
    o_hi, o_lo = split2f(1.0 - wl)
    chunk = 2 * RG

    def table_step(i, c):
        kap = iota((chunk, 1), 0) + i * chunk
        e = kap - main
        es = e // levp
        ek = jnp.where(es == 0, -1, jnp.where(es == 1, 0, jnp.where(es == 2, rows, rows - 1)))
        l = jnp.where(e < 0, kap // rows, e % levp)
        k = jnp.where(e < 0, kap % rows, ek)
        key = jnp.where(l < lev, l * 64 + k + 1, -1).astype(f32)
        m0 = key == key0
        m1 = key == key1
        at = pl.ds(pl.multiple_of(i * chunk, chunk), chunk)
        table_hi[at, :] = jnp.where(m0, o_hi, jnp.where(m1, w_hi, 0.0)).astype(bf16)
        table_lo[at, :] = jnp.where(m0, o_lo, jnp.where(m1, w_lo, 0.0)).astype(bf16)
        return c

    lax.fori_loop(0, table_hi.shape[0] // chunk, table_step, 0)

    for i in (5, 6, 7):
        loads[i].wait()
    nobs = cell.shape[1]
    crow = cell[...] // fine_cols
    ccol = cell[...] % fine_cols
    r32 = iota((4 * SUB, nobs), 0)
    col_o = jnp.where(r32 < ratio * SUB, (r32 % SUB) * ratio + r32 // SUB, -1)
    hot = (col_o == ccol).astype(f32).astype(bf16)
    hot2 = jnp.concatenate([hot, hot], axis=1)
    pr = prec[...]
    p_hi, p_lo = split2f(pr)
    v_hi, v_lo = split2f(val[:, 0, :] * pr)
    rbuf[main:, :] = jnp.zeros((gl - main, 2 * nobs), bf16)
    for g in range(ng):
        at_row = iota((RG, nobs), 0) + g * RG == crow
        for l in range(lev):
            at = slice(l * RG, (l + 1) * RG)
            rbuf[at, 0:nobs] = jnp.where(at_row, jnp.broadcast_to(v_hi[l : l + 1], (RG, nobs)), 0.0).astype(bf16)
            rbuf[at, nobs : 2 * nobs] = jnp.where(at_row, jnp.broadcast_to(v_lo[l : l + 1], (RG, nobs)), 0.0).astype(bf16)
        obs_b[:, g * gl : (g + 1) * gl] = dims(hot2, rbuf[...], 1, 1)
        ph = jnp.where(at_row, jnp.broadcast_to(p_hi, (RG, nobs)), 0.0).astype(bf16)
        plo = jnp.where(at_row, jnp.broadcast_to(p_lo, (RG, nobs)), 0.0).astype(bf16)
        for j in range(LANES // RG):
            abuf[j * RG : (j + 1) * RG, 0:nobs] = ph
            abuf[j * RG : (j + 1) * RG, nobs : 2 * nobs] = plo
        oa = dims(hot2, abuf[...], 1, 1)
        for j in range(gl // LANES):
            obs_a[:, g * gl + j * LANES : g * gl + (j + 1) * LANES] = oa

    for side in (0, 1):
        pltpu.make_async_copy(fe_recv.at[side], fe_recv.at[side], fe_rs.at[side]).wait()
    nt = wide // LANES
    left = jnp.concatenate([fe_recv[0, t : t + 1, :] for t in range(nt)], axis=1)
    right = jnp.concatenate([fe_recv[1, t : t + 1, :] for t in range(nt)], axis=1)
    fb = [fine_bg[b * SUB : (b + 1) * SUB, :] for b in range(ratio)]
    arow = iota((SUB, wide), 0)
    before0 = jnp.where(arow == 0, left, pltpu.roll(fb[ratio - 1], 1, 0))
    after_last = jnp.where(arow == SUB - 1, right, pltpu.roll(fb[0], SUB - 1, 0))
    chain = [before0] + fb + [after_last]
    slope_bg = [0.5 * (chain[b + 2] - chain[b]) for b in range(ratio)]

    for g in (0, 1):
        all_of(recv1.at[g], n - 1, rs1.at[g])
    xg = []
    for g in (0, 1):
        total = recv1[g, 0]
        for s in range(1, n):
            total = total + recv1[g, s]
        xg.append(total)
    x = jnp.concatenate(xg, axis=1)
    x_hi, x_lo = split2f(x)
    x2 = jnp.concatenate([x_hi, x_lo], axis=0).astype(bf16)
    y = dims(x2, table_hi[...], 1, 0)
    y = y[0:16] + y[16:32] + dims(x_hi.astype(bf16), table_lo[...], 1, 0)
    lbuf[...] = y
    taps = [lbuf[d : d + SUB, :] for d in range(3)]

    us, vs, moved = [], [], []
    for b in range(ratio):
        state = fb[b] + combine(wv[b], taps)
        slope = slope_bg[b] + combine(ws[b], taps)
        factor = 1.0 - advect_rate * slope
        mv = state * factor
        at = slice(b * SUB, (b + 1) * SUB)
        cot = obs_a[at, :] * mv - obs_b[at, :]
        us.append(cot * factor)
        vs.append((-advect_rate) * (state * cot))
        moved.append(mv)
    gbuf[...] = jnp.zeros(gbuf.shape, f32)
    for d in range(3):
        t = combine([wv[b][d] for b in range(ratio)] + [ws[b][d] for b in range(ratio)], us + vs)
        gbuf[d : d + SUB, :] += t
    gl_v = gbuf[...]
    g_hi, g_lo = split2f(gl_v)
    g2 = jnp.concatenate([g_hi, g_lo], axis=0).astype(bf16)
    gr = dims(g2, table_hi[...], 1, 1)
    gr = gr[0:16] + gr[16:32] + dims(g_hi.astype(bf16), table_lo[...], 1, 1)
    for g in (0, 1):
        send2[g] = gr[:, g * LANES : (g + 1) * LANES]

    def copyx(side, dst):
        return pltpu.make_async_remote_copy(
            src_ref=send2.at[1, pl.ds(0, frame), :],
            dst_ref=recvx.at[0 if xs == 1 else 1 - side, me, pl.ds(0, frame), :],
            send_sem=ssx.at[side],
            recv_sem=rsx.at[0 if xs == 1 else 1 - side],
            device_id={"mem": dst, "band": band - 1 if side == 0 else band + 1},
        )

    def copy2(g, dst):
        return pltpu.make_async_remote_copy(
            src_ref=send2.at[g, pl.ds(0, frame), :],
            dst_ref=recv2.at[g, me, pl.ds(0, frame), :],
            send_sem=ss2.at[g],
            recv_sem=rs2.at[g],
            device_id={"mem": dst},
        )

    def everyone(go):
        def step(o, c):
            go(lax.rem(me + o, n))
            return c

        lax.fori_loop(0, n, step, 0)

    for side in (0, 1):

        @pl.when(has[side])
        def _():
            everyone(lambda d: copyx(side, d).start())

    def both(d):
        copy2(0, d).start()
        copy2(1, d).start()

    others(both)
    for g in (0, 1):
        recv2[g, me] = send2[g]

    advbuf[...] = jnp.concatenate(moved + [jnp.zeros((SUB, wide), f32)], axis=0)
    pickt = jnp.concatenate([pick, pick], axis=0)
    for g in range(ng):
        hi, lo = split2(advbuf[:, g * gl : g * gl + main])
        e = dims(jnp.concatenate([hi, lo], axis=0), pickt, 0, 0)
        for l in range(lev):
            v = jnp.where(in_row, e[l * RG : (l + 1) * RG], 0.0)
            adv_ref[l, :, g * gcells : (g + 1) * gcells] = jnp.sum(v, axis=0, keepdims=True)

    for g in (0, 1):
        all_of(recv1.at[g], n - 1, ss1.at[g])
    for side in (0, 1):
        fe_copy(side).wait_send()

        @pl.when(has[side])
        def _():
            edge_copy(side).wait_send()

    for side in (0, 1):

        @pl.when(has[side])
        def _():
            i = 0 if xs == 1 else side
            all_of(recvx.at[i], n, rsx.at[i])

    for g in (0, 1):
        all_of(recv2.at[g], n - 1, rs2.at[g])

    over = iota((SUB, LANES), 0) < frame - block

    def gather(ref):
        for d in range(n):
            tail = jnp.where(over, ref[(d - 1) % n, SUB : 2 * SUB, :], 0.0)
            merged[d * SUB : (d + 1) * SUB, :] = ref[d, 0:SUB, :] + tail
        cols = [merged[t * LANES : (t + 1) * LANES, :].T for t in range(tiles)]
        cols = cols[0] if tiles == 1 else jnp.concatenate(cols, axis=1)
        return pltpu.roll(cols, lon - 1, 1)

    c0 = gather(recv2.at[0])
    c1 = gather(recv2.at[1])
    cx = [gather(recvx.at[i]) for i in range(xs)]
    cu, cd = cx[0], cx[-1]
    e0 = main - LANES
    coarse = jnp.concatenate([c0, c1[0:e0]], axis=0)
    en = whole(ensf)
    wm = en * coarse * scale
    w_up = jnp.where(kk == 0, 0.0, pltpu.roll(wm, 1, 0))
    w_dn = jnp.where(kk == rows - 1, 0.0, pltpu.roll(wm, main - 1, 0))
    zz = smooth_lon(0.25 * (w_up + w_dn) + 0.5 * wm)
    for t in range(tiles):
        grad_ref[t] = zz[:, t * LANES : (t + 1) * LANES]
    for side, k, k_in in ((0, 0, 1), (1, rows - 1, rows - 2)):
        src = (cu, cd)[side]
        mine_at = e0 + side * 2 * levp
        edge_at = e0 + (1 - side) * 2 * levp
        extra = jnp.where(has[side], src[edge_at : edge_at + lev], 0.0)
        halo = c1[mine_at : mine_at + lev] + jnp.where(has[side], src[edge_at + levp : edge_at + levp + lev], 0.0)
        we = row(ensf, k) * extra * scale
        wh = edge_recv[side, 1, 0:lev, :] * halo * scale
        z_edge = smooth_lon(0.5 * we + 0.25 * wh)
        z_in = smooth_lon(0.25 * we)
        for t in range(tiles):
            cut = slice(t * LANES, (t + 1) * LANES)
            grad_ref.at[t][pl.ds(k, lev, stride=rows), :] += z_edge[:, cut]
            grad_ref.at[t][pl.ds(k_in, lev, stride=rows), :] += z_in[:, cut]

    for side in (0, 1):

        @pl.when(has[side])
        def _():
            all_of(recvx.at[0], n, ssx.at[side])

    for g in (0, 1):
        all_of(recv2.at[g], n - 1, ss2.at[g])


def writer(adv_ref, grad_ref, adv_out, grad_out, sem):
    copies = [
        pltpu.make_async_copy(grad_ref, grad_out, sem.at[0]),
        pltpu.make_async_copy(adv_ref, adv_out, sem.at[1]),
    ]
    for c in copies:
        c.start()
    for c in copies:
        c.wait()


def up_to(x, m):
    return -(-x // m) * m


def to_tiles(x):
    return x.reshape(-1, x.shape[3] // LANES, LANES).swapaxes(0, 1)


def shards(ensemble, alpha, lat_lower, lat_weight, background, obs_cell, obs_value, obs_precision):
    n, nb = lax.axis_size("mem"), lax.axis_size("band")
    members, lev, rows, lon = ensemble.shape
    fine_rows = lat_lower.shape[0]
    cells = background.shape[2]
    nobs = obs_cell.shape[1]
    fine_cols = cells // fine_rows
    scale = 1.0 / math.sqrt(members * n - 1)
    block = lon // n
    main = lev * rows
    kaps = main + 4 * RG
    assert members == 1 and block == SUB and rows == RG and lev <= RG and kaps == 2 * LANES
    assert fine_rows % RG == 0 and fine_cols % block == 0 and fine_cols // block == 3
    cfg = (n, nb, lev, rows, lon, fine_rows, fine_cols, scale)
    tiles = lon // LANES
    ng = fine_rows // RG
    gl = RG * RG
    wide = ng * gl
    gcells = RG * fine_cols
    xs = 1 if nb == 2 else 2
    dma = pltpu.SemaphoreType.DMA
    vm = pl.BlockSpec(memory_space=pltpu.VMEM)
    hbm = pl.BlockSpec(memory_space=pltpu.HBM)
    fr = 2 * SUB
    advected, gradient = pl.pallas_call(
        functools.partial(kernel, cfg),
        out_shape=(
            jax.ShapeDtypeStruct(background.shape, f32),
            jax.ShapeDtypeStruct((tiles, main, LANES), f32),
        ),
        in_specs=[hbm] * 8,
        out_specs=(vm, vm),
        scratch_shapes=[
            pltpu.VMEM((tiles, main, LANES), bf16),
            pltpu.VMEM((tiles, main, LANES), f32),
            pltpu.VMEM((1, fine_rows), jnp.int32),
            pltpu.VMEM((1, fine_rows), f32),
            pltpu.VMEM(background.shape, f32),
            pltpu.VMEM((1, nobs), jnp.int32),
            pltpu.VMEM(obs_value.shape, f32),
            pltpu.VMEM((1, nobs), f32),
            pltpu.VMEM((tiles, main, LANES), f32),
            pltpu.VMEM((tiles, main, LANES), f32),
            pltpu.VMEM((kaps, lon), f32),
            pltpu.VMEM((2, 3, RG, lon), f32),
            pltpu.VMEM((2, 3, RG, lon), f32),
            pltpu.VMEM((2, lon + SUB, LANES), f32),
            pltpu.VMEM((2, n, fr, LANES), f32),
            pltpu.VMEM((kaps, wide), bf16),
            pltpu.VMEM((kaps, wide), bf16),
            pltpu.VMEM((gl, 2 * gcells), bf16),
            pltpu.VMEM((gl, 2 * nobs), bf16),
            pltpu.VMEM((LANES, 2 * nobs), bf16),
            pltpu.VMEM((4 * SUB, wide), f32),
            pltpu.VMEM((4 * SUB, wide), f32),
            pltpu.VMEM((4 * SUB, wide), f32),
            pltpu.VMEM((2, SUB, LANES), f32),
            pltpu.VMEM((2, SUB, LANES), f32),
            pltpu.VMEM((fr, wide), f32),
            pltpu.VMEM((fr, wide), f32),
            pltpu.VMEM((4 * SUB, wide), f32),
            pltpu.VMEM((2, fr, LANES), f32),
            pltpu.VMEM((2, n, fr, LANES), f32),
            pltpu.VMEM((xs, n, fr, LANES), f32),
            pltpu.VMEM((lon, LANES), f32),
            dma((8,)),
            dma((2,)),
            dma((2,)),
            dma((2,)),
            dma((2,)),
            dma((2,)),
            dma((2,)),
            dma((2,)),
            dma((2,)),
            dma((2,)),
            dma((xs,)),
        ],
        compiler_params=pltpu.CompilerParams(collective_id=0, has_side_effects=True, vmem_limit_bytes=48 * 2**20),
    )(
        *(
            pltpu.with_memory_space_constraint(v, pltpu.HBM)
            for v in (
                to_tiles(ensemble),
                to_tiles(alpha),
                lat_lower.reshape(1, fine_rows),
                lat_weight.reshape(1, fine_rows),
                background,
                obs_cell,
                obs_value,
                obs_precision,
            )
        )
    )
    advected, gradient = pl.pallas_call(
        writer,
        out_shape=(
            jax.ShapeDtypeStruct(background.shape, f32),
            jax.ShapeDtypeStruct((tiles, main, LANES), f32),
        ),
        in_specs=[vm, vm],
        out_specs=(hbm, hbm),
        scratch_shapes=[dma((2,))],
        compiler_params=pltpu.CompilerParams(vmem_limit_bytes=2**20),
    )(advected, gradient)
    return advected, gradient.swapaxes(0, 1).reshape(members, lev, rows, lon)


def solution(mesh):
    return jax.shard_map(
        shards,
        mesh=mesh,
        in_specs=(
            P("mem", None, "band", None),
            P("mem", None, "band", None),
            P("band"),
            P("band"),
            P(None, ("band", "mem"), None),
            P(("band", "mem"), None),
            P(None, ("band", "mem"), None),
            P(("band", "mem"), None),
        ),
        out_specs=(P(None, ("band", "mem"), None), P("mem", None, "band", None)),
        check_vma=False,
    )
```

```python
import functools
import math

import jax
import jax.numpy as jnp
from jax import lax
from jax.experimental import pallas as pl
from jax.experimental.pallas import tpu as pltpu
from jax.sharding import PartitionSpec as P

advect_rate = 0.25
LANES = 128
SUB = 8
RG = 16
f32 = jnp.float32
bf16 = jnp.bfloat16


def split2(x):
    hi = x.astype(bf16)
    lo = (x - hi.astype(f32)).astype(bf16)
    return hi, lo


def split2f(x):
    hi = x.astype(bf16).astype(f32)
    return hi, x - hi


def dims(a, b, ca, cb):
    return lax.dot_general(a, b, (((ca,), (cb,)), ((), ())), preferred_element_type=f32)


def iota(shape, d):
    return lax.broadcasted_iota(jnp.int32, shape, d)


def smooth_lon(x):
    n = x.shape[1]
    return 0.25 * pltpu.roll(x, 1, 1) + 0.5 * x + 0.25 * pltpu.roll(x, n - 1, 1)


def lon_weights(ratio):
    def parts(shift):
        num = 2 * shift + 1 + ratio
        return num // (2 * ratio), (num % (2 * ratio)) / (2 * ratio)

    def taps(shift):
        q, f = parts(shift)
        w = [0.0, 0.0, 0.0]
        for at, v in ((q, 1.0 - f), (q + 1, f)):
            if v:
                w[at] += v
        return w

    value = [taps(b) for b in range(ratio)]
    slope = [[0.5 * (p - m) for p, m in zip(taps(b + 1), taps(b - 1))] for b in range(ratio)]
    return value, slope


def combine(weights, parts):
    out = None
    for w, p in zip(weights, parts):
        if w == 0.0:
            continue
        term = p if w == 1.0 else w * p
        out = term if out is None else out + term
    return out


def kernel(
    cfg,
    ens_hbm,
    alpha_hbm,
    low_hbm,
    wt_hbm,
    bg_hbm,
    cell_hbm,
    val_hbm,
    prec_hbm,
    adv_ref,
    grad_ref,
    ens_in,
    alpha,
    low,
    wt,
    bg,
    cell,
    val,
    prec,
    ensf,
    plain,
    part,
    xpart,
    edge_send,
    edge_recv,
    flat,
    frames,
    pre_recv,
    psum,
    recv1,
    eloc,
    rece,
    ecr,
    recc,
    table_hi,
    table_lo,
    zbuf,
    rbuf,
    abuf,
    fine_bg,
    obs_a,
    obs_b,
    fe_send,
    fe_recv,
    lbuf,
    gbuf,
    advbuf,
    send2,
    recv2,
    sendx,
    recvx,
    merged,
    in_sem,
    edge_ss,
    edge_rs,
    pre_ss,
    pre_rs,
    ss1,
    rs1,
    sse,
    rse,
    ssc,
    rsc,
    fe_ss,
    fe_rs,
    ss2,
    rs2,
    rs2f,
    ssx,
    rsx,
    rsxf,
):
    n, nb, lev, rows, lon, fine_rows, fine_cols, scale = cfg
    block = lon // n
    frame = block + 2
    ratio = fine_cols // block
    main = lev * rows
    tiles = lon // LANES
    ng = fine_rows // RG
    gcells = RG * fine_cols
    gl = RG * RG
    levp = RG
    xs = recvx.shape[0]
    me = lax.axis_index("mem")
    band = lax.axis_index("band")
    has_up = band > 0
    has_down = band < nb - 1
    has = (has_up, has_down)
    wv, ws = lon_weights(ratio)

    barrier = pltpu.get_barrier_semaphore()

    core = lax.rem(me, 2)
    chip = me // 2
    partner = me + 1 - 2 * core
    spread = sorted(range(n), key=lambda o: -min(o, n - o))
    for side in (0, 1):

        @pl.when(has[side])
        def _():
            for o in spread:
                pl.semaphore_signal(
                    barrier, inc=1, device_id={"mem": lax.rem(me + o, n), "band": band - 1 if side == 0 else band + 1}
                )

    for o in spread[:-1]:
        pl.semaphore_signal(barrier, inc=1, device_id={"mem": lax.rem(me + o, n)})

    loads = [
        pltpu.make_async_copy(src, dst, in_sem.at[i])
        for i, (src, dst) in enumerate(
            (
                (alpha_hbm, alpha),
                (ens_hbm, ens_in),
                (bg_hbm, bg),
                (low_hbm, low),
                (wt_hbm, wt),
                (cell_hbm, cell),
                (val_hbm, val),
                (prec_hbm, prec),
            )
        )
    ]
    for c in loads:
        c.start()

    part[main:, :] = jnp.zeros((part.shape[0] - main, lon), f32)
    xpart[...] = jnp.zeros(xpart.shape, f32)
    edge_send[...] = jnp.zeros(edge_send.shape, f32)
    fe_send[...] = jnp.zeros(fe_send.shape, f32)

    loads[0].wait()
    loads[1].wait()

    def whole(ref):
        parts = [ref[t] for t in range(tiles)]
        return parts[0] if tiles == 1 else jnp.concatenate(parts, axis=1)

    def row(ref, k):
        parts = [ref.at[t][pl.ds(k, lev, stride=rows), :] for t in range(tiles)]
        return parts[0] if tiles == 1 else jnp.concatenate(parts, axis=1)

    for t in range(tiles):
        ensf[t] = ens_in[t].astype(f32)
    al = whole(alpha)
    en = whole(ensf)
    kk = iota((main, lon), 0) % rows
    a_up = jnp.where(kk == 0, 0.0, pltpu.roll(al, 1, 0))
    a_dn = jnp.where(kk == rows - 1, 0.0, pltpu.roll(al, main - 1, 0))
    z = smooth_lon(0.25 * (a_up + a_dn) + 0.5 * al) * en * scale
    for t in range(tiles):
        plain[t] = z[:, t * LANES : (t + 1) * LANES]
    part[0:main, :] = z
    edges = []
    for side, k in ((0, 0), (1, rows - 1)):
        a_edge = smooth_lon(row(alpha, k)) * (0.25 * scale)
        e_edge = row(ensf, k)
        edges.append((a_edge, e_edge, row(plain, k)))
        edge_send[side, 0:lev, :] = e_edge
        at = main + side * 2 * levp
        part[at : at + lev, :] = a_edge
        part[at + levp : at + levp + lev, :] = e_edge
    (a_0, e_0, p_0), (a_1, e_1, p_1) = edges
    zero = jnp.zeros_like(a_0)
    sets_up = [p_0, zero, e_0, a_0]
    sets_down = [e_1, a_1, p_1, zero]
    if xs == 1:
        sets = [jnp.where(has_up, u, d) for u, d in zip(sets_up, sets_down)]
    else:
        sets = sets_up + sets_down
    for i, v in enumerate(sets):
        xpart[i * levp : i * levp + lev, :] = v

    def lay(g, rows_of):
        rows_of = pltpu.roll(rows_of, 1, 1)
        for t in range(tiles):
            flat[g, t * LANES : (t + 1) * LANES, :] = rows_of[:, t * LANES : (t + 1) * LANES].T
        flat[g, lon : lon + SUB, :] = flat[g, 0:SUB, :]

    lay(0, part[0:LANES, :])
    lay(1, part[LANES : 2 * LANES, :])
    lay(2, xpart[...])

    lane8 = iota((SUB, LANES), 1)
    row8 = iota((SUB, LANES), 0)
    low_half = lane8 < LANES // 2
    half = LANES // 2

    def tile_of(g, d):
        return flat[g, d * SUB : (d + 1) * SUB, :]

    def views(d):
        v, x = tile_of(1, d), tile_of(2, d)
        flip, flipx = pltpu.roll(v, half, 1), pltpu.roll(x, half, 1)
        return v, flip, x, flipx, pltpu.roll(flip, 5, 0), pltpu.roll(v, 3, 0), pltpu.roll(flipx, 3, 0), pltpu.roll(x, 3, 0)

    cur = views(0)
    for d in range(n):
        nxt = views(d + 1)
        v, flip, x, flipx, r5, v3, fx3, x3 = cur
        packed = jnp.where(low_half, pltpu.roll(v, 2, 0), jnp.where(row8 < 5, r5, nxt[4]))
        frames[d // 2, d % 2, 0:SUB, :] = tile_of(0, d)
        frames[d // 2, d % 2, SUB : 2 * SUB, :] = jnp.where(row8 < 2, tile_of(0, d + 1), packed)
        eloc[d] = jnp.where(low_half, flip, jnp.where(row8 < 3, v3, nxt[5]))
        ecr[0, d] = jnp.where(low_half, x, jnp.where(row8 < 3, fx3, nxt[6]))
        if xs == 2:
            ecr[1, d] = jnp.where(low_half, flipx, jnp.where(row8 < 3, x3, nxt[7]))
        cur = nxt

    if nb == 2:
        pl.semaphore_wait(barrier, 2 * n - 1)
    else:
        pl.semaphore_wait(barrier, n - 1 + n * (has_up.astype(jnp.int32) + has_down.astype(jnp.int32)))

    pre_copy = pltpu.make_async_remote_copy(
        src_ref=frames.at[:, 1 - core],
        dst_ref=pre_recv,
        send_sem=pre_ss,
        recv_sem=pre_rs,
        device_id={"mem": partner},
    )
    pre_copy.start()
    side_band = (band - 1, band + 1)
    packed_rows = frame // 2

    def copyc(side, dst):
        i = 0 if xs == 1 else 1 - side
        return pltpu.make_async_remote_copy(
            src_ref=ecr.at[0 if xs == 1 else side, dst, pl.ds(0, packed_rows), :],
            dst_ref=recc.at[i, me, pl.ds(0, packed_rows), :],
            send_sem=ssc.at[side],
            recv_sem=rsc.at[i],
            device_id={"mem": dst, "band": side_band[side]},
        )

    def copye(dst):
        return pltpu.make_async_remote_copy(
            src_ref=eloc.at[dst, pl.ds(0, packed_rows), :],
            dst_ref=rece.at[me, pl.ds(0, packed_rows), :],
            send_sem=sse,
            recv_sem=rse,
            device_id={"mem": dst},
        )

    def edge_copy(side):
        return pltpu.make_async_remote_copy(
            src_ref=edge_send.at[side],
            dst_ref=edge_recv.at[1 - side],
            send_sem=edge_ss.at[side],
            recv_sem=edge_rs.at[1 - side],
            device_id={"band": side_band[side]},
        )

    def go_round(first, go):
        def step(o, c):
            go(lax.rem(me + o, n))
            return c

        lax.fori_loop(first, n, step, 0)

    for side in (0, 1):

        @pl.when(has[side])
        def _():
            go_round(0, lambda d: copyc(side, d).start())

        @pl.when(jnp.logical_not(has[side]))
        def _():
            edge_recv[side] = jnp.zeros(edge_recv.shape[1:], f32)

    go_round(1, lambda d: copye(d).start())
    for side in (0, 1):

        @pl.when(has[side])
        def _():
            edge_copy(side).start()

    rece[me] = eloc[me]

    loads[2].wait()
    row32 = iota((4 * SUB, gcells), 0)
    col_of = jnp.where(row32 < ratio * SUB, (row32 % SUB) * ratio + row32 // SUB, -1)
    pick = (iota((4 * SUB, gcells), 1) % fine_cols == col_of).astype(f32).astype(bf16)
    pick2 = jnp.concatenate([pick, pick], axis=1)
    in_row = iota((RG, gcells), 1) // fine_cols == iota((RG, gcells), 0)
    zbuf[main:, :] = jnp.zeros((gl - main, 2 * gcells), bf16)
    back = bg[:, 0, :]
    for g in range(ng):
        hi, lo = split2f(back[:, g * gcells : (g + 1) * gcells])
        for l in range(lev):
            at = slice(l * RG, (l + 1) * RG)
            zbuf[at, 0:gcells] = jnp.where(in_row, jnp.broadcast_to(hi[l : l + 1], (RG, gcells)), 0.0).astype(bf16)
            zbuf[at, gcells : 2 * gcells] = jnp.where(in_row, jnp.broadcast_to(lo[l : l + 1], (RG, gcells)), 0.0).astype(bf16)
        fine_bg[:, g * gl : (g + 1) * gl] = dims(pick2, zbuf[...], 1, 1)
    first = fine_bg[0:1, :]
    last = fine_bg[ratio * SUB - 1 : ratio * SUB, :]
    for t in range(ng * gl // LANES):
        fe_send[0, t : t + 1, :] = first[:, t * LANES : (t + 1) * LANES]
        fe_send[1, t : t + 1, :] = last[:, t * LANES : (t + 1) * LANES]

    def fe_copy(side):
        return pltpu.make_async_remote_copy(
            src_ref=fe_send.at[side],
            dst_ref=fe_recv.at[1 - side],
            send_sem=fe_ss.at[side],
            recv_sem=fe_rs.at[1 - side],
            device_id={"mem": lax.rem(me + (n - 1 if side == 0 else 1), n)},
        )

    fe_copy(0).start()
    fe_copy(1).start()

    pre_copy.wait_recv()
    for j in range(n // 2):
        psum[j] = frames[j, core] + pre_recv[j]

    used = frame + packed_rows

    def copy1(dst):
        return pltpu.make_async_remote_copy(
            src_ref=psum.at[dst, pl.ds(0, used), :],
            dst_ref=recv1.at[chip, pl.ds(0, used), :],
            send_sem=ss1,
            recv_sem=rs1,
            device_id={"mem": 2 * dst + core},
        )

    for o in range(1, n // 2):
        copy1(lax.rem(chip + o, n // 2)).start()
    recv1[chip] = psum[chip]

    loads[3].wait()
    loads[4].wait()
    lane = iota((SUB, LANES), 1)

    def per_row(v):
        v = jnp.concatenate([v, jnp.zeros((1, LANES - fine_rows), f32)], axis=1)
        v = jnp.broadcast_to(v, (SUB, LANES))
        out = []
        for g in range(ng):
            r = v if g == 0 else pltpu.roll(v, LANES - g * RG, 1)
            r = jnp.where(lane < RG, r, 0.0)
            for s in (RG, 2 * RG, 4 * RG):
                r = r + pltpu.roll(r, s, 1)
            out += [r] * (gl // LANES)
        return jnp.concatenate(out, axis=1)[0:1]

    wide = ng * gl
    wl = per_row(wt[...])
    jl = iota((1, wide), 1) % gl
    key0 = per_row(low[...].astype(f32)) + ((jl // RG) * 64 + 1).astype(f32)
    key1 = key0 + 1.0
    w_hi, w_lo = split2f(wl)
    o_hi, o_lo = split2f(1.0 - wl)
    chunk = 2 * RG

    def table_step(i, c):
        kap = iota((chunk, 1), 0) + i * chunk
        e = kap - main
        es = e // levp
        ek = jnp.where(es == 0, -1, jnp.where(es == 1, 0, jnp.where(es == 2, rows, rows - 1)))
        l = jnp.where(e < 0, kap // rows, e % levp)
        k = jnp.where(e < 0, kap % rows, ek)
        key = jnp.where(l < lev, l * 64 + k + 1, -1).astype(f32)
        m0 = key == key0
        m1 = key == key1
        at = pl.ds(pl.multiple_of(i * chunk, chunk), chunk)
        table_hi[at, :] = jnp.where(m0, o_hi, jnp.where(m1, w_hi, 0.0)).astype(bf16)
        table_lo[at, :] = jnp.where(m0, o_lo, jnp.where(m1, w_lo, 0.0)).astype(bf16)
        return c

    lax.fori_loop(0, table_hi.shape[0] // chunk, table_step, 0)

    for i in (5, 6, 7):
        loads[i].wait()
    nobs = cell.shape[1]
    crow = cell[...] // fine_cols
    ccol = cell[...] % fine_cols
    r32 = iota((4 * SUB, nobs), 0)
    col_o = jnp.where(r32 < ratio * SUB, (r32 % SUB) * ratio + r32 // SUB, -1)
    hot = (col_o == ccol).astype(f32).astype(bf16)
    hot2 = jnp.concatenate([hot, hot], axis=1)
    pr = prec[...]
    p_hi, p_lo = split2f(pr)
    v_hi, v_lo = split2f(val[:, 0, :] * pr)
    rbuf[main:, :] = jnp.zeros((gl - main, 2 * nobs), bf16)
    for g in range(ng):
        at_row = iota((RG, nobs), 0) + g * RG == crow
        for l in range(lev):
            at = slice(l * RG, (l + 1) * RG)
            rbuf[at, 0:nobs] = jnp.where(at_row, jnp.broadcast_to(v_hi[l : l + 1], (RG, nobs)), 0.0).astype(bf16)
            rbuf[at, nobs : 2 * nobs] = jnp.where(at_row, jnp.broadcast_to(v_lo[l : l + 1], (RG, nobs)), 0.0).astype(bf16)
        obs_b[:, g * gl : (g + 1) * gl] = dims(hot2, rbuf[...], 1, 1)
        ph = jnp.where(at_row, jnp.broadcast_to(p_hi, (RG, nobs)), 0.0).astype(bf16)
        plo = jnp.where(at_row, jnp.broadcast_to(p_lo, (RG, nobs)), 0.0).astype(bf16)
        for j in range(LANES // RG):
            abuf[j * RG : (j + 1) * RG, 0:nobs] = ph
            abuf[j * RG : (j + 1) * RG, nobs : 2 * nobs] = plo
        oa = dims(hot2, abuf[...], 1, 1)
        for j in range(gl // LANES):
            obs_a[:, g * gl + j * LANES : g * gl + (j + 1) * LANES] = oa

    for side in (0, 1):
        pltpu.make_async_copy(fe_recv.at[side], fe_recv.at[side], fe_rs.at[side]).wait()
    nt = wide // LANES
    left = jnp.concatenate([fe_recv[0, t : t + 1, :] for t in range(nt)], axis=1)
    right = jnp.concatenate([fe_recv[1, t : t + 1, :] for t in range(nt)], axis=1)
    fb = [fine_bg[b * SUB : (b + 1) * SUB, :] for b in range(ratio)]
    arow = iota((SUB, wide), 0)
    before0 = jnp.where(arow == 0, left, pltpu.roll(fb[ratio - 1], 1, 0))
    after_last = jnp.where(arow == SUB - 1, right, pltpu.roll(fb[0], SUB - 1, 0))
    chain = [before0] + fb + [after_last]
    slope_bg = [0.5 * (chain[b + 2] - chain[b]) for b in range(ratio)]

    def all_of(ref, count, height, sem):
        got = ref.at[pl.ds(0, count), pl.ds(0, height), :]
        pltpu.make_async_copy(got, got, sem).wait()

    all_of(rece, n - 1, packed_rows, rse)
    for side in (0, 1):

        @pl.when(has[side])
        def _():
            i = 0 if xs == 1 else side
            all_of(recc.at[i], n, packed_rows, rsc.at[i])

    prods, plains = [], []
    for i in range(xs):
        prod = rece[0] * recc[i, 0]
        only = recc[i, 0]
        for s in range(1, n):
            prod = prod + rece[s] * recc[i, s]
            only = only + recc[i, s]
        prods.append(prod)
        plains.append(only)
    set_of = (lane8 % half) // levp
    edge_sum = jnp.where(
        set_of < 2, jnp.where(has_up, prods[0], 0.0), jnp.where(has_down, prods[-1], 0.0)
    )
    from_up = jnp.where(has_up, pltpu.roll(plains[0], LANES - 2 * levp, 1), 0.0)
    from_down = jnp.where(has_down, pltpu.roll(plains[-1], 2 * levp, 1), 0.0)
    edge_sum = edge_sum + jnp.where(set_of == 0, from_up, jnp.where(set_of == 2, from_down, 0.0))
    edge_a = pltpu.roll(edge_sum, half, 1)
    edge_b = pltpu.roll(edge_sum, 5, 0)

    all_of(recv1, n // 2 - 1, used, rs1)
    total = recv1[0]
    for s in range(1, n // 2):
        total = total + recv1[s]
    m = total[SUB:]
    m_a = pltpu.roll(m, SUB - 2, 0)
    m_b = pltpu.roll(pltpu.roll(m, half, 1), 3, 0)
    x_a = jnp.where(low_half, m_a, edge_a)
    x_b = jnp.where(low_half, m_b, edge_b)
    x = jnp.concatenate([total, jnp.concatenate([jnp.where(row8 < 5, x_a, x_b), x_b], axis=0)], axis=1)
    x_hi, x_lo = split2f(x)
    x2 = jnp.concatenate([x_hi, x_lo], axis=0).astype(bf16)
    y = dims(x2, table_hi[...], 1, 0)
    y = y[0:16] + y[16:32] + dims(x_hi.astype(bf16), table_lo[...], 1, 0)
    lbuf[...] = y
    taps = [lbuf[d : d + SUB, :] for d in range(3)]

    us, vs, moved = [], [], []
    for b in range(ratio):
        state = fb[b] + combine(wv[b], taps)
        slope = slope_bg[b] + combine(ws[b], taps)
        factor = 1.0 - advect_rate * slope
        mv = state * factor
        at = slice(b * SUB, (b + 1) * SUB)
        cot = obs_a[at, :] * mv - obs_b[at, :]
        us.append(cot * factor)
        vs.append((-advect_rate) * (state * cot))
        moved.append(mv)
    gbuf[...] = jnp.zeros(gbuf.shape, f32)
    for d in range(3):
        t = combine([wv[b][d] for b in range(ratio)] + [ws[b][d] for b in range(ratio)], us + vs)
        gbuf[d : d + SUB, :] += t
    gl_v = gbuf[...]
    g_hi, g_lo = split2f(gl_v)
    g2 = jnp.concatenate([g_hi, g_lo], axis=0).astype(bf16)
    gr = dims(g2, table_hi[...], 1, 1)
    gr = gr[0:16] + gr[16:32] + dims(g_hi.astype(bf16), table_lo[...], 1, 1)
    for g in (0, 1):
        send2[g] = gr[:, g * LANES : (g + 1) * LANES]
    v0, v1 = gr[0:SUB, LANES:], gr[SUB:, LANES:]
    sendx[...] = jnp.where(
        low_half, pltpu.roll(v0, half, 1), jnp.where(row8 < 3, pltpu.roll(v0, 3, 0), pltpu.roll(v1, 3, 0))
    )

    def slot2(src):
        return recv2.at[src, :, pl.ds(0, frame), :]

    def copy2(dst, sem):
        return pltpu.make_async_remote_copy(
            src_ref=send2.at[:, pl.ds(0, frame), :],
            dst_ref=slot2(me),
            send_sem=ss2,
            recv_sem=sem,
            device_id={"mem": dst},
        )

    def forward2(src):
        return pltpu.make_async_remote_copy(
            src_ref=slot2(src),
            dst_ref=slot2(src),
            send_sem=ss2,
            recv_sem=rs2f,
            device_id={"mem": partner},
        )

    def slotx(i, src):
        return recvx.at[i, src, pl.ds(0, packed_rows), :]

    def copyx(side, dst):
        i = 0 if xs == 1 else 1 - side
        return pltpu.make_async_remote_copy(
            src_ref=sendx.at[pl.ds(0, packed_rows), :],
            dst_ref=slotx(i, me),
            send_sem=ssx.at[side],
            recv_sem=rsx.at[i, chip],
            device_id={"mem": dst, "band": side_band[side]},
        )

    def forwardx(i, src):
        return pltpu.make_async_remote_copy(
            src_ref=slotx(i, src),
            dst_ref=slotx(i, src),
            send_sem=ssx.at[2 + i],
            recv_sem=rsxf.at[i],
            device_id={"mem": partner},
        )

    for side in (0, 1):

        @pl.when(has[side])
        def _():
            for o in range(0, n, 2):
                copyx(side, lax.rem(me + o, n)).start()

    for o in range(2, n, 2):
        copy2(lax.rem(me + o, n), rs2.at[chip]).start()
    copy2(partner, rs2f).start()
    for g in (0, 1):
        recv2[me, g] = send2[g]

    advbuf[...] = jnp.concatenate(moved + [jnp.zeros((SUB, wide), f32)], axis=0)
    pickt = jnp.concatenate([pick, pick], axis=0)
    for g in range(ng):
        hi, lo = split2(advbuf[:, g * gl : g * gl + main])
        e = dims(jnp.concatenate([hi, lo], axis=0), pickt, 0, 0)
        for l in range(lev):
            v = jnp.where(in_row, e[l * RG : (l + 1) * RG], 0.0)
            adv_ref[l, :, g * gcells : (g + 1) * gcells] = jnp.sum(v, axis=0, keepdims=True)

    def sent_edges():
        pre_copy.wait_send()
        all_of(rece, n - 1, packed_rows, sse)
        all_of(recv1, n // 2 - 1, used, ss1)
        for side in (0, 1):
            fe_copy(side).wait_send()

            @pl.when(has[side])
            def _():
                all_of(recc.at[0], n, packed_rows, ssc.at[side])
                edge_copy(side).wait_send()
                pltpu.make_async_copy(edge_recv.at[side], edge_recv.at[side], edge_rs.at[side]).wait()

    sent_edges()
    for o in sorted(range(2, n, 2), key=lambda o: min(o, n - o)):
        src = lax.rem(me + o, n)
        pltpu.make_async_copy(slot2(src), slot2(src), rs2.at[src // 2]).wait()
        forward2(src).start()
    for side in (0, 1):

        @pl.when(has[side])
        def _():
            i = 0 if xs == 1 else side
            for o in sorted(range(0, n, 2), key=lambda o: min(o, n - o)):
                src = lax.rem(me + o, n)
                pltpu.make_async_copy(slotx(i, src), slotx(i, src), rsx.at[i, src // 2]).wait()
                forwardx(i, src).start()

    def all_2(count, sem):
        got = recv2.at[pl.ds(0, count), :, pl.ds(0, frame), :]
        pltpu.make_async_copy(got, got, sem).wait()

    for side in (0, 1):

        @pl.when(has[side])
        def _():
            i = 0 if xs == 1 else side
            all_of(recvx.at[i], n // 2, packed_rows, rsxf.at[i])

    all_2(n // 2, rs2f)

    over = iota((SUB, LANES), 0) < frame - block

    def across(ref):
        cols = [ref[t * LANES : (t + 1) * LANES, :].T for t in range(tiles)]
        cols = cols[0] if tiles == 1 else jnp.concatenate(cols, axis=1)
        return pltpu.roll(cols, lon - 1, 1)

    def gather(g):
        for d in range(n):
            tail = jnp.where(over, recv2[(d - 1) % n, g, SUB : 2 * SUB, :], 0.0)
            merged[d * SUB : (d + 1) * SUB, :] = recv2[d, g, 0:SUB, :] + tail
        return across(merged)

    def gather_edges(i):
        prev = pltpu.roll(pltpu.roll(recvx[i, n - 1], half, 1), 5, 0)
        for d in range(n):
            e = recvx[i, d]
            b = pltpu.roll(pltpu.roll(e, half, 1), 5, 0)
            merged[d * SUB : (d + 1) * SUB, :] = jnp.where(row8 < 5, e, b) + jnp.where(over, prev, 0.0)
            prev = b
        return across(merged)

    c0 = gather(0)
    c1 = gather(1)
    cx = [gather_edges(i) for i in range(xs)]
    cu, cd = cx[0], cx[-1]
    e0 = main - LANES
    coarse = jnp.concatenate([c0, c1[0:e0]], axis=0)
    en = whole(ensf)
    wm = en * coarse * scale
    w_up = jnp.where(kk == 0, 0.0, pltpu.roll(wm, 1, 0))
    w_dn = jnp.where(kk == rows - 1, 0.0, pltpu.roll(wm, main - 1, 0))
    zz = smooth_lon(0.25 * (w_up + w_dn) + 0.5 * wm)
    for t in range(tiles):
        grad_ref[t] = zz[:, t * LANES : (t + 1) * LANES]
    for side, k, k_in in ((0, 0, 1), (1, rows - 1, rows - 2)):
        src = (cu, cd)[side]
        mine_at = e0 + side * 2 * levp
        edge_at = (1 - side) * 2 * levp
        extra = jnp.where(has[side], src[edge_at : edge_at + lev], 0.0)
        halo = c1[mine_at : mine_at + lev] + jnp.where(has[side], src[edge_at + levp : edge_at + levp + lev], 0.0)
        we = row(ensf, k) * extra * scale
        wh = edge_recv[side, 0:lev, :] * halo * scale
        z_edge = smooth_lon(0.5 * we + 0.25 * wh)
        z_in = smooth_lon(0.25 * we)
        for t in range(tiles):
            cut = slice(t * LANES, (t + 1) * LANES)
            grad_ref.at[t][pl.ds(k, lev, stride=rows), :] += z_edge[:, cut]
            grad_ref.at[t][pl.ds(k_in, lev, stride=rows), :] += z_in[:, cut]

    for side in (0, 1):

        @pl.when(has[side])
        def _():
            i = 0 if xs == 1 else side
            all_of(recvx.at[0], n // 2, packed_rows, ssx.at[side])
            all_of(recvx.at[0], n // 2, packed_rows, ssx.at[2 + i])

    all_2(n - 1, ss2)


def writer(adv_ref, grad_ref, adv_out, grad_out, sem):
    copies = [
        pltpu.make_async_copy(grad_ref, grad_out, sem.at[0]),
        pltpu.make_async_copy(adv_ref, adv_out, sem.at[1]),
    ]
    for c in copies:
        c.start()
    for c in copies:
        c.wait()


def up_to(x, m):
    return -(-x // m) * m


def to_tiles(x):
    return x.reshape(-1, x.shape[3] // LANES, LANES).swapaxes(0, 1)


def shards(ensemble, alpha, lat_lower, lat_weight, background, obs_cell, obs_value, obs_precision):
    n, nb = lax.axis_size("mem"), lax.axis_size("band")
    members, lev, rows, lon = ensemble.shape
    fine_rows = lat_lower.shape[0]
    cells = background.shape[2]
    nobs = obs_cell.shape[1]
    fine_cols = cells // fine_rows
    scale = 1.0 / math.sqrt(members * n - 1)
    block = lon // n
    main = lev * rows
    kaps = main + 4 * RG
    assert n % 2 == 0 and members == 1 and block == SUB and rows == RG and lev <= RG and kaps == 2 * LANES
    assert fine_rows % RG == 0 and fine_cols % block == 0 and fine_cols // block == 3
    cfg = (n, nb, lev, rows, lon, fine_rows, fine_cols, scale)
    tiles = lon // LANES
    ng = fine_rows // RG
    gl = RG * RG
    wide = ng * gl
    gcells = RG * fine_cols
    xs = 1 if nb == 2 else 2
    dma = pltpu.SemaphoreType.DMA
    vm = pl.BlockSpec(memory_space=pltpu.VMEM)
    hbm = pl.BlockSpec(memory_space=pltpu.HBM)
    fr = 2 * SUB
    advected, gradient = pl.pallas_call(
        functools.partial(kernel, cfg),
        out_shape=(
            jax.ShapeDtypeStruct(background.shape, f32),
            jax.ShapeDtypeStruct((tiles, main, LANES), f32),
        ),
        in_specs=[hbm] * 8,
        out_specs=(vm, vm),
        scratch_shapes=[
            pltpu.VMEM((tiles, main, LANES), bf16),
            pltpu.VMEM((tiles, main, LANES), f32),
            pltpu.VMEM((1, fine_rows), jnp.int32),
            pltpu.VMEM((1, fine_rows), f32),
            pltpu.VMEM(background.shape, f32),
            pltpu.VMEM((1, nobs), jnp.int32),
            pltpu.VMEM(obs_value.shape, f32),
            pltpu.VMEM((1, nobs), f32),
            pltpu.VMEM((tiles, main, LANES), f32),
            pltpu.VMEM((tiles, main, LANES), f32),
            pltpu.VMEM((kaps, lon), f32),
            pltpu.VMEM((LANES, lon), f32),
            pltpu.VMEM((2, RG, lon), f32),
            pltpu.VMEM((2, RG, lon), f32),
            pltpu.VMEM((3, lon + SUB, LANES), f32),
            pltpu.VMEM((n // 2, 2, fr, LANES), f32),
            pltpu.VMEM((n // 2, fr, LANES), f32),
            pltpu.VMEM((n // 2, fr, LANES), f32),
            pltpu.VMEM((n // 2, fr, LANES), f32),
            pltpu.VMEM((n, SUB, LANES), f32),
            pltpu.VMEM((n, SUB, LANES), f32),
            pltpu.VMEM((xs, n, SUB, LANES), f32),
            pltpu.VMEM((xs, n, SUB, LANES), f32),
            pltpu.VMEM((kaps, wide), bf16),
            pltpu.VMEM((kaps, wide), bf16),
            pltpu.VMEM((gl, 2 * gcells), bf16),
            pltpu.VMEM((gl, 2 * nobs), bf16),
            pltpu.VMEM((LANES, 2 * nobs), bf16),
            pltpu.VMEM((4 * SUB, wide), f32),
            pltpu.VMEM((4 * SUB, wide), f32),
            pltpu.VMEM((4 * SUB, wide), f32),
            pltpu.VMEM((2, SUB, LANES), f32),
            pltpu.VMEM((2, SUB, LANES), f32),
            pltpu.VMEM((fr, wide), f32),
            pltpu.VMEM((fr, wide), f32),
            pltpu.VMEM((4 * SUB, wide), f32),
            pltpu.VMEM((2, fr, LANES), f32),
            pltpu.VMEM((n, 2, fr, LANES), f32),
            pltpu.VMEM((SUB, LANES), f32),
            pltpu.VMEM((xs, n, SUB, LANES), f32),
            pltpu.VMEM((lon, LANES), f32),
            dma((8,)),
            dma((2,)),
            dma((2,)),
            dma,
            dma,
            dma,
            dma,
            dma,
            dma,
            dma((2,)),
            dma((xs,)),
            dma((2,)),
            dma((2,)),
            dma,
            dma((n // 2,)),
            dma,
            dma((4,)),
            dma((xs, n // 2)),
            dma((xs,)),
        ],
        compiler_params=pltpu.CompilerParams(collective_id=0, has_side_effects=True, vmem_limit_bytes=48 * 2**20),
    )(
        *(
            pltpu.with_memory_space_constraint(v, pltpu.HBM)
            for v in (
                to_tiles(ensemble),
                to_tiles(alpha),
                lat_lower.reshape(1, fine_rows),
                lat_weight.reshape(1, fine_rows),
                background,
                obs_cell,
                obs_value,
                obs_precision,
            )
        )
    )
    advected, gradient = pl.pallas_call(
        writer,
        out_shape=(
            jax.ShapeDtypeStruct(background.shape, f32),
            jax.ShapeDtypeStruct((tiles, main, LANES), f32),
        ),
        in_specs=[vm, vm],
        out_specs=(hbm, hbm),
        scratch_shapes=[dma((2,))],
        compiler_params=pltpu.CompilerParams(vmem_limit_bytes=2**20),
    )(advected, gradient)
    return advected, gradient.swapaxes(0, 1).reshape(members, lev, rows, lon)


def solution(mesh):
    return jax.shard_map(
        shards,
        mesh=mesh,
        in_specs=(
            P("mem", None, "band", None),
            P("mem", None, "band", None),
            P("band"),
            P("band"),
            P(None, ("band", "mem"), None),
            P(("band", "mem"), None),
            P(None, ("band", "mem"), None),
            P(("band", "mem"), None),
        ),
        out_specs=(P(None, ("band", "mem"), None), P("mem", None, "band", None)),
        check_vma=False,
    )
```

```python
import functools
import math

import jax
import jax.numpy as jnp
from jax import lax
from jax.experimental import pallas as pl
from jax.experimental.pallas import tpu as pltpu
from jax.sharding import PartitionSpec as P

advect_rate = 0.25
LANES = 128
SUB = 8
RG = 16
f32 = jnp.float32
bf16 = jnp.bfloat16


def split2(x):
    hi = x.astype(bf16)
    lo = (x - hi.astype(f32)).astype(bf16)
    return hi, lo


def split2f(x):
    hi = x.astype(bf16).astype(f32)
    return hi, x - hi


def dims(a, b, ca, cb):
    return lax.dot_general(a, b, (((ca,), (cb,)), ((), ())), preferred_element_type=f32)


def iota(shape, d):
    return lax.broadcasted_iota(jnp.int32, shape, d)


def smooth_lon(x):
    n = x.shape[1]
    return 0.25 * pltpu.roll(x, 1, 1) + 0.5 * x + 0.25 * pltpu.roll(x, n - 1, 1)


def lon_weights(ratio):
    def parts(shift):
        num = 2 * shift + 1 + ratio
        return num // (2 * ratio), (num % (2 * ratio)) / (2 * ratio)

    def taps(shift):
        q, f = parts(shift)
        w = [0.0, 0.0, 0.0]
        for at, v in ((q, 1.0 - f), (q + 1, f)):
            if v:
                w[at] += v
        return w

    value = [taps(b) for b in range(ratio)]
    slope = [[0.5 * (p - m) for p, m in zip(taps(b + 1), taps(b - 1))] for b in range(ratio)]
    return value, slope


def combine(weights, parts):
    out = None
    for w, p in zip(weights, parts):
        if w == 0.0:
            continue
        term = p if w == 1.0 else w * p
        out = term if out is None else out + term
    return out


def kernel(
    cfg,
    ens_hbm,
    alpha_hbm,
    low_hbm,
    wt_hbm,
    bg_hbm,
    cell_hbm,
    val_hbm,
    prec_hbm,
    adv_ref,
    grad_ref,
    ens_in,
    alpha,
    low,
    wt,
    bg,
    cell,
    val,
    prec,
    ensf,
    plain,
    part,
    xpart,
    edge_send,
    edge_recv,
    flat,
    frames,
    pre_recv,
    psum,
    recv1,
    eloc,
    rece,
    ecr,
    recc,
    table_hi,
    table_lo,
    back_hi,
    back_lo,
    zbuf,
    rbuf,
    abuf,
    fine_bg,
    obs_a,
    obs_b,
    fe_send,
    fe_recv,
    lbuf,
    gbuf,
    advbuf,
    send2,
    recv2,
    sendx,
    recvx,
    merged,
    in_sem,
    edge_rs,
    pre_rs,
    rs1,
    rse,
    rsc,
    fe_rs,
    ss2,
    rs2,
    rs2f,
    ssx,
    rsx,
    rsxf,
):
    n, nb, lev, rows, lon, fine_rows, fine_cols, scale = cfg
    block = lon // n
    frame = block + 2
    ratio = fine_cols // block
    main = lev * rows
    tiles = lon // LANES
    ng = fine_rows // RG
    gcells = RG * fine_cols
    gl = RG * RG
    levp = RG
    xs = recvx.shape[0]
    me = lax.axis_index("mem")
    band = lax.axis_index("band")
    has_up = band > 0
    has_down = band < nb - 1
    has = (has_up, has_down)
    wv, ws = lon_weights(ratio)

    barrier = pltpu.get_barrier_semaphore()

    core = lax.rem(me, 2)
    chip = me // 2
    partner = me + 1 - 2 * core
    spread = sorted(range(n), key=lambda o: -min(o, n - o))
    side_band = (band - 1, band + 1)
    for o in spread:
        if nb == 2:
            pl.semaphore_signal(barrier, inc=1, device_id={"mem": lax.rem(me + o, n), "band": 1 - band})
        else:
            for side in (0, 1):

                @pl.when(has[side])
                def _():
                    pl.semaphore_signal(barrier, inc=1, device_id={"mem": lax.rem(me + o, n), "band": side_band[side]})

        if o:
            pl.semaphore_signal(barrier, inc=1, device_id={"mem": lax.rem(me + o, n)})

    loads = [
        pltpu.make_async_copy(src, dst, in_sem.at[i])
        for i, (src, dst) in enumerate(
            (
                (alpha_hbm, alpha),
                (ens_hbm, ens_in),
                (bg_hbm, bg),
                (low_hbm, low),
                (wt_hbm, wt),
                (cell_hbm, cell),
                (val_hbm, val),
                (prec_hbm, prec),
            )
        )
    ]
    for c in loads:
        c.start()

    part[main:, :] = jnp.zeros((part.shape[0] - main, lon), f32)
    xpart[...] = jnp.zeros(xpart.shape, f32)
    edge_send[...] = jnp.zeros(edge_send.shape, f32)
    fe_send[...] = jnp.zeros(fe_send.shape, f32)

    loads[0].wait()
    loads[1].wait()

    def whole(ref):
        parts = [ref[t] for t in range(tiles)]
        return parts[0] if tiles == 1 else jnp.concatenate(parts, axis=1)

    def row(ref, k):
        parts = [ref.at[t][pl.ds(k, lev, stride=rows), :] for t in range(tiles)]
        return parts[0] if tiles == 1 else jnp.concatenate(parts, axis=1)

    for t in range(tiles):
        ensf[t] = ens_in[t].astype(f32)
    al = whole(alpha)
    en = whole(ensf)
    kk = iota((main, lon), 0) % rows
    a_up = jnp.where(kk == 0, 0.0, pltpu.roll(al, 1, 0))
    a_dn = jnp.where(kk == rows - 1, 0.0, pltpu.roll(al, main - 1, 0))
    z = smooth_lon(0.25 * (a_up + a_dn) + 0.5 * al) * en * scale
    for t in range(tiles):
        plain[t] = z[:, t * LANES : (t + 1) * LANES]
    part[0:main, :] = z
    edges = []
    for side, k in ((0, 0), (1, rows - 1)):
        a_edge = smooth_lon(row(alpha, k)) * (0.25 * scale)
        e_edge = row(ensf, k)
        edges.append((a_edge, e_edge, row(plain, k)))
        edge_send[side, 0:lev, :] = e_edge
        at = main + side * 2 * levp
        part[at : at + lev, :] = a_edge
        part[at + levp : at + levp + lev, :] = e_edge
    (a_0, e_0, p_0), (a_1, e_1, p_1) = edges
    zero = jnp.zeros_like(a_0)
    sets_up = [p_0, zero, e_0, a_0]
    sets_down = [e_1, a_1, p_1, zero]
    if xs == 1:
        sets = [jnp.where(has_up, u, d) for u, d in zip(sets_up, sets_down)]
    else:
        sets = sets_up + sets_down
    for i, v in enumerate(sets):
        xpart[i * levp : i * levp + lev, :] = v

    def lay(g, rows_of):
        rows_of = pltpu.roll(rows_of, 1, 1)
        for t in range(tiles):
            flat[g, t * LANES : (t + 1) * LANES, :] = rows_of[:, t * LANES : (t + 1) * LANES].T
        flat[g, lon : lon + SUB, :] = flat[g, 0:SUB, :]

    lay(0, part[0:LANES, :])
    lay(1, part[LANES : 2 * LANES, :])
    lay(2, xpart[...])

    lane8 = iota((SUB, LANES), 1)
    row8 = iota((SUB, LANES), 0)
    low_half = lane8 < LANES // 2
    half = LANES // 2

    def tile_of(g, d):
        return flat[g, d * SUB : (d + 1) * SUB, :]

    def views(d):
        v, x = tile_of(1, d), tile_of(2, d)
        flip, flipx = pltpu.roll(v, half, 1), pltpu.roll(x, half, 1)
        return v, flip, x, flipx, pltpu.roll(flip, 5, 0), pltpu.roll(v, 3, 0), pltpu.roll(flipx, 3, 0), pltpu.roll(x, 3, 0)

    cur = views(0)
    for d in range(n):
        nxt = views(d + 1)
        v, flip, x, flipx, r5, v3, fx3, x3 = cur
        packed = jnp.where(low_half, pltpu.roll(v, 2, 0), jnp.where(row8 < 5, r5, nxt[4]))
        frames[d // 2, d % 2, 0:SUB, :] = tile_of(0, d)
        frames[d // 2, d % 2, SUB : 2 * SUB, :] = jnp.where(row8 < 2, tile_of(0, d + 1), packed)
        eloc[d] = jnp.where(low_half, flip, jnp.where(row8 < 3, v3, nxt[5]))
        ecr[0, d] = jnp.where(low_half, x, jnp.where(row8 < 3, fx3, nxt[6]))
        if xs == 2:
            ecr[1, d] = jnp.where(low_half, flipx, jnp.where(row8 < 3, x3, nxt[7]))
        cur = nxt

    loads[2].wait()
    row32 = iota((4 * SUB, gcells), 0)
    col_of = jnp.where(row32 < ratio * SUB, (row32 % SUB) * ratio + row32 // SUB, -1)
    pick = (iota((4 * SUB, gcells), 1) % fine_cols == col_of).astype(f32).astype(bf16)
    pick2 = jnp.concatenate([pick, pick], axis=1)
    in_row = iota((RG, gcells), 1) // fine_cols == iota((RG, gcells), 0)
    zbuf[main:, :] = jnp.zeros((gl - main, 2 * gcells), bf16)
    back = bg[:, 0, :]
    for g in range(ng):
        hi, lo = split2f(back[:, g * gcells : (g + 1) * gcells])
        for l in range(lev):
            at = slice(l * RG, (l + 1) * RG)
            zbuf[at, 0:gcells] = jnp.where(in_row, jnp.broadcast_to(hi[l : l + 1], (RG, gcells)), 0.0).astype(bf16)
            zbuf[at, gcells : 2 * gcells] = jnp.where(in_row, jnp.broadcast_to(lo[l : l + 1], (RG, gcells)), 0.0).astype(bf16)
        fine_bg[:, g * gl : (g + 1) * gl] = dims(pick2, zbuf[...], 1, 1)
    for c in loads[3:]:
        c.wait()

    if nb == 2:
        pl.semaphore_wait(barrier, 2 * n - 1)
    else:
        pl.semaphore_wait(barrier, n - 1 + n * (has_up.astype(jnp.int32) + has_down.astype(jnp.int32)))

    pre_copy = pltpu.make_async_remote_copy(
        src_ref=frames.at[:, 1 - core],
        dst_ref=pre_recv,
        send_sem=in_sem.at[0],
        recv_sem=pre_rs,
        device_id={"mem": partner},
    )
    pre_copy.start()
    packed_rows = frame // 2

    def copyc(side, dst):
        i = 0 if xs == 1 else 1 - side
        return pltpu.make_async_remote_copy(
            src_ref=ecr.at[0 if xs == 1 else side, dst, pl.ds(0, packed_rows), :],
            dst_ref=recc.at[i, me, pl.ds(0, packed_rows), :],
            send_sem=in_sem.at[2 + side],
            recv_sem=rsc.at[i],
            device_id={"mem": dst, "band": side_band[side]},
        )

    def copye(dst):
        return pltpu.make_async_remote_copy(
            src_ref=eloc.at[dst, pl.ds(0, packed_rows), :],
            dst_ref=rece.at[me, pl.ds(0, packed_rows), :],
            send_sem=in_sem.at[1],
            recv_sem=rse,
            device_id={"mem": dst},
        )

    def edge_copy(side):
        return pltpu.make_async_remote_copy(
            src_ref=edge_send.at[side],
            dst_ref=edge_recv.at[1 - side],
            send_sem=in_sem.at[6 + side],
            recv_sem=edge_rs.at[0 if xs == 1 else 1 - side],
            device_id={"band": side_band[side]},
        )

    def go_round(first, go):
        def step(o, c):
            go(lax.rem(me + o, n))
            return c

        lax.fori_loop(first, n, step, 0)

    for side in (0, 1):

        @pl.when(has[side])
        def _():
            go_round(0, lambda d: copyc(side, d).start())

        @pl.when(jnp.logical_not(has[side]))
        def _():
            edge_recv[side] = jnp.zeros(edge_recv.shape[1:], f32)

    go_round(1, lambda d: copye(d).start())
    for side in (0, 1):

        @pl.when(has[side])
        def _():
            edge_copy(side).start()

    rece[me] = eloc[me]

    first = fine_bg[0:1, :]
    last = fine_bg[ratio * SUB - 1 : ratio * SUB, :]
    for t in range(ng * gl // LANES):
        fe_send[0, t : t + 1, :] = first[:, t * LANES : (t + 1) * LANES]
        fe_send[1, t : t + 1, :] = last[:, t * LANES : (t + 1) * LANES]

    def fe_copy(side):
        return pltpu.make_async_remote_copy(
            src_ref=fe_send.at[side],
            dst_ref=fe_recv.at[1 - side],
            send_sem=in_sem.at[5],
            recv_sem=fe_rs,
            device_id={"mem": lax.rem(me + (n - 1 if side == 0 else 1), n)},
        )

    fe_copy(0).start()
    fe_copy(1).start()

    lane = iota((SUB, LANES), 1)
    wide = ng * gl

    def per_row(v):
        v = jnp.concatenate([v, jnp.zeros((1, LANES - fine_rows), f32)], axis=1)
        return jnp.broadcast_to(v, (SUB, LANES))

    def tiled(v, g):
        r = v if g == 0 else pltpu.roll(v, LANES - g * RG, 1)
        r = jnp.where(lane < RG, r, 0.0)
        for s in (RG, 2 * RG, 4 * RG):
            r = r + pltpu.roll(r, s, 1)
        return jnp.concatenate([r, r], axis=0)

    low_rows, wt_rows = per_row(low[...].astype(f32)), per_row(wt[...])
    down = lambda v: jnp.concatenate([v] * (LANES // SUB), axis=0).T
    low_col, wt_col = down(low_rows), down(wt_rows)
    lane16 = iota((RG, LANES), 1)
    row16 = iota((RG, LANES), 0)
    lev_of = lane16 // RG
    set_rows = (-1, 0, rows, rows - 1)
    table_hi[...] = jnp.zeros(table_hi.shape, bf16)
    table_lo[...] = jnp.zeros(table_lo.shape, bf16)
    back_hi[...] = jnp.zeros(back_hi.shape, bf16)
    back_lo[...] = jnp.zeros(back_lo.shape, bf16)
    halves = gl // LANES
    per = LANES // RG

    def weigh(k, lo_k, w):
        w_hi, w_lo = split2f(w)
        o_hi, o_lo = split2f(1.0 - w)
        m0, m1 = k == lo_k, k == lo_k + 1.0
        return (
            jnp.where(m0, o_hi, jnp.where(m1, w_hi, 0.0)),
            jnp.where(m0, o_lo, jnp.where(m1, w_lo, 0.0)),
        )

    def put(ref, r, c, v, keep):
        ref[r : r + RG, c : c + LANES] = jnp.where(keep, v, 0.0).astype(bf16)

    for g in range(ng):
        lo_t, w_t = tiled(low_rows, g), tiled(wt_rows, g)
        main_t = weigh(row16.astype(f32), lo_t, w_t)
        set_t = [weigh(jnp.full((RG, LANES), float(k), f32), lo_t, w_t) for k in set_rows]
        for ref, which in ((table_hi, 0), (table_lo, 1)):
            for l in range(lev):
                put(ref, l * RG, g * gl + l // per * LANES, main_t[which], lev_of == l % per)
            for s in range(4):
                for h in range(halves):
                    put(ref, main + s * levp, g * gl + h * LANES, set_t[s][which], (row16 == lev_of + h * per) & (row16 < lev))
        lo_c, w_c = low_col[g * RG : (g + 1) * RG], wt_col[g * RG : (g + 1) * RG]
        for h in range(halves):
            kap = lane16 + h * LANES
            e = kap - main
            es = e // levp
            ek = jnp.where(es == 0, -1, jnp.where(es == 1, 0, jnp.where(es == 2, rows, rows - 1)))
            k_of = jnp.where(e < 0, kap % rows, ek).astype(f32)
            l_of = jnp.where(e < 0, kap // rows, e % levp)
            back_t = weigh(k_of, lo_c, w_c)
            for ref, which in ((back_hi, 0), (back_lo, 1)):
                for l in range(lev):
                    if (h + 1) * LANES > main or l // per == h:
                        put(ref, g * gl + l * RG, h * LANES, back_t[which], l_of == l)

    pre_copy.wait_recv()
    for j in range(n // 2):
        psum[j] = frames[j, core] + pre_recv[j]

    used = frame + packed_rows

    def copy1(dst):
        return pltpu.make_async_remote_copy(
            src_ref=psum.at[dst, pl.ds(0, used), :],
            dst_ref=recv1.at[chip, pl.ds(0, used), :],
            send_sem=in_sem.at[4],
            recv_sem=rs1,
            device_id={"mem": 2 * dst + core},
        )

    for o in range(1, n // 2):
        copy1(lax.rem(chip + o, n // 2)).start()
    recv1[chip] = psum[chip]

    nobs = cell.shape[1]
    crow = cell[...] // fine_cols
    ccol = cell[...] % fine_cols
    r32 = iota((4 * SUB, nobs), 0)
    col_o = jnp.where(r32 < ratio * SUB, (r32 % SUB) * ratio + r32 // SUB, -1)
    hot = (col_o == ccol).astype(f32).astype(bf16)
    hot2 = jnp.concatenate([hot, hot], axis=1)
    pr = prec[...]
    p_hi, p_lo = split2f(pr)
    v_hi, v_lo = split2f(val[:, 0, :] * pr)
    rbuf[main:, :] = jnp.zeros((gl - main, 2 * nobs), bf16)
    for g in range(ng):
        at_row = iota((RG, nobs), 0) + g * RG == crow
        for l in range(lev):
            at = slice(l * RG, (l + 1) * RG)
            rbuf[at, 0:nobs] = jnp.where(at_row, jnp.broadcast_to(v_hi[l : l + 1], (RG, nobs)), 0.0).astype(bf16)
            rbuf[at, nobs : 2 * nobs] = jnp.where(at_row, jnp.broadcast_to(v_lo[l : l + 1], (RG, nobs)), 0.0).astype(bf16)
        obs_b[:, g * gl : (g + 1) * gl] = dims(hot2, rbuf[...], 1, 1)
        ph = jnp.where(at_row, jnp.broadcast_to(p_hi, (RG, nobs)), 0.0).astype(bf16)
        plo = jnp.where(at_row, jnp.broadcast_to(p_lo, (RG, nobs)), 0.0).astype(bf16)
        for j in range(LANES // RG):
            abuf[j * RG : (j + 1) * RG, 0:nobs] = ph
            abuf[j * RG : (j + 1) * RG, nobs : 2 * nobs] = plo
        oa = dims(hot2, abuf[...], 1, 1)
        for j in range(gl // LANES):
            obs_a[:, g * gl + j * LANES : g * gl + (j + 1) * LANES] = oa

    pltpu.make_async_copy(fe_recv, fe_recv, fe_rs).wait()
    nt = wide // LANES
    left = jnp.concatenate([fe_recv[0, t : t + 1, :] for t in range(nt)], axis=1)
    right = jnp.concatenate([fe_recv[1, t : t + 1, :] for t in range(nt)], axis=1)
    fb = [fine_bg[b * SUB : (b + 1) * SUB, :] for b in range(ratio)]
    arow = iota((SUB, wide), 0)
    before0 = jnp.where(arow == 0, left, pltpu.roll(fb[ratio - 1], 1, 0))
    after_last = jnp.where(arow == SUB - 1, right, pltpu.roll(fb[0], SUB - 1, 0))
    chain = [before0] + fb + [after_last]
    slope_bg = [0.5 * (chain[b + 2] - chain[b]) for b in range(ratio)]

    def all_of(ref, count, height, sem):
        got = ref.at[pl.ds(0, count), pl.ds(0, height), :]
        pltpu.make_async_copy(got, got, sem).wait()

    all_of(rece, n - 1, packed_rows, rse)
    for side in (0, 1):

        @pl.when(has[side])
        def _():
            i = 0 if xs == 1 else side
            all_of(recc.at[i], n, packed_rows, rsc.at[i])

    prods, plains = [], []
    for i in range(xs):
        prod = rece[0] * recc[i, 0]
        only = recc[i, 0]
        for s in range(1, n):
            prod = prod + rece[s] * recc[i, s]
            only = only + recc[i, s]
        prods.append(prod)
        plains.append(only)
    set_of = (lane8 % half) // levp
    edge_sum = jnp.where(
        set_of < 2, jnp.where(has_up, prods[0], 0.0), jnp.where(has_down, prods[-1], 0.0)
    )
    from_up = jnp.where(has_up, pltpu.roll(plains[0], LANES - 2 * levp, 1), 0.0)
    from_down = jnp.where(has_down, pltpu.roll(plains[-1], 2 * levp, 1), 0.0)
    edge_sum = edge_sum + jnp.where(set_of == 0, from_up, jnp.where(set_of == 2, from_down, 0.0))
    edge_a = pltpu.roll(edge_sum, half, 1)
    edge_b = pltpu.roll(edge_sum, 5, 0)

    all_of(recv1, n // 2 - 1, used, rs1)
    total = recv1[0]
    for s in range(1, n // 2):
        total = total + recv1[s]
    m = total[SUB:]
    m_a = pltpu.roll(m, SUB - 2, 0)
    m_b = pltpu.roll(pltpu.roll(m, half, 1), 3, 0)
    x_a = jnp.where(low_half, m_a, edge_a)
    x_b = jnp.where(low_half, m_b, edge_b)
    x = jnp.concatenate([total, jnp.concatenate([jnp.where(row8 < 5, x_a, x_b), x_b], axis=0)], axis=1)
    x_hi, x_lo = split2f(x)
    x2 = jnp.concatenate([x_hi, x_lo], axis=0).astype(bf16)
    y = dims(x2, table_hi[...], 1, 0)
    y = y[0:16] + y[16:32] + dims(x_hi.astype(bf16), table_lo[...], 1, 0)
    lbuf[...] = y
    taps = [lbuf[d : d + SUB, :] for d in range(3)]

    us, vs, moved = [], [], []
    for b in range(ratio):
        state = fb[b] + combine(wv[b], taps)
        slope = slope_bg[b] + combine(ws[b], taps)
        factor = 1.0 - advect_rate * slope
        mv = state * factor
        at = slice(b * SUB, (b + 1) * SUB)
        cot = obs_a[at, :] * mv - obs_b[at, :]
        us.append(cot * factor)
        vs.append((-advect_rate) * (state * cot))
        moved.append(mv)
    gbuf[...] = jnp.zeros(gbuf.shape, f32)
    for d in range(3):
        t = combine([wv[b][d] for b in range(ratio)] + [ws[b][d] for b in range(ratio)], us + vs)
        gbuf[d : d + SUB, :] += t
    gl_v = gbuf[...]
    g_hi, g_lo = split2f(gl_v)
    g2 = jnp.concatenate([g_hi, g_lo], axis=0).astype(bf16)
    gr = dims(g2, back_hi[...], 1, 0)
    gr = gr[0:16] + gr[16:32] + dims(g_hi.astype(bf16), back_lo[...], 1, 0)
    for g in (0, 1):
        send2[g] = gr[:, g * LANES : (g + 1) * LANES]
    v0, v1 = gr[0:SUB, LANES:], gr[SUB:, LANES:]
    sendx[...] = jnp.where(
        low_half, pltpu.roll(v0, half, 1), jnp.where(row8 < 3, pltpu.roll(v0, 3, 0), pltpu.roll(v1, 3, 0))
    )

    def slot2(src):
        return recv2.at[src, :, pl.ds(0, frame), :]

    def copy2(dst, sem):
        return pltpu.make_async_remote_copy(
            src_ref=send2.at[:, pl.ds(0, frame), :],
            dst_ref=slot2(me),
            send_sem=ss2,
            recv_sem=sem,
            device_id={"mem": dst},
        )

    def forward2(src):
        return pltpu.make_async_remote_copy(
            src_ref=slot2(src),
            dst_ref=slot2(src),
            send_sem=ss2,
            recv_sem=rs2f,
            device_id={"mem": partner},
        )

    def copyx(side, dst):
        i = 0 if xs == 1 else 1 - side
        return pltpu.make_async_remote_copy(
            src_ref=sendx.at[pl.ds(0, packed_rows), :],
            dst_ref=recvx.at[i, core, chip, pl.ds(0, packed_rows), :],
            send_sem=ssx.at[0 if xs == 1 else side],
            recv_sem=rsx.at[i],
            device_id={"mem": dst, "band": side_band[side]},
        )

    def forwardx(i):
        got = recvx.at[i, core, :, pl.ds(0, packed_rows), :]
        return pltpu.make_async_remote_copy(
            src_ref=got,
            dst_ref=got,
            send_sem=ssx.at[xs + i],
            recv_sem=rsxf.at[i],
            device_id={"mem": partner},
        )

    for side in (0, 1):

        @pl.when(has[side])
        def _():
            for o in range(0, n, 2):
                copyx(side, lax.rem(me + o, n)).start()

    for o in range(2, n, 2):
        copy2(lax.rem(me + o, n), rs2.at[chip]).start()
    copy2(partner, rs2f).start()
    for g in (0, 1):
        recv2[me, g] = send2[g]

    advbuf[...] = jnp.concatenate(moved + [jnp.zeros((SUB, wide), f32)], axis=0)
    pickt = jnp.concatenate([pick, pick], axis=0)
    for g in range(ng):
        hi, lo = split2(advbuf[:, g * gl : g * gl + main])
        e = dims(jnp.concatenate([hi, lo], axis=0), pickt, 0, 0)
        for l in range(lev):
            v = jnp.where(in_row, e[l * RG : (l + 1) * RG], 0.0)
            adv_ref[l, :, g * gcells : (g + 1) * gcells] = jnp.sum(v, axis=0, keepdims=True)

    def sent_edges():
        pre_copy.wait_send()
        all_of(rece, n - 1, packed_rows, in_sem.at[1])
        all_of(recv1, n // 2 - 1, used, in_sem.at[4])
        pltpu.make_async_copy(fe_recv, fe_recv, in_sem.at[5]).wait()
        for side in (0, 1):

            @pl.when(has[side])
            def _():
                all_of(recc.at[0], n, packed_rows, in_sem.at[2 + side])
                edge_copy(side).wait_send()
                pltpu.make_async_copy(edge_recv.at[side], edge_recv.at[side], edge_rs.at[0 if xs == 1 else side]).wait()

    sent_edges()
    for o in sorted(range(2, n, 2), key=lambda o: min(o, n - o)):
        src = lax.rem(me + o, n)
        pltpu.make_async_copy(slot2(src), slot2(src), rs2.at[src // 2]).wait()
        forward2(src).start()
    for side in (0, 1):

        @pl.when(has[side])
        def _():
            i = 0 if xs == 1 else side
            pltpu.make_async_copy(recvx.at[i, core, :, pl.ds(0, packed_rows), :], recvx.at[i, core, :, pl.ds(0, packed_rows), :], rsx.at[i]).wait()
            forwardx(i).start()

    def all_2(count, sem):
        got = recv2.at[pl.ds(0, count), :, pl.ds(0, frame), :]
        pltpu.make_async_copy(got, got, sem).wait()

    for side in (0, 1):

        @pl.when(has[side])
        def _():
            i = 0 if xs == 1 else side
            all_of(recvx.at[i, 0], n // 2, packed_rows, rsxf.at[i])

    all_2(n // 2, rs2f)

    over = iota((SUB, LANES), 0) < frame - block

    def across(ref):
        cols = [ref[t * LANES : (t + 1) * LANES, :].T for t in range(tiles)]
        cols = cols[0] if tiles == 1 else jnp.concatenate(cols, axis=1)
        return pltpu.roll(cols, lon - 1, 1)

    def gather(g):
        for d in range(n):
            tail = jnp.where(over, recv2[(d - 1) % n, g, SUB : 2 * SUB, :], 0.0)
            merged[d * SUB : (d + 1) * SUB, :] = recv2[d, g, 0:SUB, :] + tail
        return across(merged)

    def gather_edges(i):
        prev = pltpu.roll(pltpu.roll(recvx[i, 1, n // 2 - 1], half, 1), 5, 0)
        for d in range(n):
            e = recvx[i, d % 2, d // 2]
            b = pltpu.roll(pltpu.roll(e, half, 1), 5, 0)
            merged[d * SUB : (d + 1) * SUB, :] = jnp.where(row8 < 5, e, b) + jnp.where(over, prev, 0.0)
            prev = b
        return across(merged)

    c0 = gather(0)
    c1 = gather(1)
    cx = [gather_edges(i) for i in range(xs)]
    cu, cd = cx[0], cx[-1]
    e0 = main - LANES
    coarse = jnp.concatenate([c0, c1[0:e0]], axis=0)
    en = whole(ensf)
    wm = en * coarse * scale
    w_up = jnp.where(kk == 0, 0.0, pltpu.roll(wm, 1, 0))
    w_dn = jnp.where(kk == rows - 1, 0.0, pltpu.roll(wm, main - 1, 0))
    zz = smooth_lon(0.25 * (w_up + w_dn) + 0.5 * wm)
    for t in range(tiles):
        grad_ref[t] = zz[:, t * LANES : (t + 1) * LANES]
    for side, k, k_in in ((0, 0, 1), (1, rows - 1, rows - 2)):
        src = (cu, cd)[side]
        mine_at = e0 + side * 2 * levp
        edge_at = (1 - side) * 2 * levp
        extra = jnp.where(has[side], src[edge_at : edge_at + lev], 0.0)
        halo = c1[mine_at : mine_at + lev] + jnp.where(has[side], src[edge_at + levp : edge_at + levp + lev], 0.0)
        we = row(ensf, k) * extra * scale
        wh = edge_recv[side, 0:lev, :] * halo * scale
        z_edge = smooth_lon(0.5 * we + 0.25 * wh)
        z_in = smooth_lon(0.25 * we)
        for t in range(tiles):
            cut = slice(t * LANES, (t + 1) * LANES)
            grad_ref.at[t][pl.ds(k, lev, stride=rows), :] += z_edge[:, cut]
            grad_ref.at[t][pl.ds(k_in, lev, stride=rows), :] += z_in[:, cut]

    for side in (0, 1):

        @pl.when(has[side])
        def _():
            i = 0 if xs == 1 else side
            all_of(recvx.at[0, 0], n // 2, packed_rows, ssx.at[i])
            all_of(recvx.at[0, 0], n // 2, packed_rows, ssx.at[xs + i])

    all_2(n - 1, ss2)


def writer(adv_ref, grad_ref, adv_out, grad_out, sem):
    copies = [
        pltpu.make_async_copy(grad_ref, grad_out, sem.at[0]),
        pltpu.make_async_copy(adv_ref, adv_out, sem.at[1]),
    ]
    for c in copies:
        c.start()
    for c in copies:
        c.wait()


def up_to(x, m):
    return -(-x // m) * m


def to_tiles(x):
    return x.reshape(-1, x.shape[3] // LANES, LANES).swapaxes(0, 1)


def shards(ensemble, alpha, lat_lower, lat_weight, background, obs_cell, obs_value, obs_precision):
    n, nb = lax.axis_size("mem"), lax.axis_size("band")
    members, lev, rows, lon = ensemble.shape
    fine_rows = lat_lower.shape[0]
    cells = background.shape[2]
    nobs = obs_cell.shape[1]
    fine_cols = cells // fine_rows
    scale = 1.0 / math.sqrt(members * n - 1)
    block = lon // n
    main = lev * rows
    kaps = main + 4 * RG
    assert n % 2 == 0 and members == 1 and block == SUB and rows == RG and lev <= RG and kaps == 2 * LANES
    assert fine_rows % RG == 0 and fine_cols % block == 0 and fine_cols // block == 3
    cfg = (n, nb, lev, rows, lon, fine_rows, fine_cols, scale)
    tiles = lon // LANES
    ng = fine_rows // RG
    gl = RG * RG
    wide = ng * gl
    gcells = RG * fine_cols
    xs = 1 if nb == 2 else 2
    dma = pltpu.SemaphoreType.DMA
    vm = pl.BlockSpec(memory_space=pltpu.VMEM)
    hbm = pl.BlockSpec(memory_space=pltpu.HBM)
    fr = 2 * SUB
    advected, gradient = pl.pallas_call(
        functools.partial(kernel, cfg),
        out_shape=(
            jax.ShapeDtypeStruct(background.shape, f32),
            jax.ShapeDtypeStruct((tiles, main, LANES), f32),
        ),
        in_specs=[hbm] * 8,
        out_specs=(vm, vm),
        scratch_shapes=[
            pltpu.VMEM((tiles, main, LANES), bf16),
            pltpu.VMEM((tiles, main, LANES), f32),
            pltpu.VMEM((1, fine_rows), jnp.int32),
            pltpu.VMEM((1, fine_rows), f32),
            pltpu.VMEM(background.shape, f32),
            pltpu.VMEM((1, nobs), jnp.int32),
            pltpu.VMEM(obs_value.shape, f32),
            pltpu.VMEM((1, nobs), f32),
            pltpu.VMEM((tiles, main, LANES), f32),
            pltpu.VMEM((tiles, main, LANES), f32),
            pltpu.VMEM((kaps, lon), f32),
            pltpu.VMEM((LANES, lon), f32),
            pltpu.VMEM((2, RG, lon), f32),
            pltpu.VMEM((2, RG, lon), f32),
            pltpu.VMEM((3, lon + SUB, LANES), f32),
            pltpu.VMEM((n // 2, 2, fr, LANES), f32),
            pltpu.VMEM((n // 2, fr, LANES), f32),
            pltpu.VMEM((n // 2, fr, LANES), f32),
            pltpu.VMEM((n // 2, fr, LANES), f32),
            pltpu.VMEM((n, SUB, LANES), f32),
            pltpu.VMEM((n, SUB, LANES), f32),
            pltpu.VMEM((xs, n, SUB, LANES), f32),
            pltpu.VMEM((xs, n, SUB, LANES), f32),
            pltpu.VMEM((kaps, wide), bf16),
            pltpu.VMEM((kaps, wide), bf16),
            pltpu.VMEM((wide, kaps), bf16),
            pltpu.VMEM((wide, kaps), bf16),
            pltpu.VMEM((gl, 2 * gcells), bf16),
            pltpu.VMEM((gl, 2 * nobs), bf16),
            pltpu.VMEM((LANES, 2 * nobs), bf16),
            pltpu.VMEM((4 * SUB, wide), f32),
            pltpu.VMEM((4 * SUB, wide), f32),
            pltpu.VMEM((4 * SUB, wide), f32),
            pltpu.VMEM((2, SUB, LANES), f32),
            pltpu.VMEM((2, SUB, LANES), f32),
            pltpu.VMEM((fr, wide), f32),
            pltpu.VMEM((fr, wide), f32),
            pltpu.VMEM((4 * SUB, wide), f32),
            pltpu.VMEM((2, fr, LANES), f32),
            pltpu.VMEM((n, 2, fr, LANES), f32),
            pltpu.VMEM((SUB, LANES), f32),
            pltpu.VMEM((xs, 2, n // 2, SUB, LANES), f32),
            pltpu.VMEM((lon, LANES), f32),
            dma((8,)),
            dma((xs,)),
            dma,
            dma,
            dma,
            dma((xs,)),
            dma,
            dma,
            dma((n // 2,)),
            dma,
            dma((2 * xs,)),
            dma((xs,)),
            dma((xs,)),
        ],
        compiler_params=pltpu.CompilerParams(collective_id=0, has_side_effects=True, vmem_limit_bytes=48 * 2**20),
    )(
        *(
            pltpu.with_memory_space_constraint(v, pltpu.HBM)
            for v in (
                to_tiles(ensemble),
                to_tiles(alpha),
                lat_lower.reshape(1, fine_rows),
                lat_weight.reshape(1, fine_rows),
                background,
                obs_cell,
                obs_value,
                obs_precision,
            )
        )
    )
    advected, gradient = pl.pallas_call(
        writer,
        out_shape=(
            jax.ShapeDtypeStruct(background.shape, f32),
            jax.ShapeDtypeStruct((tiles, main, LANES), f32),
        ),
        in_specs=[vm, vm],
        out_specs=(hbm, hbm),
        scratch_shapes=[dma((2,))],
        compiler_params=pltpu.CompilerParams(vmem_limit_bytes=2**20),
    )(advected, gradient)
    return advected, gradient.swapaxes(0, 1).reshape(members, lev, rows, lon)


def solution(mesh):
    return jax.shard_map(
        shards,
        mesh=mesh,
        in_specs=(
            P("mem", None, "band", None),
            P("mem", None, "band", None),
            P("band"),
            P("band"),
            P(None, ("band", "mem"), None),
            P(("band", "mem"), None),
            P(None, ("band", "mem"), None),
            P(("band", "mem"), None),
        ),
        out_specs=(P(None, ("band", "mem"), None), P("mem", None, "band", None)),
        check_vma=False,
    )
```

```python
import functools
import math

import jax
import jax.numpy as jnp
from jax import lax
from jax.experimental import pallas as pl
from jax.experimental.pallas import tpu as pltpu
from jax.sharding import PartitionSpec as P

advect_rate = 0.25
LANES = 128
SUB = 8
RG = 16
f32 = jnp.float32
bf16 = jnp.bfloat16


def split2(x):
    hi = x.astype(bf16)
    lo = (x - hi.astype(f32)).astype(bf16)
    return hi, lo


def split2f(x):
    hi = x.astype(bf16).astype(f32)
    return hi, x - hi


def dims(a, b, ca, cb):
    return lax.dot_general(a, b, (((ca,), (cb,)), ((), ())), preferred_element_type=f32)


def iota(shape, d):
    return lax.broadcasted_iota(jnp.int32, shape, d)


def smooth_lon(x):
    n = x.shape[1]
    return 0.25 * pltpu.roll(x, 1, 1) + 0.5 * x + 0.25 * pltpu.roll(x, n - 1, 1)


def lon_weights(ratio):
    def parts(shift):
        num = 2 * shift + 1 + ratio
        return num // (2 * ratio), (num % (2 * ratio)) / (2 * ratio)

    def taps(shift):
        q, f = parts(shift)
        w = [0.0, 0.0, 0.0]
        for at, v in ((q, 1.0 - f), (q + 1, f)):
            if v:
                w[at] += v
        return w

    value = [taps(b) for b in range(ratio)]
    slope = [[0.5 * (p - m) for p, m in zip(taps(b + 1), taps(b - 1))] for b in range(ratio)]
    return value, slope


def combine(weights, parts):
    out = None
    for w, p in zip(weights, parts):
        if w == 0.0:
            continue
        term = p if w == 1.0 else w * p
        out = term if out is None else out + term
    return out


def chip_order(chips):
    ring = 4 if chips % 4 == 0 else chips
    rest = chips // ring

    def hops(step):
        return min(step[0], ring - step[0]) + min(step[1], rest - step[1])

    steps = sorted(((a, b) for a in range(ring) for b in range(rest)), key=lambda s: -hops(s))
    classes = [[s for s in steps if hops(s) == h] for h in sorted({hops(s) for s in steps if hops(s)}, reverse=True)]
    return steps, classes, ring, rest


def kernel(
    cfg,
    ens_hbm,
    alpha_hbm,
    low_hbm,
    wt_hbm,
    bg_hbm,
    cell_hbm,
    val_hbm,
    prec_hbm,
    adv_ref,
    grad_ref,
    ens_in,
    alpha,
    low,
    wt,
    bg,
    cell,
    val,
    prec,
    ensf,
    plain,
    part,
    xpart,
    edge_send,
    edge_recv,
    flat,
    frames,
    pre_recv,
    psum,
    recv1,
    eloc,
    rece,
    ecr,
    recc,
    table_hi,
    table_lo,
    back_hi,
    back_lo,
    zbuf,
    rbuf,
    abuf,
    fine_bg,
    obs_a,
    obs_b,
    fe_send,
    fe_recv,
    lbuf,
    gbuf,
    advbuf,
    send2,
    recv2,
    sendx,
    recvx,
    merged,
    in_sem,
    edge_rs,
    pre_rs,
    rs1,
    rse,
    rsc,
    fe_rs,
    ss2,
    rs2,
    rs2f,
    ssx,
    rsx,
    rsxf,
):
    n, nb, lev, rows, lon, fine_rows, fine_cols, scale = cfg
    block = lon // n
    frame = block + 2
    ratio = fine_cols // block
    main = lev * rows
    tiles = lon // LANES
    ng = fine_rows // RG
    gcells = RG * fine_cols
    gl = RG * RG
    levp = RG
    xs = recvx.shape[0]
    me = lax.axis_index("mem")
    band = lax.axis_index("band")
    has_up = band > 0
    has_down = band < nb - 1
    has = (has_up, has_down)
    wv, ws = lon_weights(ratio)

    barrier = pltpu.get_barrier_semaphore()

    core = lax.rem(me, 2)
    chip = me // 2
    partner = me + 1 - 2 * core
    chips = n // 2
    far_first, classes, ring, rest = chip_order(chips)
    ring_at, rest_at = chip // rest, lax.rem(chip, rest)

    def to_chip(step):
        return lax.rem(ring_at + step[0], ring) * rest + lax.rem(rest_at + step[1], rest)

    def from_chip(step):
        return to_chip(((ring - step[0]) % ring, (rest - step[1]) % rest))

    side_band = (band - 1, band + 1)
    for step in far_first:
        home = step == (0, 0)
        for c in (core, 1 - core):
            if nb == 2:
                pl.semaphore_signal(barrier, inc=1, device_id={"mem": 2 * to_chip(step) + c, "band": 1 - band})
            else:
                for side in (0, 1):

                    @pl.when(has[side])
                    def _():
                        pl.semaphore_signal(
                            barrier, inc=1, device_id={"mem": 2 * to_chip(step) + c, "band": side_band[side]}
                        )

            if not (home and c is core):
                pl.semaphore_signal(barrier, inc=1, device_id={"mem": 2 * to_chip(step) + c})

    loads = [
        pltpu.make_async_copy(src, dst, in_sem.at[i])
        for i, (src, dst) in enumerate(
            (
                (alpha_hbm, alpha),
                (ens_hbm, ens_in),
                (bg_hbm, bg),
                (low_hbm, low),
                (wt_hbm, wt),
                (cell_hbm, cell),
                (val_hbm, val),
                (prec_hbm, prec),
            )
        )
    ]
    for c in loads:
        c.start()

    part[main:, :] = jnp.zeros((part.shape[0] - main, lon), f32)
    xpart[...] = jnp.zeros(xpart.shape, f32)
    edge_send[...] = jnp.zeros(edge_send.shape, f32)
    fe_send[...] = jnp.zeros(fe_send.shape, f32)

    loads[0].wait()
    loads[1].wait()

    def whole(ref):
        parts = [ref[t] for t in range(tiles)]
        return parts[0] if tiles == 1 else jnp.concatenate(parts, axis=1)

    def row(ref, k):
        parts = [ref.at[t][pl.ds(k, lev, stride=rows), :] for t in range(tiles)]
        return parts[0] if tiles == 1 else jnp.concatenate(parts, axis=1)

    for t in range(tiles):
        ensf[t] = ens_in[t].astype(f32)
    al = whole(alpha)
    en = whole(ensf)
    kk = iota((main, lon), 0) % rows
    a_up = jnp.where(kk == 0, 0.0, pltpu.roll(al, 1, 0))
    a_dn = jnp.where(kk == rows - 1, 0.0, pltpu.roll(al, main - 1, 0))
    z = smooth_lon(0.25 * (a_up + a_dn) + 0.5 * al) * en * scale
    for t in range(tiles):
        plain[t] = z[:, t * LANES : (t + 1) * LANES]
    part[0:main, :] = z
    edges = []
    for side, k in ((0, 0), (1, rows - 1)):
        a_edge = smooth_lon(row(alpha, k)) * (0.25 * scale)
        e_edge = row(ensf, k)
        edges.append((a_edge, e_edge, row(plain, k)))
        edge_send[side, 0:lev, :] = e_edge
        at = main + side * 2 * levp
        part[at : at + lev, :] = a_edge
        part[at + levp : at + levp + lev, :] = e_edge
    (a_0, e_0, p_0), (a_1, e_1, p_1) = edges
    zero = jnp.zeros_like(a_0)
    sets_up = [p_0, zero, e_0, a_0]
    sets_down = [e_1, a_1, p_1, zero]
    if xs == 1:
        sets = [jnp.where(has_up, u, d) for u, d in zip(sets_up, sets_down)]
    else:
        sets = sets_up + sets_down
    for i, v in enumerate(sets):
        xpart[i * levp : i * levp + lev, :] = v

    def lay(g, rows_of):
        rows_of = pltpu.roll(rows_of, 1, 1)
        for t in range(tiles):
            flat[g, t * LANES : (t + 1) * LANES, :] = rows_of[:, t * LANES : (t + 1) * LANES].T
        flat[g, lon : lon + SUB, :] = flat[g, 0:SUB, :]

    lay(0, part[0:LANES, :])
    lay(1, part[LANES : 2 * LANES, :])
    lay(2, xpart[...])

    lane8 = iota((SUB, LANES), 1)
    row8 = iota((SUB, LANES), 0)
    low_half = lane8 < LANES // 2
    half = LANES // 2

    def tile_of(g, d):
        return flat[g, d * SUB : (d + 1) * SUB, :]

    def views(d):
        v, x = tile_of(1, d), tile_of(2, d)
        flip, flipx = pltpu.roll(v, half, 1), pltpu.roll(x, half, 1)
        return v, flip, x, flipx, pltpu.roll(flip, 5, 0), pltpu.roll(v, 3, 0), pltpu.roll(flipx, 3, 0), pltpu.roll(x, 3, 0)

    cur = views(0)
    for d in range(n):
        nxt = views(d + 1)
        v, flip, x, flipx, r5, v3, fx3, x3 = cur
        packed = jnp.where(low_half, pltpu.roll(v, 2, 0), jnp.where(row8 < 5, r5, nxt[4]))
        frames[d // 2, d % 2, 0:SUB, :] = tile_of(0, d)
        frames[d // 2, d % 2, SUB : 2 * SUB, :] = jnp.where(row8 < 2, tile_of(0, d + 1), packed)
        eloc[d] = jnp.where(low_half, flip, jnp.where(row8 < 3, v3, nxt[5]))
        ecr[0, d] = jnp.where(low_half, x, jnp.where(row8 < 3, fx3, nxt[6]))
        if xs == 2:
            ecr[1, d] = jnp.where(low_half, flipx, jnp.where(row8 < 3, x3, nxt[7]))
        cur = nxt

    loads[2].wait()
    row32 = iota((4 * SUB, gcells), 0)
    col_of = jnp.where(row32 < ratio * SUB, (row32 % SUB) * ratio + row32 // SUB, -1)
    pick = (iota((4 * SUB, gcells), 1) % fine_cols == col_of).astype(f32).astype(bf16)
    pick2 = jnp.concatenate([pick, pick], axis=1)
    in_row = iota((RG, gcells), 1) // fine_cols == iota((RG, gcells), 0)
    zbuf[main:, :] = jnp.zeros((gl - main, 2 * gcells), bf16)
    back = bg[:, 0, :]
    for g in range(ng):
        hi, lo = split2f(back[:, g * gcells : (g + 1) * gcells])
        for l in range(lev):
            at = slice(l * RG, (l + 1) * RG)
            zbuf[at, 0:gcells] = jnp.where(in_row, jnp.broadcast_to(hi[l : l + 1], (RG, gcells)), 0.0).astype(bf16)
            zbuf[at, gcells : 2 * gcells] = jnp.where(in_row, jnp.broadcast_to(lo[l : l + 1], (RG, gcells)), 0.0).astype(bf16)
        fine_bg[:, g * gl : (g + 1) * gl] = dims(pick2, zbuf[...], 1, 1)
    for c in loads[3:]:
        c.wait()

    if nb == 2:
        pl.semaphore_wait(barrier, 2 * n - 1)
    else:
        pl.semaphore_wait(barrier, n - 1 + n * (has_up.astype(jnp.int32) + has_down.astype(jnp.int32)))

    pre_copy = pltpu.make_async_remote_copy(
        src_ref=frames.at[:, 1 - core],
        dst_ref=pre_recv,
        send_sem=in_sem.at[0],
        recv_sem=pre_rs,
        device_id={"mem": partner},
    )
    pre_copy.start()
    packed_rows = frame // 2

    def copyc(side, dst):
        i = 0 if xs == 1 else 1 - side
        return pltpu.make_async_remote_copy(
            src_ref=ecr.at[0 if xs == 1 else side, dst, pl.ds(0, packed_rows), :],
            dst_ref=recc.at[i, me, pl.ds(0, packed_rows), :],
            send_sem=in_sem.at[2 + side],
            recv_sem=rsc.at[i],
            device_id={"mem": dst, "band": side_band[side]},
        )

    def copye(dst):
        return pltpu.make_async_remote_copy(
            src_ref=eloc.at[dst, pl.ds(0, packed_rows), :],
            dst_ref=rece.at[me, pl.ds(0, packed_rows), :],
            send_sem=in_sem.at[1],
            recv_sem=rse,
            device_id={"mem": dst},
        )

    def edge_copy(side):
        return pltpu.make_async_remote_copy(
            src_ref=edge_send.at[side],
            dst_ref=edge_recv.at[1 - side],
            send_sem=in_sem.at[6 + side],
            recv_sem=edge_rs.at[0 if xs == 1 else 1 - side],
            device_id={"band": side_band[side]},
        )

    for side in (0, 1):

        @pl.when(has[side])
        def _():
            for step in far_first:
                for c in (core, 1 - core):
                    copyc(side, 2 * to_chip(step) + c).start()

        @pl.when(jnp.logical_not(has[side]))
        def _():
            edge_recv[side] = jnp.zeros(edge_recv.shape[1:], f32)

    for step in far_first:
        for c in (core, 1 - core):
            if step != (0, 0) or c is not core:
                copye(2 * to_chip(step) + c).start()
    for side in (0, 1):

        @pl.when(has[side])
        def _():
            edge_copy(side).start()

    rece[me] = eloc[me]

    first = fine_bg[0:1, :]
    last = fine_bg[ratio * SUB - 1 : ratio * SUB, :]
    for t in range(ng * gl // LANES):
        fe_send[0, t : t + 1, :] = first[:, t * LANES : (t + 1) * LANES]
        fe_send[1, t : t + 1, :] = last[:, t * LANES : (t + 1) * LANES]

    def fe_copy(side):
        return pltpu.make_async_remote_copy(
            src_ref=fe_send.at[side],
            dst_ref=fe_recv.at[1 - side],
            send_sem=in_sem.at[5],
            recv_sem=fe_rs,
            device_id={"mem": lax.rem(me + (n - 1 if side == 0 else 1), n)},
        )

    fe_copy(0).start()
    fe_copy(1).start()

    lane = iota((SUB, LANES), 1)
    wide = ng * gl

    def per_row(v):
        v = jnp.concatenate([v, jnp.zeros((1, LANES - fine_rows), f32)], axis=1)
        return jnp.broadcast_to(v, (SUB, LANES))

    def tiled(v, g):
        r = v if g == 0 else pltpu.roll(v, LANES - g * RG, 1)
        r = jnp.where(lane < RG, r, 0.0)
        for s in (RG, 2 * RG, 4 * RG):
            r = r + pltpu.roll(r, s, 1)
        return jnp.concatenate([r, r], axis=0)

    low_rows, wt_rows = per_row(low[...].astype(f32)), per_row(wt[...])
    down = lambda v: jnp.concatenate([v] * (LANES // SUB), axis=0).T
    low_col, wt_col = down(low_rows), down(wt_rows)
    lane16 = iota((RG, LANES), 1)
    row16 = iota((RG, LANES), 0)
    lev_of = lane16 // RG
    set_rows = (-1, 0, rows, rows - 1)
    table_hi[...] = jnp.zeros(table_hi.shape, bf16)
    table_lo[...] = jnp.zeros(table_lo.shape, bf16)
    back_hi[...] = jnp.zeros(back_hi.shape, bf16)
    back_lo[...] = jnp.zeros(back_lo.shape, bf16)
    halves = gl // LANES
    per = LANES // RG

    def weigh(k, lo_k, w):
        w_hi, w_lo = split2f(w)
        o_hi, o_lo = split2f(1.0 - w)
        m0, m1 = k == lo_k, k == lo_k + 1.0
        return (
            jnp.where(m0, o_hi, jnp.where(m1, w_hi, 0.0)),
            jnp.where(m0, o_lo, jnp.where(m1, w_lo, 0.0)),
        )

    def put(ref, r, c, v, keep):
        ref[r : r + RG, c : c + LANES] = jnp.where(keep, v, 0.0).astype(bf16)

    for g in range(ng):
        lo_t, w_t = tiled(low_rows, g), tiled(wt_rows, g)
        main_t = weigh(row16.astype(f32), lo_t, w_t)
        set_t = [weigh(jnp.full((RG, LANES), float(k), f32), lo_t, w_t) for k in set_rows]
        for ref, which in ((table_hi, 0), (table_lo, 1)):
            for l in range(lev):
                put(ref, l * RG, g * gl + l // per * LANES, main_t[which], lev_of == l % per)
            for s in range(4):
                for h in range(halves):
                    put(ref, main + s * levp, g * gl + h * LANES, set_t[s][which], (row16 == lev_of + h * per) & (row16 < lev))
        lo_c, w_c = low_col[g * RG : (g + 1) * RG], wt_col[g * RG : (g + 1) * RG]
        for h in range(halves):
            kap = lane16 + h * LANES
            e = kap - main
            es = e // levp
            ek = jnp.where(es == 0, -1, jnp.where(es == 1, 0, jnp.where(es == 2, rows, rows - 1)))
            k_of = jnp.where(e < 0, kap % rows, ek).astype(f32)
            l_of = jnp.where(e < 0, kap // rows, e % levp)
            back_t = weigh(k_of, lo_c, w_c)
            for ref, which in ((back_hi, 0), (back_lo, 1)):
                for l in range(lev):
                    if (h + 1) * LANES > main or l // per == h:
                        put(ref, g * gl + l * RG, h * LANES, back_t[which], l_of == l)

    pre_copy.wait_recv()
    for j in range(n // 2):
        psum[j] = frames[j, core] + pre_recv[j]

    used = frame + packed_rows

    def copy1(dst):
        return pltpu.make_async_remote_copy(
            src_ref=psum.at[dst, pl.ds(0, used), :],
            dst_ref=recv1.at[chip, pl.ds(0, used), :],
            send_sem=in_sem.at[4],
            recv_sem=rs1,
            device_id={"mem": 2 * dst + core},
        )

    for step in far_first[:-1]:
        copy1(to_chip(step)).start()
    recv1[chip] = psum[chip]

    nobs = cell.shape[1]
    crow = cell[...] // fine_cols
    ccol = cell[...] % fine_cols
    r32 = iota((4 * SUB, nobs), 0)
    col_o = jnp.where(r32 < ratio * SUB, (r32 % SUB) * ratio + r32 // SUB, -1)
    hot = (col_o == ccol).astype(f32).astype(bf16)
    hot2 = jnp.concatenate([hot, hot], axis=1)
    pr = prec[...]
    p_hi, p_lo = split2f(pr)
    v_hi, v_lo = split2f(val[:, 0, :] * pr)
    rbuf[main:, :] = jnp.zeros((gl - main, 2 * nobs), bf16)
    for g in range(ng):
        at_row = iota((RG, nobs), 0) + g * RG == crow
        for l in range(lev):
            at = slice(l * RG, (l + 1) * RG)
            rbuf[at, 0:nobs] = jnp.where(at_row, jnp.broadcast_to(v_hi[l : l + 1], (RG, nobs)), 0.0).astype(bf16)
            rbuf[at, nobs : 2 * nobs] = jnp.where(at_row, jnp.broadcast_to(v_lo[l : l + 1], (RG, nobs)), 0.0).astype(bf16)
        obs_b[:, g * gl : (g + 1) * gl] = dims(hot2, rbuf[...], 1, 1)
        ph = jnp.where(at_row, jnp.broadcast_to(p_hi, (RG, nobs)), 0.0).astype(bf16)
        plo = jnp.where(at_row, jnp.broadcast_to(p_lo, (RG, nobs)), 0.0).astype(bf16)
        for j in range(LANES // RG):
            abuf[j * RG : (j + 1) * RG, 0:nobs] = ph
            abuf[j * RG : (j + 1) * RG, nobs : 2 * nobs] = plo
        oa = dims(hot2, abuf[...], 1, 1)
        for j in range(gl // LANES):
            obs_a[:, g * gl + j * LANES : g * gl + (j + 1) * LANES] = oa

    pltpu.make_async_copy(fe_recv, fe_recv, fe_rs).wait()
    nt = wide // LANES
    left = jnp.concatenate([fe_recv[0, t : t + 1, :] for t in range(nt)], axis=1)
    right = jnp.concatenate([fe_recv[1, t : t + 1, :] for t in range(nt)], axis=1)
    fb = [fine_bg[b * SUB : (b + 1) * SUB, :] for b in range(ratio)]
    arow = iota((SUB, wide), 0)
    before0 = jnp.where(arow == 0, left, pltpu.roll(fb[ratio - 1], 1, 0))
    after_last = jnp.where(arow == SUB - 1, right, pltpu.roll(fb[0], SUB - 1, 0))
    chain = [before0] + fb + [after_last]
    slope_bg = [0.5 * (chain[b + 2] - chain[b]) for b in range(ratio)]

    def all_of(ref, count, height, sem):
        got = ref.at[pl.ds(0, count), pl.ds(0, height), :]
        pltpu.make_async_copy(got, got, sem).wait()

    all_of(rece, n - 1, packed_rows, rse)
    for side in (0, 1):

        @pl.when(has[side])
        def _():
            i = 0 if xs == 1 else side
            all_of(recc.at[i], n, packed_rows, rsc.at[i])

    prods, plains = [], []
    for i in range(xs):
        prod = rece[0] * recc[i, 0]
        only = recc[i, 0]
        for s in range(1, n):
            prod = prod + rece[s] * recc[i, s]
            only = only + recc[i, s]
        prods.append(prod)
        plains.append(only)
    set_of = (lane8 % half) // levp
    edge_sum = jnp.where(
        set_of < 2, jnp.where(has_up, prods[0], 0.0), jnp.where(has_down, prods[-1], 0.0)
    )
    from_up = jnp.where(has_up, pltpu.roll(plains[0], LANES - 2 * levp, 1), 0.0)
    from_down = jnp.where(has_down, pltpu.roll(plains[-1], 2 * levp, 1), 0.0)
    edge_sum = edge_sum + jnp.where(set_of == 0, from_up, jnp.where(set_of == 2, from_down, 0.0))
    edge_a = pltpu.roll(edge_sum, half, 1)
    edge_b = pltpu.roll(edge_sum, 5, 0)

    all_of(recv1, n // 2 - 1, used, rs1)
    total = recv1[0]
    for s in range(1, n // 2):
        total = total + recv1[s]
    m = total[SUB:]
    m_a = pltpu.roll(m, SUB - 2, 0)
    m_b = pltpu.roll(pltpu.roll(m, half, 1), 3, 0)
    x_a = jnp.where(low_half, m_a, edge_a)
    x_b = jnp.where(low_half, m_b, edge_b)
    x = jnp.concatenate([total, jnp.concatenate([jnp.where(row8 < 5, x_a, x_b), x_b], axis=0)], axis=1)
    x_hi, x_lo = split2f(x)
    x2 = jnp.concatenate([x_hi, x_lo], axis=0).astype(bf16)
    y = dims(x2, table_hi[...], 1, 0)
    y = y[0:16] + y[16:32] + dims(x_hi.astype(bf16), table_lo[...], 1, 0)
    lbuf[...] = y
    taps = [lbuf[d : d + SUB, :] for d in range(3)]

    us, vs, moved = [], [], []
    for b in range(ratio):
        state = fb[b] + combine(wv[b], taps)
        slope = slope_bg[b] + combine(ws[b], taps)
        factor = 1.0 - advect_rate * slope
        mv = state * factor
        at = slice(b * SUB, (b + 1) * SUB)
        cot = obs_a[at, :] * mv - obs_b[at, :]
        us.append(cot * factor)
        vs.append((-advect_rate) * (state * cot))
        moved.append(mv)
    gbuf[...] = jnp.zeros(gbuf.shape, f32)
    for d in range(3):
        t = combine([wv[b][d] for b in range(ratio)] + [ws[b][d] for b in range(ratio)], us + vs)
        gbuf[d : d + SUB, :] += t
    gl_v = gbuf[...]
    g_hi, g_lo = split2f(gl_v)
    g2 = jnp.concatenate([g_hi, g_lo], axis=0).astype(bf16)
    gr = dims(g2, back_hi[...], 1, 0)
    gr = gr[0:16] + gr[16:32] + dims(g_hi.astype(bf16), back_lo[...], 1, 0)
    for g in (0, 1):
        send2[g] = gr[:, g * LANES : (g + 1) * LANES]
    v0, v1 = gr[0:SUB, LANES:], gr[SUB:, LANES:]
    sendx[...] = jnp.where(
        low_half, pltpu.roll(v0, half, 1), jnp.where(row8 < 3, pltpu.roll(v0, 3, 0), pltpu.roll(v1, 3, 0))
    )

    def slot2(src):
        return recv2.at[src, :, pl.ds(0, frame), :]

    def copy2(dst, sem):
        return pltpu.make_async_remote_copy(
            src_ref=send2.at[:, pl.ds(0, frame), :],
            dst_ref=slot2(me),
            send_sem=ss2,
            recv_sem=sem,
            device_id={"mem": dst},
        )

    def forward2(src):
        return pltpu.make_async_remote_copy(
            src_ref=slot2(src),
            dst_ref=slot2(src),
            send_sem=ss2,
            recv_sem=rs2f,
            device_id={"mem": partner},
        )

    def copyx(side, dst):
        i = 0 if xs == 1 else 1 - side
        return pltpu.make_async_remote_copy(
            src_ref=sendx.at[pl.ds(0, packed_rows), :],
            dst_ref=recvx.at[i, core, chip, pl.ds(0, packed_rows), :],
            send_sem=ssx.at[0 if xs == 1 else side],
            recv_sem=rsx.at[i],
            device_id={"mem": dst, "band": side_band[side]},
        )

    def forwardx(i):
        got = recvx.at[i, core, :, pl.ds(0, packed_rows), :]
        return pltpu.make_async_remote_copy(
            src_ref=got,
            dst_ref=got,
            send_sem=ssx.at[xs + i],
            recv_sem=rsxf.at[i],
            device_id={"mem": partner},
        )

    for side in (0, 1):

        @pl.when(has[side])
        def _():
            for step in far_first:
                copyx(side, 2 * to_chip(step) + core).start()

    for i, group in enumerate(classes):
        for step in group:
            copy2(2 * to_chip(step) + core, rs2.at[len(classes) - 1 - i]).start()
    copy2(partner, rs2f).start()
    for g in (0, 1):
        recv2[me, g] = send2[g]

    advbuf[...] = jnp.concatenate(moved + [jnp.zeros((SUB, wide), f32)], axis=0)
    pickt = jnp.concatenate([pick, pick], axis=0)
    for g in range(ng):
        hi, lo = split2(advbuf[:, g * gl : g * gl + main])
        e = dims(jnp.concatenate([hi, lo], axis=0), pickt, 0, 0)
        for l in range(lev):
            v = jnp.where(in_row, e[l * RG : (l + 1) * RG], 0.0)
            adv_ref[l, :, g * gcells : (g + 1) * gcells] = jnp.sum(v, axis=0, keepdims=True)

    def sent_edges():
        pre_copy.wait_send()
        all_of(rece, n - 1, packed_rows, in_sem.at[1])
        all_of(recv1, n // 2 - 1, used, in_sem.at[4])
        pltpu.make_async_copy(fe_recv, fe_recv, in_sem.at[5]).wait()
        for side in (0, 1):

            @pl.when(has[side])
            def _():
                all_of(recc.at[0], n, packed_rows, in_sem.at[2 + side])
                edge_copy(side).wait_send()
                pltpu.make_async_copy(edge_recv.at[side], edge_recv.at[side], edge_rs.at[0 if xs == 1 else side]).wait()

    sent_edges()
    def all_2(count, sem):
        got = recv2.at[pl.ds(0, count), :, pl.ds(0, frame), :]
        pltpu.make_async_copy(got, got, sem).wait()

    for i, group in enumerate(reversed(classes)):
        all_2(len(group), rs2.at[i])
        for step in group:
            forward2(2 * from_chip(step) + core).start()
    for side in (0, 1):

        @pl.when(has[side])
        def _():
            i = 0 if xs == 1 else side
            pltpu.make_async_copy(recvx.at[i, core, :, pl.ds(0, packed_rows), :], recvx.at[i, core, :, pl.ds(0, packed_rows), :], rsx.at[i]).wait()
            forwardx(i).start()

    all_2(n // 2, rs2f)

    over = iota((SUB, LANES), 0) < frame - block

    def across(ref):
        cols = [ref[t * LANES : (t + 1) * LANES, :].T for t in range(tiles)]
        cols = cols[0] if tiles == 1 else jnp.concatenate(cols, axis=1)
        return pltpu.roll(cols, lon - 1, 1)

    def gather(g):
        for d in range(n):
            tail = jnp.where(over, recv2[(d - 1) % n, g, SUB : 2 * SUB, :], 0.0)
            merged[d * SUB : (d + 1) * SUB, :] = recv2[d, g, 0:SUB, :] + tail
        return across(merged)

    def gather_edges(i):
        prev = pltpu.roll(pltpu.roll(recvx[i, 1, n // 2 - 1], half, 1), 5, 0)
        for d in range(n):
            e = recvx[i, d % 2, d // 2]
            b = pltpu.roll(pltpu.roll(e, half, 1), 5, 0)
            merged[d * SUB : (d + 1) * SUB, :] = jnp.where(row8 < 5, e, b) + jnp.where(over, prev, 0.0)
            prev = b
        return across(merged)

    c0 = gather(0)
    c1 = gather(1)
    e0 = main - LANES
    coarse = jnp.concatenate([c0, c1[0:e0]], axis=0)
    en = whole(ensf)
    wm = en * coarse * scale
    w_up = jnp.where(kk == 0, 0.0, pltpu.roll(wm, 1, 0))
    w_dn = jnp.where(kk == rows - 1, 0.0, pltpu.roll(wm, main - 1, 0))
    zz = smooth_lon(0.25 * (w_up + w_dn) + 0.5 * wm)
    for t in range(tiles):
        grad_ref[t] = zz[:, t * LANES : (t + 1) * LANES]
    for side in (0, 1):

        @pl.when(has[side])
        def _():
            i = 0 if xs == 1 else side
            all_of(recvx.at[i, 0], n // 2, packed_rows, rsxf.at[i])

    cx = [gather_edges(i) for i in range(xs)]
    cu, cd = cx[0], cx[-1]
    for side, k, k_in in ((0, 0, 1), (1, rows - 1, rows - 2)):
        src = (cu, cd)[side]
        mine_at = e0 + side * 2 * levp
        edge_at = (1 - side) * 2 * levp
        extra = jnp.where(has[side], src[edge_at : edge_at + lev], 0.0)
        halo = c1[mine_at : mine_at + lev] + jnp.where(has[side], src[edge_at + levp : edge_at + levp + lev], 0.0)
        we = row(ensf, k) * extra * scale
        wh = edge_recv[side, 0:lev, :] * halo * scale
        z_edge = smooth_lon(0.5 * we + 0.25 * wh)
        z_in = smooth_lon(0.25 * we)
        for t in range(tiles):
            cut = slice(t * LANES, (t + 1) * LANES)
            grad_ref.at[t][pl.ds(k, lev, stride=rows), :] += z_edge[:, cut]
            grad_ref.at[t][pl.ds(k_in, lev, stride=rows), :] += z_in[:, cut]

    for side in (0, 1):

        @pl.when(has[side])
        def _():
            i = 0 if xs == 1 else side
            all_of(recvx.at[0, 0], n // 2, packed_rows, ssx.at[i])
            all_of(recvx.at[0, 0], n // 2, packed_rows, ssx.at[xs + i])

    all_2(n - 1, ss2)


def writer(adv_ref, grad_ref, adv_out, grad_out, sem):
    copies = [
        pltpu.make_async_copy(grad_ref, grad_out, sem.at[0]),
        pltpu.make_async_copy(adv_ref, adv_out, sem.at[1]),
    ]
    for c in copies:
        c.start()
    for c in copies:
        c.wait()


def up_to(x, m):
    return -(-x // m) * m


def to_tiles(x):
    return x.reshape(-1, x.shape[3] // LANES, LANES).swapaxes(0, 1)


def shards(ensemble, alpha, lat_lower, lat_weight, background, obs_cell, obs_value, obs_precision):
    n, nb = lax.axis_size("mem"), lax.axis_size("band")
    members, lev, rows, lon = ensemble.shape
    fine_rows = lat_lower.shape[0]
    cells = background.shape[2]
    nobs = obs_cell.shape[1]
    fine_cols = cells // fine_rows
    scale = 1.0 / math.sqrt(members * n - 1)
    block = lon // n
    main = lev * rows
    kaps = main + 4 * RG
    assert n % 2 == 0 and members == 1 and block == SUB and rows == RG and lev <= RG and kaps == 2 * LANES
    assert fine_rows % RG == 0 and fine_cols % block == 0 and fine_cols // block == 3
    cfg = (n, nb, lev, rows, lon, fine_rows, fine_cols, scale)
    tiles = lon // LANES
    ng = fine_rows // RG
    gl = RG * RG
    wide = ng * gl
    gcells = RG * fine_cols
    xs = 1 if nb == 2 else 2
    dma = pltpu.SemaphoreType.DMA
    vm = pl.BlockSpec(memory_space=pltpu.VMEM)
    hbm = pl.BlockSpec(memory_space=pltpu.HBM)
    fr = 2 * SUB
    advected, gradient = pl.pallas_call(
        functools.partial(kernel, cfg),
        out_shape=(
            jax.ShapeDtypeStruct(background.shape, f32),
            jax.ShapeDtypeStruct((tiles, main, LANES), f32),
        ),
        in_specs=[hbm] * 8,
        out_specs=(vm, vm),
        scratch_shapes=[
            pltpu.VMEM((tiles, main, LANES), bf16),
            pltpu.VMEM((tiles, main, LANES), f32),
            pltpu.VMEM((1, fine_rows), jnp.int32),
            pltpu.VMEM((1, fine_rows), f32),
            pltpu.VMEM(background.shape, f32),
            pltpu.VMEM((1, nobs), jnp.int32),
            pltpu.VMEM(obs_value.shape, f32),
            pltpu.VMEM((1, nobs), f32),
            pltpu.VMEM((tiles, main, LANES), f32),
            pltpu.VMEM((tiles, main, LANES), f32),
            pltpu.VMEM((kaps, lon), f32),
            pltpu.VMEM((LANES, lon), f32),
            pltpu.VMEM((2, RG, lon), f32),
            pltpu.VMEM((2, RG, lon), f32),
            pltpu.VMEM((3, lon + SUB, LANES), f32),
            pltpu.VMEM((n // 2, 2, fr, LANES), f32),
            pltpu.VMEM((n // 2, fr, LANES), f32),
            pltpu.VMEM((n // 2, fr, LANES), f32),
            pltpu.VMEM((n // 2, fr, LANES), f32),
            pltpu.VMEM((n, SUB, LANES), f32),
            pltpu.VMEM((n, SUB, LANES), f32),
            pltpu.VMEM((xs, n, SUB, LANES), f32),
            pltpu.VMEM((xs, n, SUB, LANES), f32),
            pltpu.VMEM((kaps, wide), bf16),
            pltpu.VMEM((kaps, wide), bf16),
            pltpu.VMEM((wide, kaps), bf16),
            pltpu.VMEM((wide, kaps), bf16),
            pltpu.VMEM((gl, 2 * gcells), bf16),
            pltpu.VMEM((gl, 2 * nobs), bf16),
            pltpu.VMEM((LANES, 2 * nobs), bf16),
            pltpu.VMEM((4 * SUB, wide), f32),
            pltpu.VMEM((4 * SUB, wide), f32),
            pltpu.VMEM((4 * SUB, wide), f32),
            pltpu.VMEM((2, SUB, LANES), f32),
            pltpu.VMEM((2, SUB, LANES), f32),
            pltpu.VMEM((fr, wide), f32),
            pltpu.VMEM((fr, wide), f32),
            pltpu.VMEM((4 * SUB, wide), f32),
            pltpu.VMEM((2, fr, LANES), f32),
            pltpu.VMEM((n, 2, fr, LANES), f32),
            pltpu.VMEM((SUB, LANES), f32),
            pltpu.VMEM((xs, 2, n // 2, SUB, LANES), f32),
            pltpu.VMEM((lon, LANES), f32),
            dma((8,)),
            dma((xs,)),
            dma,
            dma,
            dma,
            dma((xs,)),
            dma,
            dma,
            dma((len(chip_order(n // 2)[1]),)),
            dma,
            dma((2 * xs,)),
            dma((xs,)),
            dma((xs,)),
        ],
        compiler_params=pltpu.CompilerParams(collective_id=0, has_side_effects=True, vmem_limit_bytes=48 * 2**20),
    )(
        *(
            pltpu.with_memory_space_constraint(v, pltpu.HBM)
            for v in (
                to_tiles(ensemble),
                to_tiles(alpha),
                lat_lower.reshape(1, fine_rows),
                lat_weight.reshape(1, fine_rows),
                background,
                obs_cell,
                obs_value,
                obs_precision,
            )
        )
    )
    advected, gradient = pl.pallas_call(
        writer,
        out_shape=(
            jax.ShapeDtypeStruct(background.shape, f32),
            jax.ShapeDtypeStruct((tiles, main, LANES), f32),
        ),
        in_specs=[vm, vm],
        out_specs=(hbm, hbm),
        scratch_shapes=[dma((2,))],
        compiler_params=pltpu.CompilerParams(vmem_limit_bytes=2**20),
    )(advected, gradient)
    return advected, gradient.swapaxes(0, 1).reshape(members, lev, rows, lon)


def solution(mesh):
    return jax.shard_map(
        shards,
        mesh=mesh,
        in_specs=(
            P("mem", None, "band", None),
            P("mem", None, "band", None),
            P("band"),
            P("band"),
            P(None, ("band", "mem"), None),
            P(("band", "mem"), None),
            P(None, ("band", "mem"), None),
            P(("band", "mem"), None),
        ),
        out_specs=(P(None, ("band", "mem"), None), P("mem", None, "band", None)),
        check_vma=False,
    )
```

```python
import functools
import math

import jax
import jax.numpy as jnp
from jax import lax
from jax.experimental import pallas as pl
from jax.experimental.pallas import tpu as pltpu
from jax.sharding import PartitionSpec as P

advect_rate = 0.25
LANES = 128
SUB = 8
RG = 16
f32 = jnp.float32
bf16 = jnp.bfloat16


def split2(x):
    hi = x.astype(bf16)
    lo = (x - hi.astype(f32)).astype(bf16)
    return hi, lo


def split2f(x):
    hi = x.astype(bf16).astype(f32)
    return hi, x - hi


def dims(a, b, ca, cb):
    return lax.dot_general(a, b, (((ca,), (cb,)), ((), ())), preferred_element_type=f32)


def iota(shape, d):
    return lax.broadcasted_iota(jnp.int32, shape, d)


def smooth_lon(x):
    n = x.shape[1]
    return 0.25 * pltpu.roll(x, 1, 1) + 0.5 * x + 0.25 * pltpu.roll(x, n - 1, 1)


def lon_weights(ratio):
    def parts(shift):
        num = 2 * shift + 1 + ratio
        return num // (2 * ratio), (num % (2 * ratio)) / (2 * ratio)

    def taps(shift):
        q, f = parts(shift)
        w = [0.0, 0.0, 0.0]
        for at, v in ((q, 1.0 - f), (q + 1, f)):
            if v:
                w[at] += v
        return w

    value = [taps(b) for b in range(ratio)]
    slope = [[0.5 * (p - m) for p, m in zip(taps(b + 1), taps(b - 1))] for b in range(ratio)]
    return value, slope


def combine(weights, parts):
    out = None
    for w, p in zip(weights, parts):
        if w == 0.0:
            continue
        term = p if w == 1.0 else w * p
        out = term if out is None else out + term
    return out


def chip_order(chips):
    ring = 4 if chips % 4 == 0 else chips
    rest = chips // ring

    def hops(step):
        return min(step[0], ring - step[0]) + min(step[1], rest - step[1])

    steps = sorted(((a, b) for a in range(ring) for b in range(rest)), key=lambda s: -hops(s))
    classes = [[s for s in steps if hops(s) == h] for h in sorted({hops(s) for s in steps if hops(s)}, reverse=True)]
    return steps, classes, ring, rest


def kernel(
    cfg,
    ens_hbm,
    alpha_hbm,
    low_hbm,
    wt_hbm,
    bg_hbm,
    cell_hbm,
    val_hbm,
    prec_hbm,
    adv_ref,
    grad_ref,
    ens_in,
    alpha,
    low,
    wt,
    bg,
    cell,
    val,
    prec,
    ensf,
    plain,
    part,
    xpart,
    edge_send,
    edge_recv,
    flat,
    frames,
    pre_recv,
    psum,
    recv1,
    eloc,
    rece,
    ecr,
    recc,
    table_hi,
    table_lo,
    back_hi,
    back_lo,
    zbuf,
    rbuf,
    abuf,
    fine_bg,
    obs_a,
    obs_b,
    fe_send,
    fe_recv,
    lbuf,
    gbuf,
    advbuf,
    send2,
    recv2,
    sendx,
    recvx,
    merged,
    ensr,
    in_sem,
    edge_rs,
    pre_rs,
    rs1,
    rse,
    rsc,
    fe_rs,
    ss2,
    rs2,
    rs2f,
    ssx,
    rsx,
    rsxf,
):
    n, nb, lev, rows, lon, fine_rows, fine_cols, scale = cfg
    block = lon // n
    frame = block + 2
    ratio = fine_cols // block
    main = lev * rows
    tiles = lon // LANES
    ng = fine_rows // RG
    gcells = RG * fine_cols
    gl = RG * RG
    levp = RG
    xs = recvx.shape[0]
    me = lax.axis_index("mem")
    band = lax.axis_index("band")
    has_up = band > 0
    has_down = band < nb - 1
    has = (has_up, has_down)
    wv, ws = lon_weights(ratio)

    barrier = pltpu.get_barrier_semaphore()

    core = lax.rem(me, 2)
    chip = me // 2
    partner = me + 1 - 2 * core
    chips = n // 2
    far_first, classes, ring, rest = chip_order(chips)
    ring_at, rest_at = chip // rest, lax.rem(chip, rest)

    def to_chip(step):
        return lax.rem(ring_at + step[0], ring) * rest + lax.rem(rest_at + step[1], rest)

    def from_chip(step):
        return to_chip(((ring - step[0]) % ring, (rest - step[1]) % rest))

    side_band = (band - 1, band + 1)
    for step in far_first:
        home = step == (0, 0)
        for c in (core, 1 - core):
            if nb == 2:
                pl.semaphore_signal(barrier, inc=1, device_id={"mem": 2 * to_chip(step) + c, "band": 1 - band})
            else:
                for side in (0, 1):

                    @pl.when(has[side])
                    def _():
                        pl.semaphore_signal(
                            barrier, inc=1, device_id={"mem": 2 * to_chip(step) + c, "band": side_band[side]}
                        )

            if not (home and c is core):
                pl.semaphore_signal(barrier, inc=1, device_id={"mem": 2 * to_chip(step) + c})

    loads = [
        pltpu.make_async_copy(src, dst, in_sem.at[i])
        for i, (src, dst) in enumerate(
            (
                (alpha_hbm, alpha),
                (ens_hbm, ens_in),
                (bg_hbm, bg),
                (low_hbm, low),
                (wt_hbm, wt),
                (cell_hbm, cell),
                (val_hbm, val),
                (prec_hbm, prec),
            )
        )
    ]
    for c in loads:
        c.start()

    part[main:, :] = jnp.zeros((part.shape[0] - main, lon), f32)
    xpart[...] = jnp.zeros(xpart.shape, f32)
    edge_send[...] = jnp.zeros(edge_send.shape, f32)
    fe_send[...] = jnp.zeros(fe_send.shape, f32)

    loads[0].wait()
    loads[1].wait()

    def whole(ref):
        parts = [ref[t] for t in range(tiles)]
        return parts[0] if tiles == 1 else jnp.concatenate(parts, axis=1)

    def row(ref, k):
        parts = [ref.at[t][pl.ds(k, lev, stride=rows), :] for t in range(tiles)]
        return parts[0] if tiles == 1 else jnp.concatenate(parts, axis=1)

    for t in range(tiles):
        ensf[t] = ens_in[t].astype(f32)
    al = whole(alpha)
    en = whole(ensf)
    kk = iota((main, lon), 0) % rows
    a_up = jnp.where(kk == 0, 0.0, pltpu.roll(al, 1, 0))
    a_dn = jnp.where(kk == rows - 1, 0.0, pltpu.roll(al, main - 1, 0))
    z = smooth_lon(0.25 * (a_up + a_dn) + 0.5 * al) * en * scale
    for t in range(tiles):
        plain[t] = z[:, t * LANES : (t + 1) * LANES]
    part[0:main, :] = z
    edges = []
    for side, k in ((0, 0), (1, rows - 1)):
        a_edge = smooth_lon(row(alpha, k)) * (0.25 * scale)
        e_edge = row(ensf, k)
        edges.append((a_edge, e_edge, row(plain, k)))
        edge_send[side, 0:lev, :] = e_edge
        at = main + side * 2 * levp
        for i, v in enumerate((a_edge, e_edge) if side == 0 else (e_edge, a_edge)):
            part[at + i * levp : at + i * levp + lev, :] = v
    (a_0, e_0, p_0), (a_1, e_1, p_1) = edges
    zero = jnp.zeros_like(a_0)
    sets_up = [zero, p_0, a_0, e_0]
    sets_down = [e_1, a_1, p_1, zero]
    if xs == 1:
        sets = [jnp.where(has_up, u, d) for u, d in zip(sets_up, sets_down)]
    else:
        sets = sets_up + sets_down
    for i, v in enumerate(sets):
        xpart[i * levp : i * levp + lev, :] = v

    def lay(g, rows_of):
        rows_of = pltpu.roll(rows_of, 1, 1)
        for t in range(tiles):
            flat[g, t * LANES : (t + 1) * LANES, :] = rows_of[:, t * LANES : (t + 1) * LANES].T
        flat[g, lon : lon + SUB, :] = flat[g, 0:SUB, :]

    lay(0, part[0:LANES, :])
    lay(1, part[LANES : 2 * LANES, :])
    lay(2, xpart[...])

    lane8 = iota((SUB, LANES), 1)
    row8 = iota((SUB, LANES), 0)
    low_half = lane8 < LANES // 2
    half = LANES // 2

    def tile_of(g, d):
        return flat[g, d * SUB : (d + 1) * SUB, :]

    def views(d):
        v, x = tile_of(1, d), tile_of(2, d)
        flip, flipx = pltpu.roll(v, half, 1), pltpu.roll(x, half, 1)
        return v, flip, x, flipx, pltpu.roll(flip, 5, 0), pltpu.roll(v, 3, 0), pltpu.roll(flipx, 3, 0), pltpu.roll(x, 3, 0)

    cur = views(0)
    for d in range(n):
        nxt = views(d + 1)
        v, flip, x, flipx, r5, v3, fx3, x3 = cur
        packed = jnp.where(low_half, pltpu.roll(v, 2, 0), jnp.where(row8 < 5, r5, nxt[4]))
        frames[d // 2, d % 2, 0:SUB, :] = tile_of(0, d)
        frames[d // 2, d % 2, SUB : 2 * SUB, :] = jnp.where(row8 < 2, tile_of(0, d + 1), packed)
        eloc[d] = jnp.where(low_half, flip, jnp.where(row8 < 3, v3, nxt[5]))
        ecr[0, d] = jnp.where(low_half, x, jnp.where(row8 < 3, fx3, nxt[6]))
        if xs == 2:
            ecr[1, d] = jnp.where(low_half, flipx, jnp.where(row8 < 3, x3, nxt[7]))
        cur = nxt

    loads[2].wait()
    row32 = iota((4 * SUB, gcells), 0)
    col_of = jnp.where(row32 < ratio * SUB, (row32 % SUB) * ratio + row32 // SUB, -1)
    pick = (iota((4 * SUB, gcells), 1) % fine_cols == col_of).astype(f32).astype(bf16)
    pick2 = jnp.concatenate([pick, pick], axis=1)
    in_row = iota((RG, gcells), 1) // fine_cols == iota((RG, gcells), 0)
    zbuf[main:, :] = jnp.zeros((gl - main, 2 * gcells), bf16)
    back = bg[:, 0, :]
    for g in range(ng):
        hi, lo = split2f(back[:, g * gcells : (g + 1) * gcells])
        for l in range(lev):
            at = slice(l * RG, (l + 1) * RG)
            zbuf[at, 0:gcells] = jnp.where(in_row, jnp.broadcast_to(hi[l : l + 1], (RG, gcells)), 0.0).astype(bf16)
            zbuf[at, gcells : 2 * gcells] = jnp.where(in_row, jnp.broadcast_to(lo[l : l + 1], (RG, gcells)), 0.0).astype(bf16)
        fine_bg[:, g * gl : (g + 1) * gl] = dims(pick2, zbuf[...], 1, 1)
    for c in loads[3:]:
        c.wait()

    if nb == 2:
        pl.semaphore_wait(barrier, 2 * n - 1)
    else:
        pl.semaphore_wait(barrier, n - 1 + n * (has_up.astype(jnp.int32) + has_down.astype(jnp.int32)))

    pre_copy = pltpu.make_async_remote_copy(
        src_ref=frames.at[:, 1 - core],
        dst_ref=pre_recv,
        send_sem=in_sem.at[0],
        recv_sem=pre_rs,
        device_id={"mem": partner},
    )
    pre_copy.start()
    packed_rows = frame // 2

    def copyc(side, dst):
        i = 0 if xs == 1 else 1 - side
        return pltpu.make_async_remote_copy(
            src_ref=ecr.at[0 if xs == 1 else side, dst, pl.ds(0, packed_rows), :],
            dst_ref=recc.at[i, me, pl.ds(0, packed_rows), :],
            send_sem=in_sem.at[2 + side],
            recv_sem=rsc.at[i],
            device_id={"mem": dst, "band": side_band[side]},
        )

    def copye(dst):
        return pltpu.make_async_remote_copy(
            src_ref=eloc.at[dst, pl.ds(0, packed_rows), :],
            dst_ref=rece.at[me, pl.ds(0, packed_rows), :],
            send_sem=in_sem.at[1],
            recv_sem=rse,
            device_id={"mem": dst},
        )

    def edge_copy(side):
        return pltpu.make_async_remote_copy(
            src_ref=edge_send.at[side],
            dst_ref=edge_recv.at[1 - side],
            send_sem=in_sem.at[6 + side],
            recv_sem=edge_rs.at[0 if xs == 1 else 1 - side],
            device_id={"band": side_band[side]},
        )

    for side in (0, 1):

        @pl.when(has[side])
        def _():
            for step in far_first:
                for c in (core, 1 - core):
                    copyc(side, 2 * to_chip(step) + c).start()

        @pl.when(jnp.logical_not(has[side]))
        def _():
            edge_recv[side] = jnp.zeros(edge_recv.shape[1:], f32)

    for step in far_first:
        for c in (core, 1 - core):
            if step != (0, 0) or c is not core:
                copye(2 * to_chip(step) + c).start()
    for side in (0, 1):

        @pl.when(has[side])
        def _():
            edge_copy(side).start()

    rece[me] = eloc[me]

    first = fine_bg[0:1, :]
    last = fine_bg[ratio * SUB - 1 : ratio * SUB, :]
    for t in range(ng * gl // LANES):
        fe_send[0, t : t + 1, :] = first[:, t * LANES : (t + 1) * LANES]
        fe_send[1, t : t + 1, :] = last[:, t * LANES : (t + 1) * LANES]

    def fe_copy(side):
        return pltpu.make_async_remote_copy(
            src_ref=fe_send.at[side],
            dst_ref=fe_recv.at[1 - side],
            send_sem=in_sem.at[5],
            recv_sem=fe_rs,
            device_id={"mem": lax.rem(me + (n - 1 if side == 0 else 1), n)},
        )

    fe_copy(0).start()
    fe_copy(1).start()

    lane = iota((SUB, LANES), 1)
    wide = ng * gl

    def per_row(v):
        v = jnp.concatenate([v, jnp.zeros((1, LANES - fine_rows), f32)], axis=1)
        return jnp.broadcast_to(v, (SUB, LANES))

    def tiled(v, g):
        r = v if g == 0 else pltpu.roll(v, LANES - g * RG, 1)
        r = jnp.where(lane < RG, r, 0.0)
        for s in (RG, 2 * RG, 4 * RG):
            r = r + pltpu.roll(r, s, 1)
        return jnp.concatenate([r, r], axis=0)

    low_rows, wt_rows = per_row(low[...].astype(f32)), per_row(wt[...])
    down = lambda v: jnp.concatenate([v] * (LANES // SUB), axis=0).T
    low_col, wt_col = down(low_rows), down(wt_rows)
    lane16 = iota((RG, LANES), 1)
    row16 = iota((RG, LANES), 0)
    lev_of = lane16 // RG
    set_rows = (-1, 0, rows - 1, rows)
    table_hi[...] = jnp.zeros(table_hi.shape, bf16)
    table_lo[...] = jnp.zeros(table_lo.shape, bf16)
    back_hi[...] = jnp.zeros(back_hi.shape, bf16)
    back_lo[...] = jnp.zeros(back_lo.shape, bf16)
    halves = gl // LANES
    per = LANES // RG

    def weigh(k, lo_k, w):
        w_hi, w_lo = split2f(w)
        o_hi, o_lo = split2f(1.0 - w)
        m0, m1 = k == lo_k, k == lo_k + 1.0
        return (
            jnp.where(m0, o_hi, jnp.where(m1, w_hi, 0.0)),
            jnp.where(m0, o_lo, jnp.where(m1, w_lo, 0.0)),
        )

    def put(ref, r, c, v, keep):
        ref[r : r + RG, c : c + LANES] = jnp.where(keep, v, 0.0).astype(bf16)

    for g in range(ng):
        lo_t, w_t = tiled(low_rows, g), tiled(wt_rows, g)
        main_t = weigh(row16.astype(f32), lo_t, w_t)
        set_t = [weigh(jnp.full((RG, LANES), float(k), f32), lo_t, w_t) for k in set_rows]
        for ref, which in ((table_hi, 0), (table_lo, 1)):
            for l in range(lev):
                put(ref, l * RG, g * gl + l // per * LANES, main_t[which], lev_of == l % per)
            for s in range(4):
                for h in range(halves):
                    put(ref, main + s * levp, g * gl + h * LANES, set_t[s][which], (row16 == lev_of + h * per) & (row16 < lev))
        lo_c, w_c = low_col[g * RG : (g + 1) * RG], wt_col[g * RG : (g + 1) * RG]
        for h in range(halves):
            kap = lane16 + h * LANES
            e = kap - main
            es = e // levp
            ek = jnp.where(es == 0, -1, jnp.where(es == 1, 0, jnp.where(es == 2, rows - 1, rows)))
            k_of = jnp.where(e < 0, kap % rows, ek).astype(f32)
            l_of = jnp.where(e < 0, kap // rows, e % levp)
            back_t = weigh(k_of, lo_c, w_c)
            for ref, which in ((back_hi, 0), (back_lo, 1)):
                for l in range(lev):
                    if (h + 1) * LANES > main or l // per == h:
                        put(ref, g * gl + l * RG, h * LANES, back_t[which], l_of == l)

    pre_copy.wait_recv()
    for j in range(n // 2):
        psum[j] = frames[j, core] + pre_recv[j]

    used = frame + packed_rows

    def copy1(dst):
        return pltpu.make_async_remote_copy(
            src_ref=psum.at[dst, pl.ds(0, used), :],
            dst_ref=recv1.at[chip, pl.ds(0, used), :],
            send_sem=in_sem.at[4],
            recv_sem=rs1,
            device_id={"mem": 2 * dst + core},
        )

    for step in far_first[:-1]:
        copy1(to_chip(step)).start()
    recv1[chip] = psum[chip]

    nobs = cell.shape[1]
    crow = cell[...] // fine_cols
    ccol = cell[...] % fine_cols
    r32 = iota((4 * SUB, nobs), 0)
    col_o = jnp.where(r32 < ratio * SUB, (r32 % SUB) * ratio + r32 // SUB, -1)
    hot = (col_o == ccol).astype(f32).astype(bf16)
    hot2 = jnp.concatenate([hot, hot], axis=1)
    pr = prec[...]
    p_hi, p_lo = split2f(pr)
    v_hi, v_lo = split2f(val[:, 0, :] * pr)
    rbuf[main:, :] = jnp.zeros((gl - main, 2 * nobs), bf16)
    for g in range(ng):
        at_row = iota((RG, nobs), 0) + g * RG == crow
        for l in range(lev):
            at = slice(l * RG, (l + 1) * RG)
            rbuf[at, 0:nobs] = jnp.where(at_row, jnp.broadcast_to(v_hi[l : l + 1], (RG, nobs)), 0.0).astype(bf16)
            rbuf[at, nobs : 2 * nobs] = jnp.where(at_row, jnp.broadcast_to(v_lo[l : l + 1], (RG, nobs)), 0.0).astype(bf16)
        obs_b[:, g * gl : (g + 1) * gl] = dims(hot2, rbuf[...], 1, 1)
        ph = jnp.where(at_row, jnp.broadcast_to(p_hi, (RG, nobs)), 0.0).astype(bf16)
        plo = jnp.where(at_row, jnp.broadcast_to(p_lo, (RG, nobs)), 0.0).astype(bf16)
        for j in range(LANES // RG):
            abuf[j * RG : (j + 1) * RG, 0:nobs] = ph
            abuf[j * RG : (j + 1) * RG, nobs : 2 * nobs] = plo
        oa = dims(hot2, abuf[...], 1, 1)
        for j in range(gl // LANES):
            obs_a[:, g * gl + j * LANES : g * gl + (j + 1) * LANES] = oa

    pltpu.make_async_copy(fe_recv, fe_recv, fe_rs).wait()
    nt = wide // LANES
    left = jnp.concatenate([fe_recv[0, t : t + 1, :] for t in range(nt)], axis=1)
    right = jnp.concatenate([fe_recv[1, t : t + 1, :] for t in range(nt)], axis=1)
    fb = [fine_bg[b * SUB : (b + 1) * SUB, :] for b in range(ratio)]
    arow = iota((SUB, wide), 0)
    before0 = jnp.where(arow == 0, left, pltpu.roll(fb[ratio - 1], 1, 0))
    after_last = jnp.where(arow == SUB - 1, right, pltpu.roll(fb[0], SUB - 1, 0))
    chain = [before0] + fb + [after_last]
    slope_bg = [0.5 * (chain[b + 2] - chain[b]) for b in range(ratio)]

    def all_of(ref, count, height, sem):
        got = ref.at[pl.ds(0, count), pl.ds(0, height), :]
        pltpu.make_async_copy(got, got, sem).wait()

    all_of(rece, n - 1, packed_rows, rse)
    for side in (0, 1):

        @pl.when(has[side])
        def _():
            i = 0 if xs == 1 else side
            all_of(recc.at[i], n, packed_rows, rsc.at[i])

    prods, plains = [], []
    for i in range(xs):
        prod = rece[0] * recc[i, 0]
        only = recc[i, 0]
        for s in range(1, n):
            prod = prod + rece[s] * recc[i, s]
            only = only + recc[i, s]
        prods.append(prod)
        plains.append(only)
    set_of = (lane8 % half) // levp
    edge_sum = jnp.where(
        set_of < 2, jnp.where(has_up, prods[0], 0.0), jnp.where(has_down, prods[-1], 0.0)
    )
    from_up = jnp.where(has_up, pltpu.roll(plains[0], LANES - 2 * levp, 1), 0.0)
    from_down = jnp.where(has_down, pltpu.roll(plains[-1], 2 * levp, 1), 0.0)
    edge_sum = edge_sum + jnp.where(set_of == 0, from_up, jnp.where(set_of == 3, from_down, 0.0))
    edge_a = pltpu.roll(edge_sum, half, 1)
    edge_b = pltpu.roll(edge_sum, 5, 0)

    all_of(recv1, n // 2 - 1, used, rs1)
    total = recv1[0]
    for s in range(1, n // 2):
        total = total + recv1[s]
    m = total[SUB:]
    m_a = pltpu.roll(m, SUB - 2, 0)
    m_b = pltpu.roll(pltpu.roll(m, half, 1), 3, 0)
    x_a = jnp.where(low_half, m_a, edge_a)
    x_b = jnp.where(low_half, m_b, edge_b)
    x = jnp.concatenate([total, jnp.concatenate([jnp.where(row8 < 5, x_a, x_b), x_b], axis=0)], axis=1)
    x_hi, x_lo = split2f(x)
    x2 = jnp.concatenate([x_hi, x_lo], axis=0).astype(bf16)
    y = dims(x2, table_hi[...], 1, 0)
    y = y[0:16] + y[16:32] + dims(x_hi.astype(bf16), table_lo[...], 1, 0)
    lbuf[...] = y
    taps = [lbuf[d : d + SUB, :] for d in range(3)]

    us, vs, moved = [], [], []
    for b in range(ratio):
        state = fb[b] + combine(wv[b], taps)
        slope = slope_bg[b] + combine(ws[b], taps)
        factor = 1.0 - advect_rate * slope
        mv = state * factor
        at = slice(b * SUB, (b + 1) * SUB)
        cot = obs_a[at, :] * mv - obs_b[at, :]
        us.append(cot * factor)
        vs.append((-advect_rate) * (state * cot))
        moved.append(mv)
    gbuf[...] = jnp.zeros(gbuf.shape, f32)
    for d in range(3):
        t = combine([wv[b][d] for b in range(ratio)] + [ws[b][d] for b in range(ratio)], us + vs)
        gbuf[d : d + SUB, :] += t
    gl_v = gbuf[...]
    g_hi, g_lo = split2f(gl_v)
    g2 = jnp.concatenate([g_hi, g_lo], axis=0).astype(bf16)
    gr = dims(g2, back_hi[...], 1, 0)
    gr = gr[0:16] + gr[16:32] + dims(g_hi.astype(bf16), back_lo[...], 1, 0)
    for g in (0, 1):
        send2[g] = gr[:, g * LANES : (g + 1) * LANES]
    v0, v1 = gr[0:SUB, LANES:], gr[SUB:, LANES:]
    quarter = lane8 // (2 * levp)
    v32, v96, w32, w96 = (pltpu.roll(v, r, 1) for v in (v0, v1) for r in (2 * levp, 6 * levp))

    def late(a, b):
        return jnp.where(row8 < 3, pltpu.roll(a, 3, 0), pltpu.roll(b, 3, 0))

    def pack_for(up_there):
        near = jnp.where(up_there, v32, v96)
        rest_cols = late(jnp.where(up_there, v96, v32), jnp.where(up_there, w96, w32))
        q = jnp.where(up_there, quarter - 1, quarter)
        return jnp.where(q == 2, near, jnp.where(q == 0, rest_cols, 0.0))

    if xs == 1:
        sendx[0] = pack_for(has_up)
    else:
        for side in (0, 1):
            sendx[side] = pack_for(side == 0)

    def slot2(src):
        return recv2.at[src, :, pl.ds(0, frame), :]

    def copy2(dst, sem):
        return pltpu.make_async_remote_copy(
            src_ref=send2.at[:, pl.ds(0, frame), :],
            dst_ref=slot2(me),
            send_sem=ss2,
            recv_sem=sem,
            device_id={"mem": dst},
        )

    def forward2(src):
        return pltpu.make_async_remote_copy(
            src_ref=slot2(src),
            dst_ref=slot2(src),
            send_sem=ss2,
            recv_sem=rs2f,
            device_id={"mem": partner},
        )

    def copyx(side, dst):
        i = 0 if xs == 1 else 1 - side
        return pltpu.make_async_remote_copy(
            src_ref=sendx.at[0 if xs == 1 else side, pl.ds(0, packed_rows), :],
            dst_ref=recvx.at[i, core, chip, pl.ds(0, packed_rows), :],
            send_sem=ssx.at[0 if xs == 1 else side],
            recv_sem=rsx.at[i],
            device_id={"mem": dst, "band": side_band[side]},
        )

    def forwardx(i):
        got = recvx.at[i, core, :, pl.ds(0, packed_rows), :]
        return pltpu.make_async_remote_copy(
            src_ref=got,
            dst_ref=got,
            send_sem=ssx.at[xs + i],
            recv_sem=rsxf.at[i],
            device_id={"mem": partner},
        )

    for side in (0, 1):

        @pl.when(has[side])
        def _():
            for step in far_first:
                copyx(side, 2 * to_chip(step) + core).start()

    for i, group in enumerate(classes):
        for step in group:
            copy2(2 * to_chip(step) + core, rs2.at[len(classes) - 1 - i]).start()
    copy2(partner, rs2f).start()
    for g in (0, 1):
        recv2[me, g] = send2[g]

    advbuf[...] = jnp.concatenate(moved + [jnp.zeros((SUB, wide), f32)], axis=0)
    pickt = jnp.concatenate([pick, pick], axis=0)
    for g in range(ng):
        hi, lo = split2(advbuf[:, g * gl : g * gl + main])
        e = dims(jnp.concatenate([hi, lo], axis=0), pickt, 0, 0)
        for l in range(lev):
            v = jnp.where(in_row, e[l * RG : (l + 1) * RG], 0.0)
            adv_ref[l, :, g * gcells : (g + 1) * gcells] = jnp.sum(v, axis=0, keepdims=True)

    def sent_edges():
        pre_copy.wait_send()
        all_of(rece, n - 1, packed_rows, in_sem.at[1])
        all_of(recv1, n // 2 - 1, used, in_sem.at[4])
        pltpu.make_async_copy(fe_recv, fe_recv, in_sem.at[5]).wait()
        for side in (0, 1):

            @pl.when(has[side])
            def _():
                all_of(recc.at[0], n, packed_rows, in_sem.at[2 + side])
                edge_copy(side).wait_send()
                pltpu.make_async_copy(edge_recv.at[side], edge_recv.at[side], edge_rs.at[0 if xs == 1 else side]).wait()

    sent_edges()
    def all_2(count, sem):
        got = recv2.at[pl.ds(0, count), :, pl.ds(0, frame), :]
        pltpu.make_async_copy(got, got, sem).wait()

    ensr[...] = pltpu.roll(whole(ensf), 1, 1) * scale
    edge_ens = [pltpu.roll(row(ensf, k), 1, 1) * scale for k in (0, rows - 1)]
    halo_ens = [pltpu.roll(edge_recv[side, 0:lev, :], 1, 1) * scale for side in (0, 1)]

    def smooth_back(v):
        return 0.25 * v + 0.5 * pltpu.roll(v, lon - 1, 1) + 0.25 * pltpu.roll(v, lon - 2, 1)

    for i, group in enumerate(reversed(classes)):
        all_2(len(group), rs2.at[i])
        for step in group:
            forward2(2 * from_chip(step) + core).start()
    for side in (0, 1):

        @pl.when(has[side])
        def _():
            i = 0 if xs == 1 else side
            pltpu.make_async_copy(recvx.at[i, core, :, pl.ds(0, packed_rows), :], recvx.at[i, core, :, pl.ds(0, packed_rows), :], rsx.at[i]).wait()
            forwardx(i).start()

    all_2(n // 2, rs2f)

    over = iota((SUB, LANES), 0) < frame - block

    def across(ref):
        cols = [ref[t * LANES : (t + 1) * LANES, :].T for t in range(tiles)]
        return cols[0] if tiles == 1 else jnp.concatenate(cols, axis=1)

    ours = (quarter < 2) | (set_of == 0) | (set_of == 3)
    set_lanes = lane8 >= half

    def edges_at(i, d):
        e = recvx[i, d % 2, d // 2]
        b = pltpu.roll(pltpu.roll(e, half, 1), 5, 0)
        return jnp.where(row8 < 5, e, b), jnp.where(over, b, 0.0)

    def gather(g):
        sides = range(xs) if g else ()
        prev = [edges_at(i, n - 1)[1] for i in sides]
        for d in range(n):
            tile = recv2[d, g, 0:SUB, :] + jnp.where(over, recv2[(d - 1) % n, g, SUB : 2 * SUB, :], 0.0)
            if g:
                theirs = None
                for i in sides:
                    here, tail = edges_at(i, d)
                    v = here + prev[i]
                    if xs == 2:
                        v = jnp.where(has[i], v, 0.0)
                    theirs = v if theirs is None else theirs + v
                    prev[i] = tail
                tile = jnp.where(ours, tile, 0.0) + jnp.where(set_lanes, theirs, 0.0)
            merged[g, d * SUB : (d + 1) * SUB, :] = tile
        return across(merged.at[g])

    c0 = gather(0)
    for side in (0, 1):

        @pl.when(has[side])
        def _():
            i = 0 if xs == 1 else side
            all_of(recvx.at[i, 0], n // 2, packed_rows, rsxf.at[i])

    c1 = gather(1)
    e0 = main - LANES
    coarse = jnp.concatenate([c0, c1[0:e0]], axis=0)
    wm = ensr[...] * coarse
    w_up = jnp.where(kk == 0, 0.0, pltpu.roll(wm, 1, 0))
    w_dn = jnp.where(kk == rows - 1, 0.0, pltpu.roll(wm, main - 1, 0))
    zz = smooth_back(0.25 * (w_up + w_dn) + 0.5 * wm)
    for t in range(tiles):
        grad_ref[t] = zz[:, t * LANES : (t + 1) * LANES]
    for side, k, k_in in ((0, 0, 1), (1, rows - 1, rows - 2)):
        halo_at, extra_at = (e0, e0 + levp) if side == 0 else (e0 + 3 * levp, e0 + 2 * levp)
        we = edge_ens[side] * c1[extra_at : extra_at + lev]
        wh = halo_ens[side] * c1[halo_at : halo_at + lev]
        z_edge = smooth_back(0.5 * we + 0.25 * wh)
        z_in = smooth_back(0.25 * we)
        for t in range(tiles):
            cut = slice(t * LANES, (t + 1) * LANES)
            grad_ref.at[t][pl.ds(k, lev, stride=rows), :] += z_edge[:, cut]
            grad_ref.at[t][pl.ds(k_in, lev, stride=rows), :] += z_in[:, cut]

    for side in (0, 1):

        @pl.when(has[side])
        def _():
            i = 0 if xs == 1 else side
            all_of(recvx.at[0, 0], n // 2, packed_rows, ssx.at[i])
            all_of(recvx.at[0, 0], n // 2, packed_rows, ssx.at[xs + i])

    all_2(n - 1, ss2)


def writer(adv_ref, grad_ref, adv_out, grad_out, sem):
    copies = [
        pltpu.make_async_copy(grad_ref, grad_out, sem.at[0]),
        pltpu.make_async_copy(adv_ref, adv_out, sem.at[1]),
    ]
    for c in copies:
        c.start()
    for c in copies:
        c.wait()


def up_to(x, m):
    return -(-x // m) * m


def to_tiles(x):
    return x.reshape(-1, x.shape[3] // LANES, LANES).swapaxes(0, 1)


def shards(ensemble, alpha, lat_lower, lat_weight, background, obs_cell, obs_value, obs_precision):
    n, nb = lax.axis_size("mem"), lax.axis_size("band")
    members, lev, rows, lon = ensemble.shape
    fine_rows = lat_lower.shape[0]
    cells = background.shape[2]
    nobs = obs_cell.shape[1]
    fine_cols = cells // fine_rows
    scale = 1.0 / math.sqrt(members * n - 1)
    block = lon // n
    main = lev * rows
    kaps = main + 4 * RG
    assert n % 2 == 0 and members == 1 and block == SUB and rows == RG and lev <= RG and kaps == 2 * LANES
    assert fine_rows % RG == 0 and fine_cols % block == 0 and fine_cols // block == 3
    cfg = (n, nb, lev, rows, lon, fine_rows, fine_cols, scale)
    tiles = lon // LANES
    ng = fine_rows // RG
    gl = RG * RG
    wide = ng * gl
    gcells = RG * fine_cols
    xs = 1 if nb == 2 else 2
    dma = pltpu.SemaphoreType.DMA
    vm = pl.BlockSpec(memory_space=pltpu.VMEM)
    hbm = pl.BlockSpec(memory_space=pltpu.HBM)
    fr = 2 * SUB
    advected, gradient = pl.pallas_call(
        functools.partial(kernel, cfg),
        out_shape=(
            jax.ShapeDtypeStruct(background.shape, f32),
            jax.ShapeDtypeStruct((tiles, main, LANES), f32),
        ),
        in_specs=[hbm] * 8,
        out_specs=(vm, vm),
        scratch_shapes=[
            pltpu.VMEM((tiles, main, LANES), bf16),
            pltpu.VMEM((tiles, main, LANES), f32),
            pltpu.VMEM((1, fine_rows), jnp.int32),
            pltpu.VMEM((1, fine_rows), f32),
            pltpu.VMEM(background.shape, f32),
            pltpu.VMEM((1, nobs), jnp.int32),
            pltpu.VMEM(obs_value.shape, f32),
            pltpu.VMEM((1, nobs), f32),
            pltpu.VMEM((tiles, main, LANES), f32),
            pltpu.VMEM((tiles, main, LANES), f32),
            pltpu.VMEM((kaps, lon), f32),
            pltpu.VMEM((LANES, lon), f32),
            pltpu.VMEM((2, RG, lon), f32),
            pltpu.VMEM((2, RG, lon), f32),
            pltpu.VMEM((3, lon + SUB, LANES), f32),
            pltpu.VMEM((n // 2, 2, fr, LANES), f32),
            pltpu.VMEM((n // 2, fr, LANES), f32),
            pltpu.VMEM((n // 2, fr, LANES), f32),
            pltpu.VMEM((n // 2, fr, LANES), f32),
            pltpu.VMEM((n, SUB, LANES), f32),
            pltpu.VMEM((n, SUB, LANES), f32),
            pltpu.VMEM((xs, n, SUB, LANES), f32),
            pltpu.VMEM((xs, n, SUB, LANES), f32),
            pltpu.VMEM((kaps, wide), bf16),
            pltpu.VMEM((kaps, wide), bf16),
            pltpu.VMEM((wide, kaps), bf16),
            pltpu.VMEM((wide, kaps), bf16),
            pltpu.VMEM((gl, 2 * gcells), bf16),
            pltpu.VMEM((gl, 2 * nobs), bf16),
            pltpu.VMEM((LANES, 2 * nobs), bf16),
            pltpu.VMEM((4 * SUB, wide), f32),
            pltpu.VMEM((4 * SUB, wide), f32),
            pltpu.VMEM((4 * SUB, wide), f32),
            pltpu.VMEM((2, SUB, LANES), f32),
            pltpu.VMEM((2, SUB, LANES), f32),
            pltpu.VMEM((fr, wide), f32),
            pltpu.VMEM((fr, wide), f32),
            pltpu.VMEM((4 * SUB, wide), f32),
            pltpu.VMEM((2, fr, LANES), f32),
            pltpu.VMEM((n, 2, fr, LANES), f32),
            pltpu.VMEM((xs, SUB, LANES), f32),
            pltpu.VMEM((xs, 2, n // 2, SUB, LANES), f32),
            pltpu.VMEM((2, lon, LANES), f32),
            pltpu.VMEM((main, lon), f32),
            dma((8,)),
            dma((xs,)),
            dma,
            dma,
            dma,
            dma((xs,)),
            dma,
            dma,
            dma((len(chip_order(n // 2)[1]),)),
            dma,
            dma((2 * xs,)),
            dma((xs,)),
            dma((xs,)),
        ],
        compiler_params=pltpu.CompilerParams(collective_id=0, has_side_effects=True, vmem_limit_bytes=48 * 2**20),
    )(
        *(
            pltpu.with_memory_space_constraint(v, pltpu.HBM)
            for v in (
                to_tiles(ensemble),
                to_tiles(alpha),
                lat_lower.reshape(1, fine_rows),
                lat_weight.reshape(1, fine_rows),
                background,
                obs_cell,
                obs_value,
                obs_precision,
            )
        )
    )
    advected, gradient = pl.pallas_call(
        writer,
        out_shape=(
            jax.ShapeDtypeStruct(background.shape, f32),
            jax.ShapeDtypeStruct((tiles, main, LANES), f32),
        ),
        in_specs=[vm, vm],
        out_specs=(hbm, hbm),
        scratch_shapes=[dma((2,))],
        compiler_params=pltpu.CompilerParams(vmem_limit_bytes=2**20),
    )(advected, gradient)
    return advected, gradient.swapaxes(0, 1).reshape(members, lev, rows, lon)


def solution(mesh):
    return jax.shard_map(
        shards,
        mesh=mesh,
        in_specs=(
            P("mem", None, "band", None),
            P("mem", None, "band", None),
            P("band"),
            P("band"),
            P(None, ("band", "mem"), None),
            P(("band", "mem"), None),
            P(None, ("band", "mem"), None),
            P(("band", "mem"), None),
        ),
        out_specs=(P(None, ("band", "mem"), None), P("mem", None, "band", None)),
        check_vma=False,
    )
```

```python
import functools
import math

import jax
import jax.numpy as jnp
from jax import lax
from jax.experimental import pallas as pl
from jax.experimental.pallas import tpu as pltpu
from jax.sharding import PartitionSpec as P

advect_rate = 0.25
LANES = 128
SUB = 8
RG = 16
f32 = jnp.float32
bf16 = jnp.bfloat16


def split2(x):
    hi = x.astype(bf16)
    lo = (x - hi.astype(f32)).astype(bf16)
    return hi, lo


def split2f(x):
    hi = x.astype(bf16).astype(f32)
    return hi, x - hi


def dims(a, b, ca, cb):
    return lax.dot_general(a, b, (((ca,), (cb,)), ((), ())), preferred_element_type=f32)


def iota(shape, d):
    return lax.broadcasted_iota(jnp.int32, shape, d)


def smooth_lon(x):
    n = x.shape[1]
    return 0.25 * pltpu.roll(x, 1, 1) + 0.5 * x + 0.25 * pltpu.roll(x, n - 1, 1)


def lon_weights(ratio):
    def parts(shift):
        num = 2 * shift + 1 + ratio
        return num // (2 * ratio), (num % (2 * ratio)) / (2 * ratio)

    def taps(shift):
        q, f = parts(shift)
        w = [0.0, 0.0, 0.0]
        for at, v in ((q, 1.0 - f), (q + 1, f)):
            if v:
                w[at] += v
        return w

    value = [taps(b) for b in range(ratio)]
    slope = [[0.5 * (p - m) for p, m in zip(taps(b + 1), taps(b - 1))] for b in range(ratio)]
    return value, slope


def combine(weights, parts):
    out = None
    for w, p in zip(weights, parts):
        if w == 0.0:
            continue
        term = p if w == 1.0 else w * p
        out = term if out is None else out + term
    return out


def chip_order(chips):
    ring = 4 if chips % 4 == 0 else chips
    rest = chips // ring

    def hops(step):
        return min(step[0], ring - step[0]) + min(step[1], rest - step[1])

    steps = sorted(((a, b) for a in range(ring) for b in range(rest)), key=lambda s: -hops(s))
    classes = [[s for s in steps if hops(s) == h] for h in sorted({hops(s) for s in steps if hops(s)}, reverse=True)]
    return steps, classes, ring, rest


def kernel(
    cfg,
    ens_hbm,
    alpha_hbm,
    low_hbm,
    wt_hbm,
    bg_hbm,
    cell_hbm,
    val_hbm,
    prec_hbm,
    adv_ref,
    grad_ref,
    ens_in,
    alpha,
    low,
    wt,
    bg,
    cell,
    val,
    prec,
    ensf,
    plain,
    part,
    xpart,
    edge_send,
    edge_recv,
    flat,
    frames,
    pre_recv,
    psum,
    recv1,
    eloc,
    rece,
    ecr,
    recc,
    table_hi,
    table_lo,
    back_hi,
    back_lo,
    zbuf,
    rbuf,
    abuf,
    fine_bg,
    obs_a,
    obs_b,
    fe_send,
    fe_recv,
    advbuf,
    send2,
    recv2,
    sendx,
    recvx,
    ebuf,
    ensr,
    in_sem,
    edge_rs,
    pre_rs,
    rs1,
    rse,
    rsc,
    fe_rs,
    ss2,
    rs2,
    rs2f,
    ssx,
    rsx,
    rsxf,
):
    n, nb, lev, rows, lon, fine_rows, fine_cols, scale = cfg
    block = lon // n
    frame = block + 2
    ratio = fine_cols // block
    main = lev * rows
    tiles = lon // LANES
    ng = fine_rows // RG
    gcells = RG * fine_cols
    gl = RG * RG
    levp = RG
    xs = recvx.shape[0]
    me = lax.axis_index("mem")
    band = lax.axis_index("band")
    has_up = band > 0
    has_down = band < nb - 1
    has = (has_up, has_down)
    wv, ws = lon_weights(ratio)

    barrier = pltpu.get_barrier_semaphore()

    core = lax.rem(me, 2)
    chip = me // 2
    partner = me + 1 - 2 * core
    chips = n // 2
    far_first, classes, ring, rest = chip_order(chips)
    ring_at, rest_at = chip // rest, lax.rem(chip, rest)

    def to_chip(step):
        return lax.rem(ring_at + step[0], ring) * rest + lax.rem(rest_at + step[1], rest)

    def from_chip(step):
        return to_chip(((ring - step[0]) % ring, (rest - step[1]) % rest))

    side_band = (band - 1, band + 1)
    for step in far_first:
        home = step == (0, 0)
        for c in (core, 1 - core):
            if nb == 2:
                pl.semaphore_signal(barrier, inc=1, device_id={"mem": 2 * to_chip(step) + c, "band": 1 - band})
            else:
                for side in (0, 1):

                    @pl.when(has[side])
                    def _():
                        pl.semaphore_signal(
                            barrier, inc=1, device_id={"mem": 2 * to_chip(step) + c, "band": side_band[side]}
                        )

            if not (home and c is core):
                pl.semaphore_signal(barrier, inc=1, device_id={"mem": 2 * to_chip(step) + c})

    loads = [
        pltpu.make_async_copy(src, dst, in_sem.at[i])
        for i, (src, dst) in enumerate(
            (
                (alpha_hbm, alpha),
                (ens_hbm, ens_in),
                (bg_hbm, bg),
                (low_hbm, low),
                (wt_hbm, wt),
                (cell_hbm, cell),
                (val_hbm, val),
                (prec_hbm, prec),
            )
        )
    ]
    for c in loads:
        c.start()

    part[main:, :] = jnp.zeros((part.shape[0] - main, lon), f32)
    xpart[...] = jnp.zeros(xpart.shape, f32)
    edge_send[...] = jnp.zeros(edge_send.shape, f32)
    fe_send[...] = jnp.zeros(fe_send.shape, f32)

    loads[0].wait()
    loads[1].wait()

    def whole(ref):
        parts = [ref[t] for t in range(tiles)]
        return parts[0] if tiles == 1 else jnp.concatenate(parts, axis=1)

    def row(ref, k):
        parts = [ref.at[t][pl.ds(k, lev, stride=rows), :] for t in range(tiles)]
        return parts[0] if tiles == 1 else jnp.concatenate(parts, axis=1)

    for t in range(tiles):
        ensf[t] = ens_in[t].astype(f32)
    al = whole(alpha)
    en = whole(ensf)
    kk = iota((main, lon), 0) % rows
    a_up = jnp.where(kk == 0, 0.0, pltpu.roll(al, 1, 0))
    a_dn = jnp.where(kk == rows - 1, 0.0, pltpu.roll(al, main - 1, 0))
    z = smooth_lon(0.25 * (a_up + a_dn) + 0.5 * al) * en * scale
    for t in range(tiles):
        plain[t] = z[:, t * LANES : (t + 1) * LANES]
    part[0:main, :] = z
    edges = []
    for side, k in ((0, 0), (1, rows - 1)):
        a_edge = smooth_lon(row(alpha, k)) * (0.25 * scale)
        e_edge = row(ensf, k)
        edges.append((a_edge, e_edge, row(plain, k)))
        edge_send[side, 0:lev, :] = e_edge
        at = main + side * 2 * levp
        for i, v in enumerate((a_edge, e_edge) if side == 0 else (e_edge, a_edge)):
            part[at + i * levp : at + i * levp + lev, :] = v
    (a_0, e_0, p_0), (a_1, e_1, p_1) = edges
    zero = jnp.zeros_like(a_0)
    sets_up = [zero, p_0, a_0, e_0]
    sets_down = [e_1, a_1, p_1, zero]
    if xs == 1:
        sets = [jnp.where(has_up, u, d) for u, d in zip(sets_up, sets_down)]
    else:
        sets = sets_up + sets_down
    for i, v in enumerate(sets):
        xpart[i * levp : i * levp + lev, :] = v

    def lay(g, rows_of):
        rows_of = pltpu.roll(rows_of, 1, 1)
        for t in range(tiles):
            flat[g, t * LANES : (t + 1) * LANES, :] = rows_of[:, t * LANES : (t + 1) * LANES].T
        flat[g, lon : lon + SUB, :] = flat[g, 0:SUB, :]

    lay(0, part[0:LANES, :])
    lay(1, part[LANES : 2 * LANES, :])
    lay(2, xpart[...])

    lane8 = iota((SUB, LANES), 1)
    row8 = iota((SUB, LANES), 0)
    low_half = lane8 < LANES // 2
    half = LANES // 2

    def tile_of(g, d):
        return flat[g, d * SUB : (d + 1) * SUB, :]

    def views(d):
        v, x = tile_of(1, d), tile_of(2, d)
        flip, flipx = pltpu.roll(v, half, 1), pltpu.roll(x, half, 1)
        return v, flip, x, flipx, pltpu.roll(flip, 5, 0), pltpu.roll(v, 3, 0), pltpu.roll(flipx, 3, 0), pltpu.roll(x, 3, 0)

    cur = views(0)
    for d in range(n):
        nxt = views(d + 1)
        v, flip, x, flipx, r5, v3, fx3, x3 = cur
        packed = jnp.where(low_half, pltpu.roll(v, 2, 0), jnp.where(row8 < 5, r5, nxt[4]))
        frames[d // 2, d % 2, 0:SUB, :] = tile_of(0, d)
        frames[d // 2, d % 2, SUB : 2 * SUB, :] = jnp.where(row8 < 2, tile_of(0, d + 1), packed)
        eloc[d] = jnp.where(low_half, flip, jnp.where(row8 < 3, v3, nxt[5]))
        ecr[0, d] = jnp.where(low_half, x, jnp.where(row8 < 3, fx3, nxt[6]))
        if xs == 2:
            ecr[1, d] = jnp.where(low_half, flipx, jnp.where(row8 < 3, x3, nxt[7]))
        cur = nxt

    loads[2].wait()
    row32 = iota((4 * SUB, gcells), 0)
    col_of = jnp.where(row32 < ratio * SUB, (row32 % SUB) * ratio + row32 // SUB, -1)
    pick = (iota((4 * SUB, gcells), 1) % fine_cols == col_of).astype(f32).astype(bf16)
    pick2 = jnp.concatenate([pick, pick], axis=1)
    in_row = iota((RG, gcells), 1) // fine_cols == iota((RG, gcells), 0)
    zbuf[main:, :] = jnp.zeros((gl - main, 2 * gcells), bf16)
    back = bg[:, 0, :]
    for g in range(ng):
        hi, lo = split2f(back[:, g * gcells : (g + 1) * gcells])
        for l in range(lev):
            at = slice(l * RG, (l + 1) * RG)
            zbuf[at, 0:gcells] = jnp.where(in_row, jnp.broadcast_to(hi[l : l + 1], (RG, gcells)), 0.0).astype(bf16)
            zbuf[at, gcells : 2 * gcells] = jnp.where(in_row, jnp.broadcast_to(lo[l : l + 1], (RG, gcells)), 0.0).astype(bf16)
        fine_bg[:, g * gl : (g + 1) * gl] = dims(pick2, zbuf[...], 1, 1)
    for c in loads[3:]:
        c.wait()

    if nb == 2:
        pl.semaphore_wait(barrier, 2 * n - 1)
    else:
        pl.semaphore_wait(barrier, n - 1 + n * (has_up.astype(jnp.int32) + has_down.astype(jnp.int32)))

    pre_copy = pltpu.make_async_remote_copy(
        src_ref=frames.at[:, 1 - core],
        dst_ref=pre_recv,
        send_sem=in_sem.at[0],
        recv_sem=pre_rs,
        device_id={"mem": partner},
    )
    pre_copy.start()
    packed_rows = frame // 2

    def copyc(side, dst):
        i = 0 if xs == 1 else 1 - side
        return pltpu.make_async_remote_copy(
            src_ref=ecr.at[0 if xs == 1 else side, dst, pl.ds(0, packed_rows), :],
            dst_ref=recc.at[i, me, pl.ds(0, packed_rows), :],
            send_sem=in_sem.at[2 + side],
            recv_sem=rsc.at[i],
            device_id={"mem": dst, "band": side_band[side]},
        )

    def copye(dst):
        return pltpu.make_async_remote_copy(
            src_ref=eloc.at[dst, pl.ds(0, packed_rows), :],
            dst_ref=rece.at[me, pl.ds(0, packed_rows), :],
            send_sem=in_sem.at[1],
            recv_sem=rse,
            device_id={"mem": dst},
        )

    def edge_copy(side):
        return pltpu.make_async_remote_copy(
            src_ref=edge_send.at[side],
            dst_ref=edge_recv.at[1 - side],
            send_sem=in_sem.at[6 + side],
            recv_sem=edge_rs.at[0 if xs == 1 else 1 - side],
            device_id={"band": side_band[side]},
        )

    for side in (0, 1):

        @pl.when(has[side])
        def _():
            for step in far_first:
                for c in (core, 1 - core):
                    copyc(side, 2 * to_chip(step) + c).start()

        @pl.when(jnp.logical_not(has[side]))
        def _():
            edge_recv[side] = jnp.zeros(edge_recv.shape[1:], f32)

    for step in far_first:
        for c in (core, 1 - core):
            if step != (0, 0) or c is not core:
                copye(2 * to_chip(step) + c).start()
    for side in (0, 1):

        @pl.when(has[side])
        def _():
            edge_copy(side).start()

    rece[me] = eloc[me]

    first = fine_bg[0:1, :]
    last = fine_bg[ratio * SUB - 1 : ratio * SUB, :]
    for t in range(ng * gl // LANES):
        fe_send[0, t : t + 1, :] = first[:, t * LANES : (t + 1) * LANES]
        fe_send[1, t : t + 1, :] = last[:, t * LANES : (t + 1) * LANES]

    def fe_copy(side):
        return pltpu.make_async_remote_copy(
            src_ref=fe_send.at[side],
            dst_ref=fe_recv.at[1 - side],
            send_sem=in_sem.at[5],
            recv_sem=fe_rs,
            device_id={"mem": lax.rem(me + (n - 1 if side == 0 else 1), n)},
        )

    fe_copy(0).start()
    fe_copy(1).start()

    lane = iota((SUB, LANES), 1)
    wide = ng * gl

    def per_row(v):
        v = jnp.concatenate([v, jnp.zeros((1, LANES - fine_rows), f32)], axis=1)
        return jnp.broadcast_to(v, (SUB, LANES))

    def tiled(v, g):
        r = v if g == 0 else pltpu.roll(v, LANES - g * RG, 1)
        r = jnp.where(lane < RG, r, 0.0)
        for s in (RG, 2 * RG, 4 * RG):
            r = r + pltpu.roll(r, s, 1)
        return jnp.concatenate([r, r], axis=0)

    low_rows, wt_rows = per_row(low[...].astype(f32)), per_row(wt[...])
    down = lambda v: jnp.concatenate([v] * (LANES // SUB), axis=0).T
    low_col, wt_col = down(low_rows), down(wt_rows)
    lane16 = iota((RG, LANES), 1)
    row16 = iota((RG, LANES), 0)
    lev_of = lane16 // RG
    set_rows = (-1, 0, rows - 1, rows)
    table_hi[...] = jnp.zeros(table_hi.shape, bf16)
    table_lo[...] = jnp.zeros(table_lo.shape, bf16)
    back_hi[...] = jnp.zeros(back_hi.shape, bf16)
    back_lo[...] = jnp.zeros(back_lo.shape, bf16)
    halves = gl // LANES
    per = LANES // RG

    def weigh(k, lo_k, w):
        w_hi, w_lo = split2f(w)
        o_hi, o_lo = split2f(1.0 - w)
        m0, m1 = k == lo_k, k == lo_k + 1.0
        return (
            jnp.where(m0, o_hi, jnp.where(m1, w_hi, 0.0)),
            jnp.where(m0, o_lo, jnp.where(m1, w_lo, 0.0)),
        )

    def put(ref, r, c, v, keep):
        ref[r : r + RG, c : c + LANES] = jnp.where(keep, v, 0.0).astype(bf16)

    for g in range(ng):
        lo_t, w_t = tiled(low_rows, g), tiled(wt_rows, g)
        main_t = weigh(row16.astype(f32), lo_t, w_t)
        set_t = [weigh(jnp.full((RG, LANES), float(k), f32), lo_t, w_t) for k in set_rows]
        for ref, which in ((table_hi, 0), (table_lo, 1)):
            for l in range(lev):
                put(ref, l * RG, g * gl + l // per * LANES, main_t[which], lev_of == l % per)
            for s in range(4):
                for h in range(halves):
                    put(ref, main + s * levp, g * gl + h * LANES, set_t[s][which], (row16 == lev_of + h * per) & (row16 < lev))
        lo_c, w_c = low_col[g * RG : (g + 1) * RG], wt_col[g * RG : (g + 1) * RG]
        for h in range(halves):
            kap = lane16 + h * LANES
            e = kap - main
            es = e // levp
            ek = jnp.where(es == 0, -1, jnp.where(es == 1, 0, jnp.where(es == 2, rows - 1, rows)))
            k_of = jnp.where(e < 0, kap % rows, ek).astype(f32)
            l_of = jnp.where(e < 0, kap // rows, e % levp)
            back_t = weigh(k_of, lo_c, w_c)
            for ref, which in ((back_hi, 0), (back_lo, 1)):
                for l in range(lev):
                    if (h + 1) * LANES > main or l // per == h:
                        put(ref, g * gl + l * RG, h * LANES, back_t[which], l_of == l)

    pre_copy.wait_recv()
    for j in range(n // 2):
        psum[j] = frames[j, core] + pre_recv[j]

    used = frame + packed_rows

    def copy1(dst):
        return pltpu.make_async_remote_copy(
            src_ref=psum.at[dst, pl.ds(0, used), :],
            dst_ref=recv1.at[chip, pl.ds(0, used), :],
            send_sem=in_sem.at[4],
            recv_sem=rs1,
            device_id={"mem": 2 * dst + core},
        )

    for step in far_first[:-1]:
        copy1(to_chip(step)).start()
    recv1[chip] = psum[chip]

    nobs = cell.shape[1]
    crow = cell[...] // fine_cols
    ccol = cell[...] % fine_cols
    r32 = iota((4 * SUB, nobs), 0)
    col_o = jnp.where(r32 < ratio * SUB, (r32 % SUB) * ratio + r32 // SUB, -1)
    hot = (col_o == ccol).astype(f32).astype(bf16)
    hot2 = jnp.concatenate([hot, hot], axis=1)
    pr = prec[...]
    p_hi, p_lo = split2f(pr)
    v_hi, v_lo = split2f(val[:, 0, :] * pr)
    rbuf[main:, :] = jnp.zeros((gl - main, 2 * nobs), bf16)
    for g in range(ng):
        at_row = iota((RG, nobs), 0) + g * RG == crow
        for l in range(lev):
            at = slice(l * RG, (l + 1) * RG)
            rbuf[at, 0:nobs] = jnp.where(at_row, jnp.broadcast_to(v_hi[l : l + 1], (RG, nobs)), 0.0).astype(bf16)
            rbuf[at, nobs : 2 * nobs] = jnp.where(at_row, jnp.broadcast_to(v_lo[l : l + 1], (RG, nobs)), 0.0).astype(bf16)
        obs_b[:, g * gl : (g + 1) * gl] = dims(hot2, rbuf[...], 1, 1)
        ph = jnp.where(at_row, jnp.broadcast_to(p_hi, (RG, nobs)), 0.0).astype(bf16)
        plo = jnp.where(at_row, jnp.broadcast_to(p_lo, (RG, nobs)), 0.0).astype(bf16)
        for j in range(LANES // RG):
            abuf[j * RG : (j + 1) * RG, 0:nobs] = ph
            abuf[j * RG : (j + 1) * RG, nobs : 2 * nobs] = plo
        oa = dims(hot2, abuf[...], 1, 1)
        for j in range(gl // LANES):
            obs_a[:, g * gl + j * LANES : g * gl + (j + 1) * LANES] = oa

    pltpu.make_async_copy(fe_recv, fe_recv, fe_rs).wait()
    nt = wide // LANES
    left = jnp.concatenate([fe_recv[0, t : t + 1, :] for t in range(nt)], axis=1)
    right = jnp.concatenate([fe_recv[1, t : t + 1, :] for t in range(nt)], axis=1)
    fb = [fine_bg[b * SUB : (b + 1) * SUB, :] for b in range(ratio)]
    arow = iota((SUB, wide), 0)
    before0 = jnp.where(arow == 0, left, pltpu.roll(fb[ratio - 1], 1, 0))
    after_last = jnp.where(arow == SUB - 1, right, pltpu.roll(fb[0], SUB - 1, 0))
    chain = [before0] + fb + [after_last]
    slope_bg = [0.5 * (chain[b + 2] - chain[b]) for b in range(ratio)]

    def all_of(ref, count, height, sem):
        got = ref.at[pl.ds(0, count), pl.ds(0, height), :]
        pltpu.make_async_copy(got, got, sem).wait()

    all_of(rece, n - 1, packed_rows, rse)
    for side in (0, 1):

        @pl.when(has[side])
        def _():
            i = 0 if xs == 1 else side
            all_of(recc.at[i], n, packed_rows, rsc.at[i])

    prods, plains = [], []
    for i in range(xs):
        prod = rece[0] * recc[i, 0]
        only = recc[i, 0]
        for s in range(1, n):
            prod = prod + rece[s] * recc[i, s]
            only = only + recc[i, s]
        prods.append(prod)
        plains.append(only)
    set_of = (lane8 % half) // levp
    edge_sum = jnp.where(
        set_of < 2, jnp.where(has_up, prods[0], 0.0), jnp.where(has_down, prods[-1], 0.0)
    )
    from_up = jnp.where(has_up, pltpu.roll(plains[0], LANES - 2 * levp, 1), 0.0)
    from_down = jnp.where(has_down, pltpu.roll(plains[-1], 2 * levp, 1), 0.0)
    edge_sum = edge_sum + jnp.where(set_of == 0, from_up, jnp.where(set_of == 3, from_down, 0.0))
    edge_a = pltpu.roll(edge_sum, half, 1)
    edge_b = pltpu.roll(edge_sum, 5, 0)

    all_of(recv1, n // 2 - 1, used, rs1)
    total = recv1[0]
    for s in range(1, n // 2):
        total = total + recv1[s]
    m = total[SUB:]
    m_a = pltpu.roll(m, SUB - 2, 0)
    m_b = pltpu.roll(pltpu.roll(m, half, 1), 3, 0)
    x_a = jnp.where(low_half, m_a, edge_a)
    x_b = jnp.where(low_half, m_b, edge_b)
    x = jnp.concatenate([total, jnp.concatenate([jnp.where(row8 < 5, x_a, x_b), x_b], axis=0)], axis=1)
    x_hi, x_lo = split2f(x)
    x2 = jnp.concatenate([x_hi, x_lo], axis=0).astype(bf16)
    y = dims(x2, table_hi[...], 1, 0)
    y = y[0:16] + y[16:32] + dims(x_hi.astype(bf16), table_lo[...], 1, 0)
    taps = [y[0:SUB]] + [pltpu.roll(y, 2 * SUB - d, 0)[0:SUB] for d in (1, 2)]

    us, vs, moved = [], [], []
    for b in range(ratio):
        state = fb[b] + combine(wv[b], taps)
        slope = slope_bg[b] + combine(ws[b], taps)
        factor = 1.0 - advect_rate * slope
        mv = state * factor
        at = slice(b * SUB, (b + 1) * SUB)
        cot = obs_a[at, :] * mv - obs_b[at, :]
        us.append(cot * factor)
        vs.append((-advect_rate) * (state * cot))
        moved.append(mv)
    gl_v = None
    for d in range(3):
        t = combine([wv[b][d] for b in range(ratio)] + [ws[b][d] for b in range(ratio)], us + vs)
        t = jnp.concatenate([t, jnp.zeros_like(t)], axis=0)
        gl_v = t if d == 0 else gl_v + pltpu.roll(t, d, 0)
    g_hi, g_lo = split2f(gl_v)
    g2 = jnp.concatenate([g_hi, g_lo], axis=0).astype(bf16)
    gr = dims(g2, back_hi[...], 1, 0)
    gr = gr[0:16] + gr[16:32] + dims(g_hi.astype(bf16), back_lo[...], 1, 0)
    for g in (0, 1):
        send2[g] = gr[:, g * LANES : (g + 1) * LANES]
    def slot2(src):
        return recv2.at[src, :, pl.ds(0, frame), :]

    def copy2(dst, sem):
        return pltpu.make_async_remote_copy(
            src_ref=send2.at[:, pl.ds(0, frame), :],
            dst_ref=slot2(me),
            send_sem=ss2,
            recv_sem=sem,
            device_id={"mem": dst},
        )

    def forward2(src):
        return pltpu.make_async_remote_copy(
            src_ref=slot2(src),
            dst_ref=slot2(src),
            send_sem=ss2,
            recv_sem=rs2f,
            device_id={"mem": partner},
        )

    def copyx(side, dst):
        i = 0 if xs == 1 else 1 - side
        return pltpu.make_async_remote_copy(
            src_ref=sendx.at[0 if xs == 1 else side, pl.ds(0, packed_rows), :],
            dst_ref=recvx.at[i, core, chip, pl.ds(0, packed_rows), :],
            send_sem=ssx.at[0 if xs == 1 else side],
            recv_sem=rsx.at[i],
            device_id={"mem": dst, "band": side_band[side]},
        )

    def forwardx(i):
        got = recvx.at[i, core, :, pl.ds(0, packed_rows), :]
        return pltpu.make_async_remote_copy(
            src_ref=got,
            dst_ref=got,
            send_sem=ssx.at[xs + i],
            recv_sem=rsxf.at[i],
            device_id={"mem": partner},
        )

    for i, group in enumerate(classes):
        for step in group:
            copy2(2 * to_chip(step) + core, rs2.at[len(classes) - 1 - i]).start()
    v0, v1 = gr[0:SUB, LANES:], gr[SUB:, LANES:]
    quarter = lane8 // (2 * levp)
    v32, v96, w32, w96 = (pltpu.roll(v, r, 1) for v in (v0, v1) for r in (2 * levp, 6 * levp))

    def late(a, b):
        return jnp.where(row8 < 3, pltpu.roll(a, 3, 0), pltpu.roll(b, 3, 0))

    def pack_for(up_there):
        near = jnp.where(up_there, v32, v96)
        rest_cols = late(jnp.where(up_there, v96, v32), jnp.where(up_there, w96, w32))
        q = jnp.where(up_there, quarter - 1, quarter)
        return jnp.where(q == 2, near, jnp.where(q == 0, rest_cols, 0.0))

    if xs == 1:
        sendx[0] = pack_for(has_up)
    else:
        for side in (0, 1):
            sendx[side] = pack_for(side == 0)

    for side in (0, 1):

        @pl.when(has[side])
        def _():
            for step in far_first:
                copyx(side, 2 * to_chip(step) + core).start()

    copy2(partner, rs2f).start()
    for g in (0, 1):
        recv2[me, g] = send2[g]

    advbuf[...] = jnp.concatenate(moved + [jnp.zeros((SUB, wide), f32)], axis=0)
    pickt = jnp.concatenate([pick, pick], axis=0)
    for g in range(ng):
        hi, lo = split2(advbuf[:, g * gl : g * gl + main])
        e = dims(jnp.concatenate([hi, lo], axis=0), pickt, 0, 0)
        for l in range(lev):
            v = jnp.where(in_row, e[l * RG : (l + 1) * RG], 0.0)
            adv_ref[l, :, g * gcells : (g + 1) * gcells] = jnp.sum(v, axis=0, keepdims=True)

    def sent_edges():
        pre_copy.wait_send()
        all_of(rece, n - 1, packed_rows, in_sem.at[1])
        all_of(recv1, n // 2 - 1, used, in_sem.at[4])
        pltpu.make_async_copy(fe_recv, fe_recv, in_sem.at[5]).wait()
        for side in (0, 1):

            @pl.when(has[side])
            def _():
                all_of(recc.at[0], n, packed_rows, in_sem.at[2 + side])
                edge_copy(side).wait_send()
                pltpu.make_async_copy(edge_recv.at[side], edge_recv.at[side], edge_rs.at[0 if xs == 1 else side]).wait()

    sent_edges()
    def all_2(count, sem):
        got = recv2.at[pl.ds(0, count), :, pl.ds(0, frame), :]
        pltpu.make_async_copy(got, got, sem).wait()

    ensr[...] = pltpu.roll(whole(ensf), 1, 1) * scale
    ebuf[...] = jnp.zeros(ebuf.shape, f32)
    edge_ens = [pltpu.roll(row(ensf, k), 1, 1) * scale for k in (0, rows - 1)]
    halo_ens = [pltpu.roll(edge_recv[side, 0:lev, :], 1, 1) * scale for side in (0, 1)]

    def smooth_back(v):
        return 0.25 * v + 0.5 * pltpu.roll(v, lon - 1, 1) + 0.25 * pltpu.roll(v, lon - 2, 1)

    for i, group in enumerate(reversed(classes)):
        all_2(len(group), rs2.at[i])
        for step in group:
            forward2(2 * from_chip(step) + core).start()
    for side in (0, 1):

        @pl.when(has[side])
        def _():
            i = 0 if xs == 1 else side
            pltpu.make_async_copy(recvx.at[i, core, :, pl.ds(0, packed_rows), :], recvx.at[i, core, :, pl.ds(0, packed_rows), :], rsx.at[i]).wait()
            forwardx(i).start()

    all_2(n // 2, rs2f)

    over = iota((SUB, LANES), 0) < frame - block

    def across(parts):
        per_tile = LANES // SUB
        cols = [jnp.concatenate(parts[t * per_tile : (t + 1) * per_tile], axis=0).T for t in range(tiles)]
        return cols[0] if tiles == 1 else jnp.concatenate(cols, axis=1)

    ours = (quarter < 2) | (set_of == 0) | (set_of == 3)
    set_lanes = lane8 >= half

    def edges_at(i, d):
        e = recvx[i, d % 2, d // 2]
        b = pltpu.roll(pltpu.roll(e, half, 1), 5, 0)
        return jnp.where(row8 < 5, e, b), jnp.where(over, b, 0.0)

    def gather(g):
        sides = range(xs) if g else ()
        prev = [edges_at(i, n - 1)[1] for i in sides]
        parts = []
        for d in range(n):
            tile = recv2[d, g, 0:SUB, :] + jnp.where(over, recv2[(d - 1) % n, g, SUB : 2 * SUB, :], 0.0)
            if g:
                theirs = None
                for i in sides:
                    here, tail = edges_at(i, d)
                    v = here + prev[i]
                    if xs == 2:
                        v = jnp.where(has[i], v, 0.0)
                    theirs = v if theirs is None else theirs + v
                    prev[i] = tail
                tile = jnp.where(ours, tile, 0.0) + jnp.where(set_lanes, theirs, 0.0)
            parts.append(tile)
        return across(parts)

    c0 = gather(0)
    for side in (0, 1):

        @pl.when(has[side])
        def _():
            i = 0 if xs == 1 else side
            all_of(recvx.at[i, 0], n // 2, packed_rows, rsxf.at[i])

    c1 = gather(1)
    e0 = main - LANES
    for side, k, k_in in ((0, 0, 1), (1, rows - 1, rows - 2)):
        halo_at, extra_at = (e0, e0 + levp) if side == 0 else (e0 + 3 * levp, e0 + 2 * levp)
        we = edge_ens[side] * c1[extra_at : extra_at + lev]
        wh = halo_ens[side] * c1[halo_at : halo_at + lev]
        for at, v in ((k, 0.5 * we + 0.25 * wh), (k_in, 0.25 * we)):
            for t in range(tiles):
                ebuf.at[t][pl.ds(at, lev, stride=rows), :] = v[:, t * LANES : (t + 1) * LANES]
    wm = ensr[...] * jnp.concatenate([c0, c1[0:e0]], axis=0)
    w_up = jnp.where(kk == 0, 0.0, pltpu.roll(wm, 1, 0))
    w_dn = jnp.where(kk == rows - 1, 0.0, pltpu.roll(wm, main - 1, 0))
    zz = smooth_back(0.25 * (w_up + w_dn) + 0.5 * wm + whole(ebuf))
    for t in range(tiles):
        grad_ref[t] = zz[:, t * LANES : (t + 1) * LANES]

    for side in (0, 1):

        @pl.when(has[side])
        def _():
            i = 0 if xs == 1 else side
            all_of(recvx.at[0, 0], n // 2, packed_rows, ssx.at[i])
            all_of(recvx.at[0, 0], n // 2, packed_rows, ssx.at[xs + i])

    all_2(n - 1, ss2)


def writer(adv_ref, grad_ref, adv_out, grad_out, sem):
    copies = [
        pltpu.make_async_copy(grad_ref, grad_out, sem.at[0]),
        pltpu.make_async_copy(adv_ref, adv_out, sem.at[1]),
    ]
    for c in copies:
        c.start()
    for c in copies:
        c.wait()


def up_to(x, m):
    return -(-x // m) * m


def to_tiles(x):
    return x.reshape(-1, x.shape[3] // LANES, LANES).swapaxes(0, 1)


def shards(ensemble, alpha, lat_lower, lat_weight, background, obs_cell, obs_value, obs_precision):
    n, nb = lax.axis_size("mem"), lax.axis_size("band")
    members, lev, rows, lon = ensemble.shape
    fine_rows = lat_lower.shape[0]
    cells = background.shape[2]
    nobs = obs_cell.shape[1]
    fine_cols = cells // fine_rows
    scale = 1.0 / math.sqrt(members * n - 1)
    block = lon // n
    main = lev * rows
    kaps = main + 4 * RG
    assert n % 2 == 0 and members == 1 and block == SUB and rows == RG and lev <= RG and kaps == 2 * LANES
    assert fine_rows % RG == 0 and fine_cols % block == 0 and fine_cols // block == 3
    cfg = (n, nb, lev, rows, lon, fine_rows, fine_cols, scale)
    tiles = lon // LANES
    ng = fine_rows // RG
    gl = RG * RG
    wide = ng * gl
    gcells = RG * fine_cols
    xs = 1 if nb == 2 else 2
    dma = pltpu.SemaphoreType.DMA
    vm = pl.BlockSpec(memory_space=pltpu.VMEM)
    hbm = pl.BlockSpec(memory_space=pltpu.HBM)
    fr = 2 * SUB
    advected, gradient = pl.pallas_call(
        functools.partial(kernel, cfg),
        out_shape=(
            jax.ShapeDtypeStruct(background.shape, f32),
            jax.ShapeDtypeStruct((tiles, main, LANES), f32),
        ),
        in_specs=[hbm] * 8,
        out_specs=(vm, vm),
        scratch_shapes=[
            pltpu.VMEM((tiles, main, LANES), bf16),
            pltpu.VMEM((tiles, main, LANES), f32),
            pltpu.VMEM((1, fine_rows), jnp.int32),
            pltpu.VMEM((1, fine_rows), f32),
            pltpu.VMEM(background.shape, f32),
            pltpu.VMEM((1, nobs), jnp.int32),
            pltpu.VMEM(obs_value.shape, f32),
            pltpu.VMEM((1, nobs), f32),
            pltpu.VMEM((tiles, main, LANES), f32),
            pltpu.VMEM((tiles, main, LANES), f32),
            pltpu.VMEM((kaps, lon), f32),
            pltpu.VMEM((LANES, lon), f32),
            pltpu.VMEM((2, RG, lon), f32),
            pltpu.VMEM((2, RG, lon), f32),
            pltpu.VMEM((3, lon + SUB, LANES), f32),
            pltpu.VMEM((n // 2, 2, fr, LANES), f32),
            pltpu.VMEM((n // 2, fr, LANES), f32),
            pltpu.VMEM((n // 2, fr, LANES), f32),
            pltpu.VMEM((n // 2, fr, LANES), f32),
            pltpu.VMEM((n, SUB, LANES), f32),
            pltpu.VMEM((n, SUB, LANES), f32),
            pltpu.VMEM((xs, n, SUB, LANES), f32),
            pltpu.VMEM((xs, n, SUB, LANES), f32),
            pltpu.VMEM((kaps, wide), bf16),
            pltpu.VMEM((kaps, wide), bf16),
            pltpu.VMEM((wide, kaps), bf16),
            pltpu.VMEM((wide, kaps), bf16),
            pltpu.VMEM((gl, 2 * gcells), bf16),
            pltpu.VMEM((gl, 2 * nobs), bf16),
            pltpu.VMEM((LANES, 2 * nobs), bf16),
            pltpu.VMEM((4 * SUB, wide), f32),
            pltpu.VMEM((4 * SUB, wide), f32),
            pltpu.VMEM((4 * SUB, wide), f32),
            pltpu.VMEM((2, SUB, LANES), f32),
            pltpu.VMEM((2, SUB, LANES), f32),
            pltpu.VMEM((4 * SUB, wide), f32),
            pltpu.VMEM((2, fr, LANES), f32),
            pltpu.VMEM((n, 2, fr, LANES), f32),
            pltpu.VMEM((xs, SUB, LANES), f32),
            pltpu.VMEM((xs, 2, n // 2, SUB, LANES), f32),
            pltpu.VMEM((tiles, main, LANES), f32),
            pltpu.VMEM((main, lon), f32),
            dma((8,)),
            dma((xs,)),
            dma,
            dma,
            dma,
            dma((xs,)),
            dma,
            dma,
            dma((len(chip_order(n // 2)[1]),)),
            dma,
            dma((2 * xs,)),
            dma((xs,)),
            dma((xs,)),
        ],
        compiler_params=pltpu.CompilerParams(collective_id=0, has_side_effects=True, vmem_limit_bytes=48 * 2**20),
    )(
        *(
            pltpu.with_memory_space_constraint(v, pltpu.HBM)
            for v in (
                to_tiles(ensemble),
                to_tiles(alpha),
                lat_lower.reshape(1, fine_rows),
                lat_weight.reshape(1, fine_rows),
                background,
                obs_cell,
                obs_value,
                obs_precision,
            )
        )
    )
    advected, gradient = pl.pallas_call(
        writer,
        out_shape=(
            jax.ShapeDtypeStruct(background.shape, f32),
            jax.ShapeDtypeStruct((tiles, main, LANES), f32),
        ),
        in_specs=[vm, vm],
        out_specs=(hbm, hbm),
        scratch_shapes=[dma((2,))],
        compiler_params=pltpu.CompilerParams(vmem_limit_bytes=2**20),
    )(advected, gradient)
    return advected, gradient.swapaxes(0, 1).reshape(members, lev, rows, lon)


def solution(mesh):
    return jax.shard_map(
        shards,
        mesh=mesh,
        in_specs=(
            P("mem", None, "band", None),
            P("mem", None, "band", None),
            P("band"),
            P("band"),
            P(None, ("band", "mem"), None),
            P(("band", "mem"), None),
            P(None, ("band", "mem"), None),
            P(("band", "mem"), None),
        ),
        out_specs=(P(None, ("band", "mem"), None), P("mem", None, "band", None)),
        check_vma=False,
    )
```

```python
import functools
import math

import jax
import jax.numpy as jnp
from jax import lax
from jax.experimental import pallas as pl
from jax.experimental.pallas import tpu as pltpu
from jax.sharding import PartitionSpec as P

advect_rate = 0.25
LANES = 128
SUB = 8
RG = 16
f32 = jnp.float32
bf16 = jnp.bfloat16


def split2(x):
    hi = x.astype(bf16)
    lo = (x - hi.astype(f32)).astype(bf16)
    return hi, lo


def split2f(x):
    hi = x.astype(bf16).astype(f32)
    return hi, x - hi


def dims(a, b, ca, cb):
    return lax.dot_general(a, b, (((ca,), (cb,)), ((), ())), preferred_element_type=f32)


def iota(shape, d):
    return lax.broadcasted_iota(jnp.int32, shape, d)


def smooth_lon(x):
    n = x.shape[1]
    return 0.25 * pltpu.roll(x, 1, 1) + 0.5 * x + 0.25 * pltpu.roll(x, n - 1, 1)


def lon_weights(ratio):
    def parts(shift):
        num = 2 * shift + 1 + ratio
        return num // (2 * ratio), (num % (2 * ratio)) / (2 * ratio)

    def taps(shift):
        q, f = parts(shift)
        w = [0.0, 0.0, 0.0]
        for at, v in ((q, 1.0 - f), (q + 1, f)):
            if v:
                w[at] += v
        return w

    value = [taps(b) for b in range(ratio)]
    slope = [[0.5 * (p - m) for p, m in zip(taps(b + 1), taps(b - 1))] for b in range(ratio)]
    return value, slope


def combine(weights, parts):
    out = None
    for w, p in zip(weights, parts):
        if w == 0.0:
            continue
        term = p if w == 1.0 else w * p
        out = term if out is None else out + term
    return out


def chip_order(chips):
    ring = 4 if chips % 4 == 0 else chips
    rest = chips // ring

    def hops(step):
        return min(step[0], ring - step[0]) + min(step[1], rest - step[1])

    steps = sorted(((a, b) for a in range(ring) for b in range(rest)), key=lambda s: -hops(s))
    classes = [[s for s in steps if hops(s) == h] for h in sorted({hops(s) for s in steps if hops(s)}, reverse=True)]
    return steps, classes, ring, rest


def kernel(
    cfg,
    ens_hbm,
    alpha_hbm,
    low_hbm,
    wt_hbm,
    bg_hbm,
    cell_hbm,
    val_hbm,
    prec_hbm,
    adv_ref,
    grad_ref,
    ens_in,
    alpha,
    low,
    wt,
    bg,
    cell,
    val,
    prec,
    ensf,
    plain,
    part,
    xpart,
    edge_send,
    edge_recv,
    flat,
    frames,
    pre_recv,
    psum,
    recv1,
    eloc,
    rece,
    ecr,
    recc,
    table_hi,
    table_lo,
    back_hi,
    back_lo,
    zbuf,
    rbuf,
    abuf,
    fine_bg,
    obs_a,
    obs_b,
    fe_send,
    fe_recv,
    advbuf,
    send2,
    recv2,
    sendx,
    recvx,
    ebuf,
    ensr,
    in_sem,
    edge_rs,
    pre_rs,
    rs1,
    rse,
    rsc,
    fe_rs,
    ss2,
    rs2,
    rs2f,
    ssx,
    rsx,
    rsxf,
):
    n, nb, lev, rows, lon, fine_rows, fine_cols, scale = cfg
    block = lon // n
    frame = block + 2
    ratio = fine_cols // block
    main = lev * rows
    tiles = lon // LANES
    ng = fine_rows // RG
    gcells = RG * fine_cols
    gl = RG * RG
    levp = RG
    xs = recvx.shape[0]
    me = lax.axis_index("mem")
    band = lax.axis_index("band")
    has_up = band > 0
    has_down = band < nb - 1
    has = (has_up, has_down)
    wv, ws = lon_weights(ratio)

    barrier = pltpu.get_barrier_semaphore()

    core = lax.rem(me, 2)
    chip = me // 2
    partner = me + 1 - 2 * core
    chips = n // 2
    far_first, classes, ring, rest = chip_order(chips)
    ring_at, rest_at = chip // rest, lax.rem(chip, rest)

    def to_chip(step):
        return lax.rem(ring_at + step[0], ring) * rest + lax.rem(rest_at + step[1], rest)

    def from_chip(step):
        return to_chip(((ring - step[0]) % ring, (rest - step[1]) % rest))

    side_band = (band - 1, band + 1)
    for step in far_first:
        home = step == (0, 0)
        for c in (core, 1 - core):
            if nb == 2:
                pl.semaphore_signal(barrier, inc=1, device_id={"mem": 2 * to_chip(step) + c, "band": 1 - band})
            else:
                for side in (0, 1):

                    @pl.when(has[side])
                    def _():
                        pl.semaphore_signal(
                            barrier, inc=1, device_id={"mem": 2 * to_chip(step) + c, "band": side_band[side]}
                        )

            if not (home and c is core):
                pl.semaphore_signal(barrier, inc=1, device_id={"mem": 2 * to_chip(step) + c})

    loads = [
        pltpu.make_async_copy(src, dst, in_sem.at[i])
        for i, (src, dst) in enumerate(
            (
                (alpha_hbm, alpha),
                (ens_hbm, ens_in),
                (bg_hbm, bg),
                (low_hbm, low),
                (wt_hbm, wt),
                (cell_hbm, cell),
                (val_hbm, val),
                (prec_hbm, prec),
            )
        )
    ]
    for c in loads:
        c.start()

    part[main:, :] = jnp.zeros((part.shape[0] - main, lon), f32)
    xpart[...] = jnp.zeros(xpart.shape, f32)
    edge_send[...] = jnp.zeros(edge_send.shape, f32)
    fe_send[...] = jnp.zeros(fe_send.shape, f32)

    loads[0].wait()
    loads[1].wait()

    def whole(ref):
        parts = [ref[t] for t in range(tiles)]
        return parts[0] if tiles == 1 else jnp.concatenate(parts, axis=1)

    def row(ref, k):
        parts = [ref.at[t][pl.ds(k, lev, stride=rows), :] for t in range(tiles)]
        return parts[0] if tiles == 1 else jnp.concatenate(parts, axis=1)

    for t in range(tiles):
        ensf[t] = ens_in[t].astype(f32)
    al = whole(alpha)
    en = whole(ensf)
    kk = iota((main, lon), 0) % rows
    a_up = jnp.where(kk == 0, 0.0, pltpu.roll(al, 1, 0))
    a_dn = jnp.where(kk == rows - 1, 0.0, pltpu.roll(al, main - 1, 0))
    z = smooth_lon(0.25 * (a_up + a_dn) + 0.5 * al) * en * scale
    for t in range(tiles):
        plain[t] = z[:, t * LANES : (t + 1) * LANES]
    part[0:main, :] = z
    edges = []
    for side, k in ((0, 0), (1, rows - 1)):
        a_edge = smooth_lon(row(alpha, k)) * (0.25 * scale)
        e_edge = row(ensf, k)
        edges.append((a_edge, e_edge, row(plain, k)))
        edge_send[side, 0:lev, :] = e_edge
        at = main + side * 2 * levp
        for i, v in enumerate((a_edge, e_edge) if side == 0 else (e_edge, a_edge)):
            part[at + i * levp : at + i * levp + lev, :] = v
    (a_0, e_0, p_0), (a_1, e_1, p_1) = edges
    zero = jnp.zeros_like(a_0)
    sets_up = [zero, p_0, a_0, e_0]
    sets_down = [e_1, a_1, p_1, zero]
    if xs == 1:
        sets = [jnp.where(has_up, u, d) for u, d in zip(sets_up, sets_down)]
    else:
        sets = sets_up + sets_down
    for i, v in enumerate(sets):
        xpart[i * levp : i * levp + lev, :] = v

    def lay(g, rows_of):
        rows_of = pltpu.roll(rows_of, 1, 1)
        for t in range(tiles):
            flat[g, t * LANES : (t + 1) * LANES, :] = rows_of[:, t * LANES : (t + 1) * LANES].T
        flat[g, lon : lon + SUB, :] = flat[g, 0:SUB, :]

    lay(0, part[0:LANES, :])
    lay(1, part[LANES : 2 * LANES, :])
    lay(2, xpart[...])

    lane8 = iota((SUB, LANES), 1)
    row8 = iota((SUB, LANES), 0)
    low_half = lane8 < LANES // 2
    half = LANES // 2

    def tile_of(g, d):
        return flat[g, d * SUB : (d + 1) * SUB, :]

    def views(d):
        v, x = tile_of(1, d), tile_of(2, d)
        flip, flipx = pltpu.roll(v, half, 1), pltpu.roll(x, half, 1)
        return v, flip, x, flipx, pltpu.roll(flip, 5, 0), pltpu.roll(v, 3, 0), pltpu.roll(flipx, 3, 0), pltpu.roll(x, 3, 0)

    cur = views(0)
    for d in range(n):
        nxt = views(d + 1)
        v, flip, x, flipx, r5, v3, fx3, x3 = cur
        packed = jnp.where(low_half, pltpu.roll(v, 2, 0), jnp.where(row8 < 5, r5, nxt[4]))
        frames[d // 2, d % 2, 0:SUB, :] = tile_of(0, d)
        frames[d // 2, d % 2, SUB : 2 * SUB, :] = jnp.where(row8 < 2, tile_of(0, d + 1), packed)
        eloc[d] = jnp.where(low_half, flip, jnp.where(row8 < 3, v3, nxt[5]))
        ecr[0, d] = jnp.where(low_half, x, jnp.where(row8 < 3, fx3, nxt[6]))
        if xs == 2:
            ecr[1, d] = jnp.where(low_half, flipx, jnp.where(row8 < 3, x3, nxt[7]))
        cur = nxt

    loads[2].wait()
    row32 = iota((4 * SUB, gcells), 0)
    col_of = jnp.where(row32 < ratio * SUB, (row32 % SUB) * ratio + row32 // SUB, -1)
    pick = (iota((4 * SUB, gcells), 1) % fine_cols == col_of).astype(f32).astype(bf16)
    pick2 = jnp.concatenate([pick, pick], axis=1)
    in_row = iota((RG, gcells), 1) // fine_cols == iota((RG, gcells), 0)
    zbuf[main:, :] = jnp.zeros((gl - main, 2 * gcells), bf16)
    back = bg[:, 0, :]
    for g in range(ng):
        hi, lo = split2f(back[:, g * gcells : (g + 1) * gcells])
        for l in range(lev):
            at = slice(l * RG, (l + 1) * RG)
            zbuf[at, 0:gcells] = jnp.where(in_row, jnp.broadcast_to(hi[l : l + 1], (RG, gcells)), 0.0).astype(bf16)
            zbuf[at, gcells : 2 * gcells] = jnp.where(in_row, jnp.broadcast_to(lo[l : l + 1], (RG, gcells)), 0.0).astype(bf16)
        fine_bg[:, g * gl : (g + 1) * gl] = dims(pick2, zbuf[...], 1, 1)
    for c in loads[3:]:
        c.wait()

    if nb == 2:
        pl.semaphore_wait(barrier, 2 * n - 1)
    else:
        pl.semaphore_wait(barrier, n - 1 + n * (has_up.astype(jnp.int32) + has_down.astype(jnp.int32)))

    pre_copy = pltpu.make_async_remote_copy(
        src_ref=frames.at[:, 1 - core],
        dst_ref=pre_recv,
        send_sem=in_sem.at[0],
        recv_sem=pre_rs,
        device_id={"mem": partner},
    )
    pre_copy.start()
    packed_rows = frame // 2

    def copyc(side, dst):
        i = 0 if xs == 1 else 1 - side
        return pltpu.make_async_remote_copy(
            src_ref=ecr.at[0 if xs == 1 else side, dst, pl.ds(0, packed_rows), :],
            dst_ref=recc.at[i, me, pl.ds(0, packed_rows), :],
            send_sem=in_sem.at[2 + side],
            recv_sem=rsc.at[i],
            device_id={"mem": dst, "band": side_band[side]},
        )

    def copye(dst):
        return pltpu.make_async_remote_copy(
            src_ref=eloc.at[dst, pl.ds(0, packed_rows), :],
            dst_ref=rece.at[me, pl.ds(0, packed_rows), :],
            send_sem=in_sem.at[1],
            recv_sem=rse,
            device_id={"mem": dst},
        )

    def edge_copy(side):
        return pltpu.make_async_remote_copy(
            src_ref=edge_send.at[side],
            dst_ref=edge_recv.at[1 - side],
            send_sem=in_sem.at[6 + side],
            recv_sem=edge_rs.at[0 if xs == 1 else 1 - side],
            device_id={"band": side_band[side]},
        )

    for side in (0, 1):

        @pl.when(has[side])
        def _():
            for step in far_first:
                for c in (core, 1 - core):
                    copyc(side, 2 * to_chip(step) + c).start()

        @pl.when(jnp.logical_not(has[side]))
        def _():
            edge_recv[side] = jnp.zeros(edge_recv.shape[1:], f32)

    for step in far_first:
        for c in (core, 1 - core):
            if step != (0, 0) or c is not core:
                copye(2 * to_chip(step) + c).start()
    for side in (0, 1):

        @pl.when(has[side])
        def _():
            edge_copy(side).start()

    rece[me] = eloc[me]

    first = fine_bg[0:1, :]
    last = fine_bg[ratio * SUB - 1 : ratio * SUB, :]
    for t in range(ng * gl // LANES):
        fe_send[0, t : t + 1, :] = first[:, t * LANES : (t + 1) * LANES]
        fe_send[1, t : t + 1, :] = last[:, t * LANES : (t + 1) * LANES]

    def fe_copy(side):
        return pltpu.make_async_remote_copy(
            src_ref=fe_send.at[side],
            dst_ref=fe_recv.at[1 - side],
            send_sem=in_sem.at[5],
            recv_sem=fe_rs,
            device_id={"mem": lax.rem(me + (n - 1 if side == 0 else 1), n)},
        )

    fe_copy(0).start()
    fe_copy(1).start()

    lane = iota((SUB, LANES), 1)
    wide = ng * gl

    def per_row(v):
        v = jnp.concatenate([v, jnp.zeros((1, LANES - fine_rows), f32)], axis=1)
        return jnp.broadcast_to(v, (SUB, LANES))

    def tiled(v, g):
        r = v if g == 0 else pltpu.roll(v, LANES - g * RG, 1)
        r = jnp.where(lane < RG, r, 0.0)
        for s in (RG, 2 * RG, 4 * RG):
            r = r + pltpu.roll(r, s, 1)
        return jnp.concatenate([r, r], axis=0)

    low_rows, wt_rows = per_row(low[...].astype(f32)), per_row(wt[...])
    down = lambda v: jnp.concatenate([v] * (LANES // SUB), axis=0).T
    low_col, wt_col = down(low_rows), down(wt_rows)
    lane16 = iota((RG, LANES), 1)
    row16 = iota((RG, LANES), 0)
    lev_of = lane16 // RG
    set_rows = (-1, 0, rows - 1, rows)
    table_hi[...] = jnp.zeros(table_hi.shape, bf16)
    table_lo[...] = jnp.zeros(table_lo.shape, bf16)
    back_hi[...] = jnp.zeros(back_hi.shape, bf16)
    back_lo[...] = jnp.zeros(back_lo.shape, bf16)
    halves = gl // LANES
    per = LANES // RG

    def weigh(k, lo_k, w):
        w_hi, w_lo = split2f(w)
        o_hi, o_lo = split2f(1.0 - w)
        m0, m1 = k == lo_k, k == lo_k + 1.0
        return (
            jnp.where(m0, o_hi, jnp.where(m1, w_hi, 0.0)),
            jnp.where(m0, o_lo, jnp.where(m1, w_lo, 0.0)),
        )

    def put(ref, r, c, v, keep):
        ref[r : r + RG, c : c + LANES] = jnp.where(keep, v, 0.0).astype(bf16)

    for g in range(ng):
        lo_t, w_t = tiled(low_rows, g), tiled(wt_rows, g)
        main_t = weigh(row16.astype(f32), lo_t, w_t)
        set_t = [weigh(jnp.full((RG, LANES), float(k), f32), lo_t, w_t) for k in set_rows]
        for ref, which in ((table_hi, 0), (table_lo, 1)):
            for l in range(lev):
                put(ref, l * RG, g * gl + l // per * LANES, main_t[which], lev_of == l % per)
            for s in range(4):
                for h in range(halves):
                    put(ref, main + s * levp, g * gl + h * LANES, set_t[s][which], (row16 == lev_of + h * per) & (row16 < lev))
        lo_c, w_c = low_col[g * RG : (g + 1) * RG], wt_col[g * RG : (g + 1) * RG]
        for h in range(halves):
            kap = lane16 + h * LANES
            e = kap - main
            es = e // levp
            ek = jnp.where(es == 0, -1, jnp.where(es == 1, 0, jnp.where(es == 2, rows - 1, rows)))
            k_of = jnp.where(e < 0, kap % rows, ek).astype(f32)
            l_of = jnp.where(e < 0, kap // rows, e % levp)
            back_t = weigh(k_of, lo_c, w_c)
            for ref, which in ((back_hi, 0), (back_lo, 1)):
                for l in range(lev):
                    if (h + 1) * LANES > main or l // per == h:
                        put(ref, g * gl + l * RG, h * LANES, back_t[which], l_of == l)

    pre_copy.wait_recv()
    for j in range(n // 2):
        psum[j] = frames[j, core] + pre_recv[j]

    used = frame + packed_rows

    def copy1(dst):
        return pltpu.make_async_remote_copy(
            src_ref=psum.at[dst, pl.ds(0, used), :],
            dst_ref=recv1.at[chip, pl.ds(0, used), :],
            send_sem=in_sem.at[4],
            recv_sem=rs1,
            device_id={"mem": 2 * dst + core},
        )

    for step in far_first[:-1]:
        copy1(to_chip(step)).start()
    recv1[chip] = psum[chip]

    nobs = cell.shape[1]
    crow = cell[...] // fine_cols
    ccol = cell[...] % fine_cols
    r32 = iota((4 * SUB, nobs), 0)
    col_o = jnp.where(r32 < ratio * SUB, (r32 % SUB) * ratio + r32 // SUB, -1)
    hot = (col_o == ccol).astype(f32).astype(bf16)
    hot2 = jnp.concatenate([hot, hot], axis=1)
    pr = prec[...]
    p_hi, p_lo = split2f(pr)
    v_hi, v_lo = split2f(val[:, 0, :] * pr)
    rbuf[main:, :] = jnp.zeros((gl - main, 2 * nobs), bf16)
    for g in range(ng):
        at_row = iota((RG, nobs), 0) + g * RG == crow
        for l in range(lev):
            at = slice(l * RG, (l + 1) * RG)
            rbuf[at, 0:nobs] = jnp.where(at_row, jnp.broadcast_to(v_hi[l : l + 1], (RG, nobs)), 0.0).astype(bf16)
            rbuf[at, nobs : 2 * nobs] = jnp.where(at_row, jnp.broadcast_to(v_lo[l : l + 1], (RG, nobs)), 0.0).astype(bf16)
        obs_b[:, g * gl : (g + 1) * gl] = dims(hot2, rbuf[...], 1, 1)
        ph = jnp.where(at_row, jnp.broadcast_to(p_hi, (RG, nobs)), 0.0).astype(bf16)
        plo = jnp.where(at_row, jnp.broadcast_to(p_lo, (RG, nobs)), 0.0).astype(bf16)
        for j in range(LANES // RG):
            abuf[j * RG : (j + 1) * RG, 0:nobs] = ph
            abuf[j * RG : (j + 1) * RG, nobs : 2 * nobs] = plo
        oa = dims(hot2, abuf[...], 1, 1)
        for j in range(gl // LANES):
            obs_a[:, g * gl + j * LANES : g * gl + (j + 1) * LANES] = oa

    pltpu.make_async_copy(fe_recv, fe_recv, fe_rs).wait()
    nt = wide // LANES
    left = jnp.concatenate([fe_recv[0, t : t + 1, :] for t in range(nt)], axis=1)
    right = jnp.concatenate([fe_recv[1, t : t + 1, :] for t in range(nt)], axis=1)
    fb = [fine_bg[b * SUB : (b + 1) * SUB, :] for b in range(ratio)]
    arow = iota((SUB, wide), 0)
    before0 = jnp.where(arow == 0, left, pltpu.roll(fb[ratio - 1], 1, 0))
    after_last = jnp.where(arow == SUB - 1, right, pltpu.roll(fb[0], SUB - 1, 0))
    chain = [before0] + fb + [after_last]
    slope_bg = [0.5 * (chain[b + 2] - chain[b]) for b in range(ratio)]

    def all_of(ref, count, height, sem):
        got = ref.at[pl.ds(0, count), pl.ds(0, height), :]
        pltpu.make_async_copy(got, got, sem).wait()

    all_of(rece, n - 1, packed_rows, rse)
    for side in (0, 1):

        @pl.when(has[side])
        def _():
            i = 0 if xs == 1 else side
            all_of(recc.at[i], n, packed_rows, rsc.at[i])

    prods, plains = [], []
    for i in range(xs):
        prod = rece[0] * recc[i, 0]
        only = recc[i, 0]
        for s in range(1, n):
            prod = prod + rece[s] * recc[i, s]
            only = only + recc[i, s]
        prods.append(prod)
        plains.append(only)
    set_of = (lane8 % half) // levp
    edge_sum = jnp.where(
        set_of < 2, jnp.where(has_up, prods[0], 0.0), jnp.where(has_down, prods[-1], 0.0)
    )
    from_up = jnp.where(has_up, pltpu.roll(plains[0], LANES - 2 * levp, 1), 0.0)
    from_down = jnp.where(has_down, pltpu.roll(plains[-1], 2 * levp, 1), 0.0)
    edge_sum = edge_sum + jnp.where(set_of == 0, from_up, jnp.where(set_of == 3, from_down, 0.0))
    edge_a = pltpu.roll(edge_sum, half, 1)
    edge_b = pltpu.roll(edge_sum, 5, 0)

    all_of(recv1, n // 2 - 1, used, rs1)
    total = recv1[0]
    for s in range(1, n // 2):
        total = total + recv1[s]
    m = total[SUB:]
    m_a = pltpu.roll(m, SUB - 2, 0)
    m_b = pltpu.roll(pltpu.roll(m, half, 1), 3, 0)
    x_a = jnp.where(low_half, m_a, edge_a)
    x_b = jnp.where(low_half, m_b, edge_b)
    x = jnp.concatenate([total, jnp.concatenate([jnp.where(row8 < 5, x_a, x_b), x_b], axis=0)], axis=1)
    x_hi, x_lo = split2f(x)
    x2 = jnp.concatenate([x_hi, x_lo], axis=0).astype(bf16)
    y = dims(x2, table_hi[...], 1, 0)
    y = y[0:16] + y[16:32] + dims(x_hi.astype(bf16), table_lo[...], 1, 0)
    taps = [y[0:SUB]] + [pltpu.roll(y, 2 * SUB - d, 0)[0:SUB] for d in (1, 2)]

    us, vs, moved = [], [], []
    for b in range(ratio):
        state = fb[b] + combine(wv[b], taps)
        slope = slope_bg[b] + combine(ws[b], taps)
        factor = 1.0 - advect_rate * slope
        mv = state * factor
        at = slice(b * SUB, (b + 1) * SUB)
        cot = obs_a[at, :] * mv - obs_b[at, :]
        us.append(cot * factor)
        vs.append((-advect_rate) * (state * cot))
        moved.append(mv)
    gl_v = None
    for d in range(3):
        t = combine([wv[b][d] for b in range(ratio)] + [ws[b][d] for b in range(ratio)], us + vs)
        t = jnp.concatenate([t, jnp.zeros_like(t)], axis=0)
        gl_v = t if d == 0 else gl_v + pltpu.roll(t, d, 0)
    g_hi, g_lo = split2f(gl_v)
    g2 = jnp.concatenate([g_hi, g_lo], axis=0).astype(bf16)
    gr = dims(g2, back_hi[...], 1, 0)
    gr = gr[0:16] + gr[16:32] + dims(g_hi.astype(bf16), back_lo[...], 1, 0)
    for g in (0, 1):
        send2[g] = gr[:, g * LANES : (g + 1) * LANES]
    def slot2(src):
        return recv2.at[src, :, pl.ds(0, frame), :]

    def copy2(dst, sem):
        return pltpu.make_async_remote_copy(
            src_ref=send2.at[:, pl.ds(0, frame), :],
            dst_ref=slot2(me),
            send_sem=ss2,
            recv_sem=sem,
            device_id={"mem": dst},
        )

    def forward2(src):
        return pltpu.make_async_remote_copy(
            src_ref=slot2(src),
            dst_ref=slot2(src),
            send_sem=ss2,
            recv_sem=rs2f,
            device_id={"mem": partner},
        )

    def copyx(side, dst):
        i = 0 if xs == 1 else 1 - side
        return pltpu.make_async_remote_copy(
            src_ref=sendx.at[0 if xs == 1 else side, pl.ds(0, packed_rows), :],
            dst_ref=recvx.at[i, core, chip, pl.ds(0, packed_rows), :],
            send_sem=ssx.at[0 if xs == 1 else side],
            recv_sem=rsx.at[i],
            device_id={"mem": dst, "band": side_band[side]},
        )

    def forwardx(i):
        got = recvx.at[i, core, :, pl.ds(0, packed_rows), :]
        return pltpu.make_async_remote_copy(
            src_ref=got,
            dst_ref=got,
            send_sem=ssx.at[xs + i],
            recv_sem=rsxf.at[i],
            device_id={"mem": partner},
        )

    def send_class(i):
        for step in classes[i]:
            copy2(2 * to_chip(step) + core, rs2.at[len(classes) - 1 - i]).start()

    for i in range(len(classes) - 1):
        send_class(i)
    v0, v1 = gr[0:SUB, LANES:], gr[SUB:, LANES:]
    quarter = lane8 // (2 * levp)
    v32, v96, w32, w96 = (pltpu.roll(v, r, 1) for v in (v0, v1) for r in (2 * levp, 6 * levp))

    def late(a, b):
        return jnp.where(row8 < 3, pltpu.roll(a, 3, 0), pltpu.roll(b, 3, 0))

    def pack_for(up_there):
        near = jnp.where(up_there, v32, v96)
        rest_cols = late(jnp.where(up_there, v96, v32), jnp.where(up_there, w96, w32))
        q = jnp.where(up_there, quarter - 1, quarter)
        return jnp.where(q == 2, near, jnp.where(q == 0, rest_cols, 0.0))

    if xs == 1:
        sendx[0] = pack_for(has_up)
    else:
        for side in (0, 1):
            sendx[side] = pack_for(side == 0)

    for side in (0, 1):

        @pl.when(has[side])
        def _():
            for step in far_first:
                copyx(side, 2 * to_chip(step) + core).start()

    send_class(len(classes) - 1)
    copy2(partner, rs2f).start()
    for g in (0, 1):
        recv2[me, g] = send2[g]

    advbuf[...] = jnp.concatenate(moved + [jnp.zeros((SUB, wide), f32)], axis=0)
    pickt = jnp.concatenate([pick, pick], axis=0)
    for g in range(ng):
        hi, lo = split2(advbuf[:, g * gl : g * gl + main])
        e = dims(jnp.concatenate([hi, lo], axis=0), pickt, 0, 0)
        for l in range(lev):
            v = jnp.where(in_row, e[l * RG : (l + 1) * RG], 0.0)
            adv_ref[l, :, g * gcells : (g + 1) * gcells] = jnp.sum(v, axis=0, keepdims=True)

    def sent_edges():
        pre_copy.wait_send()
        all_of(rece, n - 1, packed_rows, in_sem.at[1])
        all_of(recv1, n // 2 - 1, used, in_sem.at[4])
        pltpu.make_async_copy(fe_recv, fe_recv, in_sem.at[5]).wait()
        for side in (0, 1):

            @pl.when(has[side])
            def _():
                all_of(recc.at[0], n, packed_rows, in_sem.at[2 + side])
                edge_copy(side).wait_send()
                pltpu.make_async_copy(edge_recv.at[side], edge_recv.at[side], edge_rs.at[0 if xs == 1 else side]).wait()

    sent_edges()
    def all_2(count, sem):
        got = recv2.at[pl.ds(0, count), :, pl.ds(0, frame), :]
        pltpu.make_async_copy(got, got, sem).wait()

    ensr[...] = pltpu.roll(whole(ensf), 1, 1) * scale
    ebuf[...] = jnp.zeros(ebuf.shape, f32)
    edge_ens = [pltpu.roll(row(ensf, k), 1, 1) * scale for k in (0, rows - 1)]
    halo_ens = [pltpu.roll(edge_recv[side, 0:lev, :], 1, 1) * scale for side in (0, 1)]

    def smooth_back(v):
        return 0.25 * v + 0.5 * pltpu.roll(v, lon - 1, 1) + 0.25 * pltpu.roll(v, lon - 2, 1)

    for i, group in enumerate(reversed(classes)):
        all_2(len(group), rs2.at[i])
        for step in group:
            forward2(2 * from_chip(step) + core).start()
    for side in (0, 1):

        @pl.when(has[side])
        def _():
            i = 0 if xs == 1 else side
            pltpu.make_async_copy(recvx.at[i, core, :, pl.ds(0, packed_rows), :], recvx.at[i, core, :, pl.ds(0, packed_rows), :], rsx.at[i]).wait()
            forwardx(i).start()

    all_2(n // 2, rs2f)

    over = iota((SUB, LANES), 0) < frame - block

    def across(parts):
        per_tile = LANES // SUB
        cols = [jnp.concatenate(parts[t * per_tile : (t + 1) * per_tile], axis=0).T for t in range(tiles)]
        return cols[0] if tiles == 1 else jnp.concatenate(cols, axis=1)

    ours = (quarter < 2) | (set_of == 0) | (set_of == 3)
    set_lanes = lane8 >= half

    def edges_at(i, d):
        e = recvx[i, d % 2, d // 2]
        b = pltpu.roll(pltpu.roll(e, half, 1), 5, 0)
        return jnp.where(row8 < 5, e, b), jnp.where(over, b, 0.0)

    def gather(g):
        sides = range(xs) if g else ()
        prev = [edges_at(i, n - 1)[1] for i in sides]
        parts = []
        for d in range(n):
            tile = recv2[d, g, 0:SUB, :] + jnp.where(over, recv2[(d - 1) % n, g, SUB : 2 * SUB, :], 0.0)
            if g:
                theirs = None
                for i in sides:
                    here, tail = edges_at(i, d)
                    v = here + prev[i]
                    if xs == 2:
                        v = jnp.where(has[i], v, 0.0)
                    theirs = v if theirs is None else theirs + v
                    prev[i] = tail
                tile = jnp.where(ours, tile, 0.0) + jnp.where(set_lanes, theirs, 0.0)
            parts.append(tile)
        return across(parts)

    c0 = gather(0)
    for side in (0, 1):

        @pl.when(has[side])
        def _():
            i = 0 if xs == 1 else side
            all_of(recvx.at[i, 0], n // 2, packed_rows, rsxf.at[i])

    c1 = gather(1)
    e0 = main - LANES
    wm = ensr[...] * jnp.concatenate([c0, c1[0:e0]], axis=0)
    w_up = jnp.where(kk == 0, 0.0, pltpu.roll(wm, 1, 0))
    w_dn = jnp.where(kk == rows - 1, 0.0, pltpu.roll(wm, main - 1, 0))
    zz = smooth_back(0.25 * (w_up + w_dn) + 0.5 * wm)
    for t in range(tiles):
        grad_ref[t] = zz[:, t * LANES : (t + 1) * LANES]
    for side, k, k_in in ((0, 0, 1), (1, rows - 1, rows - 2)):
        halo_at, extra_at = (e0, e0 + levp) if side == 0 else (e0 + 3 * levp, e0 + 2 * levp)
        we = edge_ens[side] * c1[extra_at : extra_at + lev]
        wh = halo_ens[side] * c1[halo_at : halo_at + lev]
        z_edge = smooth_back(0.5 * we + 0.25 * wh)
        z_in = smooth_back(0.25 * we)
        for t in range(tiles):
            cut = slice(t * LANES, (t + 1) * LANES)
            grad_ref.at[t][pl.ds(k, lev, stride=rows), :] += z_edge[:, cut]
            grad_ref.at[t][pl.ds(k_in, lev, stride=rows), :] += z_in[:, cut]

    for side in (0, 1):

        @pl.when(has[side])
        def _():
            i = 0 if xs == 1 else side
            all_of(recvx.at[0, 0], n // 2, packed_rows, ssx.at[i])
            all_of(recvx.at[0, 0], n // 2, packed_rows, ssx.at[xs + i])

    all_2(n - 1, ss2)


def writer(adv_ref, grad_ref, adv_out, grad_out, sem):
    copies = [
        pltpu.make_async_copy(grad_ref, grad_out, sem.at[0]),
        pltpu.make_async_copy(adv_ref, adv_out, sem.at[1]),
    ]
    for c in copies:
        c.start()
    for c in copies:
        c.wait()


def up_to(x, m):
    return -(-x // m) * m


def to_tiles(x):
    return x.reshape(-1, x.shape[3] // LANES, LANES).swapaxes(0, 1)


def shards(ensemble, alpha, lat_lower, lat_weight, background, obs_cell, obs_value, obs_precision):
    n, nb = lax.axis_size("mem"), lax.axis_size("band")
    members, lev, rows, lon = ensemble.shape
    fine_rows = lat_lower.shape[0]
    cells = background.shape[2]
    nobs = obs_cell.shape[1]
    fine_cols = cells // fine_rows
    scale = 1.0 / math.sqrt(members * n - 1)
    block = lon // n
    main = lev * rows
    kaps = main + 4 * RG
    assert n % 2 == 0 and members == 1 and block == SUB and rows == RG and lev <= RG and kaps == 2 * LANES
    assert fine_rows % RG == 0 and fine_cols % block == 0 and fine_cols // block == 3
    cfg = (n, nb, lev, rows, lon, fine_rows, fine_cols, scale)
    tiles = lon // LANES
    ng = fine_rows // RG
    gl = RG * RG
    wide = ng * gl
    gcells = RG * fine_cols
    xs = 1 if nb == 2 else 2
    dma = pltpu.SemaphoreType.DMA
    vm = pl.BlockSpec(memory_space=pltpu.VMEM)
    hbm = pl.BlockSpec(memory_space=pltpu.HBM)
    fr = 2 * SUB
    advected, gradient = pl.pallas_call(
        functools.partial(kernel, cfg),
        out_shape=(
            jax.ShapeDtypeStruct(background.shape, f32),
            jax.ShapeDtypeStruct((tiles, main, LANES), f32),
        ),
        in_specs=[hbm] * 8,
        out_specs=(vm, vm),
        scratch_shapes=[
            pltpu.VMEM((tiles, main, LANES), bf16),
            pltpu.VMEM((tiles, main, LANES), f32),
            pltpu.VMEM((1, fine_rows), jnp.int32),
            pltpu.VMEM((1, fine_rows), f32),
            pltpu.VMEM(background.shape, f32),
            pltpu.VMEM((1, nobs), jnp.int32),
            pltpu.VMEM(obs_value.shape, f32),
            pltpu.VMEM((1, nobs), f32),
            pltpu.VMEM((tiles, main, LANES), f32),
            pltpu.VMEM((tiles, main, LANES), f32),
            pltpu.VMEM((kaps, lon), f32),
            pltpu.VMEM((LANES, lon), f32),
            pltpu.VMEM((2, RG, lon), f32),
            pltpu.VMEM((2, RG, lon), f32),
            pltpu.VMEM((3, lon + SUB, LANES), f32),
            pltpu.VMEM((n // 2, 2, fr, LANES), f32),
            pltpu.VMEM((n // 2, fr, LANES), f32),
            pltpu.VMEM((n // 2, fr, LANES), f32),
            pltpu.VMEM((n // 2, fr, LANES), f32),
            pltpu.VMEM((n, SUB, LANES), f32),
            pltpu.VMEM((n, SUB, LANES), f32),
            pltpu.VMEM((xs, n, SUB, LANES), f32),
            pltpu.VMEM((xs, n, SUB, LANES), f32),
            pltpu.VMEM((kaps, wide), bf16),
            pltpu.VMEM((kaps, wide), bf16),
            pltpu.VMEM((wide, kaps), bf16),
            pltpu.VMEM((wide, kaps), bf16),
            pltpu.VMEM((gl, 2 * gcells), bf16),
            pltpu.VMEM((gl, 2 * nobs), bf16),
            pltpu.VMEM((LANES, 2 * nobs), bf16),
            pltpu.VMEM((4 * SUB, wide), f32),
            pltpu.VMEM((4 * SUB, wide), f32),
            pltpu.VMEM((4 * SUB, wide), f32),
            pltpu.VMEM((2, SUB, LANES), f32),
            pltpu.VMEM((2, SUB, LANES), f32),
            pltpu.VMEM((4 * SUB, wide), f32),
            pltpu.VMEM((2, fr, LANES), f32),
            pltpu.VMEM((n, 2, fr, LANES), f32),
            pltpu.VMEM((xs, SUB, LANES), f32),
            pltpu.VMEM((xs, 2, n // 2, SUB, LANES), f32),
            pltpu.VMEM((tiles, main, LANES), f32),
            pltpu.VMEM((main, lon), f32),
            dma((8,)),
            dma((xs,)),
            dma,
            dma,
            dma,
            dma((xs,)),
            dma,
            dma,
            dma((len(chip_order(n // 2)[1]),)),
            dma,
            dma((2 * xs,)),
            dma((xs,)),
            dma((xs,)),
        ],
        compiler_params=pltpu.CompilerParams(collective_id=0, has_side_effects=True, vmem_limit_bytes=48 * 2**20),
    )(
        *(
            pltpu.with_memory_space_constraint(v, pltpu.HBM)
            for v in (
                to_tiles(ensemble),
                to_tiles(alpha),
                lat_lower.reshape(1, fine_rows),
                lat_weight.reshape(1, fine_rows),
                background,
                obs_cell,
                obs_value,
                obs_precision,
            )
        )
    )
    advected, gradient = pl.pallas_call(
        writer,
        out_shape=(
            jax.ShapeDtypeStruct(background.shape, f32),
            jax.ShapeDtypeStruct((tiles, main, LANES), f32),
        ),
        in_specs=[vm, vm],
        out_specs=(hbm, hbm),
        scratch_shapes=[dma((2,))],
        compiler_params=pltpu.CompilerParams(vmem_limit_bytes=2**20),
    )(advected, gradient)
    return advected, gradient.swapaxes(0, 1).reshape(members, lev, rows, lon)


def solution(mesh):
    return jax.shard_map(
        shards,
        mesh=mesh,
        in_specs=(
            P("mem", None, "band", None),
            P("mem", None, "band", None),
            P("band"),
            P("band"),
            P(None, ("band", "mem"), None),
            P(("band", "mem"), None),
            P(None, ("band", "mem"), None),
            P(("band", "mem"), None),
        ),
        out_specs=(P(None, ("band", "mem"), None), P("mem", None, "band", None)),
        check_vma=False,
    )
```

```python
import functools
import math

import jax
import jax.numpy as jnp
from jax import lax
from jax.experimental import pallas as pl
from jax.experimental.pallas import tpu as pltpu
from jax.sharding import PartitionSpec as P

advect_rate = 0.25
LANES = 128
SUB = 8
RG = 16
f32 = jnp.float32
bf16 = jnp.bfloat16


def split2(x):
    hi = x.astype(bf16)
    lo = (x - hi.astype(f32)).astype(bf16)
    return hi, lo


def split2f(x):
    hi = x.astype(bf16).astype(f32)
    return hi, x - hi


def dims(a, b, ca, cb):
    return lax.dot_general(a, b, (((ca,), (cb,)), ((), ())), preferred_element_type=f32)


def iota(shape, d):
    return lax.broadcasted_iota(jnp.int32, shape, d)


def smooth_lon(x):
    n = x.shape[1]
    return 0.25 * pltpu.roll(x, 1, 1) + 0.5 * x + 0.25 * pltpu.roll(x, n - 1, 1)


def lon_weights(ratio):
    def parts(shift):
        num = 2 * shift + 1 + ratio
        return num // (2 * ratio), (num % (2 * ratio)) / (2 * ratio)

    def taps(shift):
        q, f = parts(shift)
        w = [0.0, 0.0, 0.0]
        for at, v in ((q, 1.0 - f), (q + 1, f)):
            if v:
                w[at] += v
        return w

    value = [taps(b) for b in range(ratio)]
    slope = [[0.5 * (p - m) for p, m in zip(taps(b + 1), taps(b - 1))] for b in range(ratio)]
    return value, slope


def combine(weights, parts):
    out = None
    for w, p in zip(weights, parts):
        if w == 0.0:
            continue
        term = p if w == 1.0 else w * p
        out = term if out is None else out + term
    return out


def chip_order(chips):
    ring = 4 if chips % 4 == 0 else chips
    rest = chips // ring

    def hops(step):
        return min(step[0], ring - step[0]) + min(step[1], rest - step[1])

    steps = sorted(((a, b) for a in range(ring) for b in range(rest)), key=lambda s: -hops(s))
    classes = [[s for s in steps if hops(s) == h] for h in sorted({hops(s) for s in steps if hops(s)}, reverse=True)]
    return steps, classes, ring, rest


def kernel(
    cfg,
    ens_hbm,
    alpha_hbm,
    low_hbm,
    wt_hbm,
    bg_hbm,
    cell_hbm,
    val_hbm,
    prec_hbm,
    adv_ref,
    grad_ref,
    ens_in,
    alpha,
    low,
    wt,
    bg,
    cell,
    val,
    prec,
    ensf,
    plain,
    part,
    xpart,
    edge_send,
    edge_recv,
    flat,
    frames,
    pre_recv,
    psum,
    recv1,
    eloc,
    rece,
    ecr,
    recc,
    table_hi,
    table_lo,
    back_hi,
    back_lo,
    zbuf,
    rbuf,
    abuf,
    fine_bg,
    obs_a,
    obs_b,
    fe_send,
    fe_recv,
    advbuf,
    send2,
    recv2,
    sendx,
    recvx,
    ebuf,
    ensr,
    in_sem,
    edge_rs,
    pre_rs,
    rs1,
    rse,
    rsc,
    fe_rs,
    ss2,
    rs2,
    rs2f,
    ssx,
    rsx,
    rsxf,
):
    n, nb, lev, rows, lon, fine_rows, fine_cols, scale = cfg
    block = lon // n
    frame = block + 2
    ratio = fine_cols // block
    main = lev * rows
    tiles = lon // LANES
    ng = fine_rows // RG
    gcells = RG * fine_cols
    gl = RG * RG
    levp = RG
    xs = recvx.shape[0]
    me = lax.axis_index("mem")
    band = lax.axis_index("band")
    has_up = band > 0
    has_down = band < nb - 1
    has = (has_up, has_down)
    wv, ws = lon_weights(ratio)

    barrier = pltpu.get_barrier_semaphore()

    core = lax.rem(me, 2)
    chip = me // 2
    partner = me + 1 - 2 * core
    chips = n // 2
    far_first, classes, ring, rest = chip_order(chips)
    ring_at, rest_at = chip // rest, lax.rem(chip, rest)

    def to_chip(step):
        return lax.rem(ring_at + step[0], ring) * rest + lax.rem(rest_at + step[1], rest)

    def from_chip(step):
        return to_chip(((ring - step[0]) % ring, (rest - step[1]) % rest))

    side_band = (band - 1, band + 1)
    for step in far_first:
        home = step == (0, 0)
        for c in (core, 1 - core):
            if nb == 2:
                pl.semaphore_signal(barrier, inc=1, device_id={"mem": 2 * to_chip(step) + c, "band": 1 - band})
            else:
                for side in (0, 1):

                    @pl.when(has[side])
                    def _():
                        pl.semaphore_signal(
                            barrier, inc=1, device_id={"mem": 2 * to_chip(step) + c, "band": side_band[side]}
                        )

            if not (home and c is core):
                pl.semaphore_signal(barrier, inc=1, device_id={"mem": 2 * to_chip(step) + c})

    loads = [
        pltpu.make_async_copy(src, dst, in_sem.at[i])
        for i, (src, dst) in enumerate(
            (
                (alpha_hbm, alpha),
                (ens_hbm, ens_in),
                (bg_hbm, bg),
                (low_hbm, low),
                (wt_hbm, wt),
                (cell_hbm, cell),
                (val_hbm, val),
                (prec_hbm, prec),
            )
        )
    ]
    for c in loads:
        c.start()

    part[main:, :] = jnp.zeros((part.shape[0] - main, lon), f32)
    xpart[...] = jnp.zeros(xpart.shape, f32)
    edge_send[...] = jnp.zeros(edge_send.shape, f32)
    fe_send[...] = jnp.zeros(fe_send.shape, f32)

    loads[0].wait()
    loads[1].wait()

    def whole(ref):
        parts = [ref[t] for t in range(tiles)]
        return parts[0] if tiles == 1 else jnp.concatenate(parts, axis=1)

    def row(ref, k):
        parts = [ref.at[t][pl.ds(k, lev, stride=rows), :] for t in range(tiles)]
        return parts[0] if tiles == 1 else jnp.concatenate(parts, axis=1)

    for t in range(tiles):
        ensf[t] = ens_in[t].astype(f32)
    al = whole(alpha)
    en = whole(ensf)
    kk = iota((main, lon), 0) % rows
    a_up = jnp.where(kk == 0, 0.0, pltpu.roll(al, 1, 0))
    a_dn = jnp.where(kk == rows - 1, 0.0, pltpu.roll(al, main - 1, 0))
    z = smooth_lon(0.25 * (a_up + a_dn) + 0.5 * al) * en * scale
    for t in range(tiles):
        plain[t] = z[:, t * LANES : (t + 1) * LANES]
    part[0:main, :] = z
    edges = []
    for side, k in ((0, 0), (1, rows - 1)):
        a_edge = smooth_lon(row(alpha, k)) * (0.25 * scale)
        e_edge = row(ensf, k)
        edges.append((a_edge, e_edge, row(plain, k)))
        edge_send[side, 0:lev, :] = e_edge
        at = main + side * 2 * levp
        for i, v in enumerate((a_edge, e_edge) if side == 0 else (e_edge, a_edge)):
            part[at + i * levp : at + i * levp + lev, :] = v
    (a_0, e_0, p_0), (a_1, e_1, p_1) = edges
    zero = jnp.zeros_like(a_0)
    sets_up = [zero, p_0, a_0, e_0]
    sets_down = [e_1, a_1, p_1, zero]
    if xs == 1:
        sets = [jnp.where(has_up, u, d) for u, d in zip(sets_up, sets_down)]
    else:
        sets = sets_up + sets_down
    for i, v in enumerate(sets):
        xpart[i * levp : i * levp + lev, :] = v

    def lay(g, rows_of):
        rows_of = pltpu.roll(rows_of, 1, 1)
        for t in range(tiles):
            flat[g, t * LANES : (t + 1) * LANES, :] = rows_of[:, t * LANES : (t + 1) * LANES].T
        flat[g, lon : lon + SUB, :] = flat[g, 0:SUB, :]

    lay(0, part[0:LANES, :])
    lay(1, part[LANES : 2 * LANES, :])
    lay(2, xpart[...])

    lane8 = iota((SUB, LANES), 1)
    row8 = iota((SUB, LANES), 0)
    low_half = lane8 < LANES // 2
    half = LANES // 2

    def tile_of(g, d):
        return flat[g, d * SUB : (d + 1) * SUB, :]

    def views(d):
        v, x = tile_of(1, d), tile_of(2, d)
        flip, flipx = pltpu.roll(v, half, 1), pltpu.roll(x, half, 1)
        return v, flip, x, flipx, pltpu.roll(flip, 5, 0), pltpu.roll(v, 3, 0), pltpu.roll(flipx, 3, 0), pltpu.roll(x, 3, 0)

    cur = views(0)
    for d in range(n):
        nxt = views(d + 1)
        v, flip, x, flipx, r5, v3, fx3, x3 = cur
        packed = jnp.where(low_half, pltpu.roll(v, 2, 0), jnp.where(row8 < 5, r5, nxt[4]))
        frames[d // 2, d % 2, 0:SUB, :] = tile_of(0, d)
        frames[d // 2, d % 2, SUB : 2 * SUB, :] = jnp.where(row8 < 2, tile_of(0, d + 1), packed)
        eloc[d] = jnp.where(low_half, flip, jnp.where(row8 < 3, v3, nxt[5]))
        ecr[0, d] = jnp.where(low_half, x, jnp.where(row8 < 3, fx3, nxt[6]))
        if xs == 2:
            ecr[1, d] = jnp.where(low_half, flipx, jnp.where(row8 < 3, x3, nxt[7]))
        cur = nxt

    loads[2].wait()
    row32 = iota((4 * SUB, gcells), 0)
    col_of = jnp.where(row32 < ratio * SUB, (row32 % SUB) * ratio + row32 // SUB, -1)
    pick = (iota((4 * SUB, gcells), 1) % fine_cols == col_of).astype(f32).astype(bf16)
    pick2 = jnp.concatenate([pick, pick], axis=1)
    in_row = iota((RG, gcells), 1) // fine_cols == iota((RG, gcells), 0)
    zbuf[main:, :] = jnp.zeros((gl - main, 2 * gcells), bf16)
    back = bg[:, 0, :]
    for g in range(ng):
        hi, lo = split2f(back[:, g * gcells : (g + 1) * gcells])
        for l in range(lev):
            at = slice(l * RG, (l + 1) * RG)
            zbuf[at, 0:gcells] = jnp.where(in_row, jnp.broadcast_to(hi[l : l + 1], (RG, gcells)), 0.0).astype(bf16)
            zbuf[at, gcells : 2 * gcells] = jnp.where(in_row, jnp.broadcast_to(lo[l : l + 1], (RG, gcells)), 0.0).astype(bf16)
        fine_bg[:, g * gl : (g + 1) * gl] = dims(pick2, zbuf[...], 1, 1)
    for c in loads[3:]:
        c.wait()

    if nb == 2:
        pl.semaphore_wait(barrier, 2 * n - 1)
    else:
        pl.semaphore_wait(barrier, n - 1 + n * (has_up.astype(jnp.int32) + has_down.astype(jnp.int32)))

    pre_copy = pltpu.make_async_remote_copy(
        src_ref=frames.at[:, core],
        dst_ref=pre_recv,
        send_sem=in_sem.at[0],
        recv_sem=pre_rs,
        device_id={"mem": partner},
    )
    pre_copy.start()
    packed_rows = frame // 2

    def copyc(side, dst):
        i = 0 if xs == 1 else 1 - side
        return pltpu.make_async_remote_copy(
            src_ref=ecr.at[0 if xs == 1 else side, dst, pl.ds(0, packed_rows), :],
            dst_ref=recc.at[i, me, pl.ds(0, packed_rows), :],
            send_sem=in_sem.at[2 + side],
            recv_sem=rsc.at[i],
            device_id={"mem": dst, "band": side_band[side]},
        )

    def copye(dst):
        return pltpu.make_async_remote_copy(
            src_ref=eloc.at[dst, pl.ds(0, packed_rows), :],
            dst_ref=rece.at[me, pl.ds(0, packed_rows), :],
            send_sem=in_sem.at[1],
            recv_sem=rse,
            device_id={"mem": dst},
        )

    def edge_copy(side):
        return pltpu.make_async_remote_copy(
            src_ref=edge_send.at[side],
            dst_ref=edge_recv.at[1 - side],
            send_sem=in_sem.at[6 + side],
            recv_sem=edge_rs.at[0 if xs == 1 else 1 - side],
            device_id={"band": side_band[side]},
        )

    for side in (0, 1):

        @pl.when(has[side])
        def _():
            for step in far_first:
                for c in (core, 1 - core):
                    copyc(side, 2 * to_chip(step) + c).start()

        @pl.when(jnp.logical_not(has[side]))
        def _():
            edge_recv[side] = jnp.zeros(edge_recv.shape[1:], f32)

    for step in far_first:
        for c in (core, 1 - core):
            if step != (0, 0) or c is not core:
                copye(2 * to_chip(step) + c).start()
    for side in (0, 1):

        @pl.when(has[side])
        def _():
            edge_copy(side).start()

    rece[me] = eloc[me]

    first = fine_bg[0:1, :]
    last = fine_bg[ratio * SUB - 1 : ratio * SUB, :]
    for t in range(ng * gl // LANES):
        fe_send[0, t : t + 1, :] = first[:, t * LANES : (t + 1) * LANES]
        fe_send[1, t : t + 1, :] = last[:, t * LANES : (t + 1) * LANES]

    def fe_copy(side):
        return pltpu.make_async_remote_copy(
            src_ref=fe_send.at[side],
            dst_ref=fe_recv.at[1 - side],
            send_sem=in_sem.at[5],
            recv_sem=fe_rs,
            device_id={"mem": lax.rem(me + (n - 1 if side == 0 else 1), n)},
        )

    fe_copy(0).start()
    fe_copy(1).start()

    lane = iota((SUB, LANES), 1)
    wide = ng * gl

    def per_row(v):
        v = jnp.concatenate([v, jnp.zeros((1, LANES - fine_rows), f32)], axis=1)
        return jnp.broadcast_to(v, (SUB, LANES))

    def tiled(v, g):
        r = v if g == 0 else pltpu.roll(v, LANES - g * RG, 1)
        r = jnp.where(lane < RG, r, 0.0)
        for s in (RG, 2 * RG, 4 * RG):
            r = r + pltpu.roll(r, s, 1)
        return jnp.concatenate([r, r], axis=0)

    low_rows, wt_rows = per_row(low[...].astype(f32)), per_row(wt[...])
    down = lambda v: jnp.concatenate([v] * (LANES // SUB), axis=0).T
    low_col, wt_col = down(low_rows), down(wt_rows)
    lane16 = iota((RG, LANES), 1)
    row16 = iota((RG, LANES), 0)
    lev_of = lane16 // RG
    set_rows = (-1, 0, rows - 1, rows)
    table_hi[...] = jnp.zeros(table_hi.shape, bf16)
    table_lo[...] = jnp.zeros(table_lo.shape, bf16)
    back_hi[...] = jnp.zeros(back_hi.shape, bf16)
    back_lo[...] = jnp.zeros(back_lo.shape, bf16)
    halves = gl // LANES
    per = LANES // RG

    def weigh(k, lo_k, w):
        w_hi, w_lo = split2f(w)
        o_hi, o_lo = split2f(1.0 - w)
        m0, m1 = k == lo_k, k == lo_k + 1.0
        return (
            jnp.where(m0, o_hi, jnp.where(m1, w_hi, 0.0)),
            jnp.where(m0, o_lo, jnp.where(m1, w_lo, 0.0)),
        )

    def put(ref, r, c, v, keep):
        ref[r : r + RG, c : c + LANES] = jnp.where(keep, v, 0.0).astype(bf16)

    for g in range(ng):
        lo_t, w_t = tiled(low_rows, g), tiled(wt_rows, g)
        main_t = weigh(row16.astype(f32), lo_t, w_t)
        set_t = [weigh(jnp.full((RG, LANES), float(k), f32), lo_t, w_t) for k in set_rows]
        for ref, which in ((table_hi, 0), (table_lo, 1)):
            for l in range(lev):
                put(ref, l * RG, g * gl + l // per * LANES, main_t[which], lev_of == l % per)
            for s in range(4):
                for h in range(halves):
                    put(ref, main + s * levp, g * gl + h * LANES, set_t[s][which], (row16 == lev_of + h * per) & (row16 < lev))
        lo_c, w_c = low_col[g * RG : (g + 1) * RG], wt_col[g * RG : (g + 1) * RG]
        for h in range(halves):
            kap = lane16 + h * LANES
            e = kap - main
            es = e // levp
            ek = jnp.where(es == 0, -1, jnp.where(es == 1, 0, jnp.where(es == 2, rows - 1, rows)))
            k_of = jnp.where(e < 0, kap % rows, ek).astype(f32)
            l_of = jnp.where(e < 0, kap // rows, e % levp)
            back_t = weigh(k_of, lo_c, w_c)
            for ref, which in ((back_hi, 0), (back_lo, 1)):
                for l in range(lev):
                    if (h + 1) * LANES > main or l // per == h:
                        put(ref, g * gl + l * RG, h * LANES, back_t[which], l_of == l)

    pre_copy.wait_recv()
    for j in range(n // 2):
        psum[j] = frames[j, 1 - core] + pre_recv[j]

    used = frame + packed_rows

    def copy1(dst):
        return pltpu.make_async_remote_copy(
            src_ref=psum.at[dst, pl.ds(0, used), :],
            dst_ref=recv1.at[chip, pl.ds(0, used), :],
            send_sem=in_sem.at[4],
            recv_sem=rs1,
            device_id={"mem": 2 * dst + 1 - core},
        )

    for step in far_first:
        copy1(to_chip(step)).start()

    nobs = cell.shape[1]
    crow = cell[...] // fine_cols
    ccol = cell[...] % fine_cols
    r32 = iota((4 * SUB, nobs), 0)
    col_o = jnp.where(r32 < ratio * SUB, (r32 % SUB) * ratio + r32 // SUB, -1)
    hot = (col_o == ccol).astype(f32).astype(bf16)
    hot2 = jnp.concatenate([hot, hot], axis=1)
    pr = prec[...]
    p_hi, p_lo = split2f(pr)
    v_hi, v_lo = split2f(val[:, 0, :] * pr)
    rbuf[main:, :] = jnp.zeros((gl - main, 2 * nobs), bf16)
    for g in range(ng):
        at_row = iota((RG, nobs), 0) + g * RG == crow
        for l in range(lev):
            at = slice(l * RG, (l + 1) * RG)
            rbuf[at, 0:nobs] = jnp.where(at_row, jnp.broadcast_to(v_hi[l : l + 1], (RG, nobs)), 0.0).astype(bf16)
            rbuf[at, nobs : 2 * nobs] = jnp.where(at_row, jnp.broadcast_to(v_lo[l : l + 1], (RG, nobs)), 0.0).astype(bf16)
        obs_b[:, g * gl : (g + 1) * gl] = dims(hot2, rbuf[...], 1, 1)
        ph = jnp.where(at_row, jnp.broadcast_to(p_hi, (RG, nobs)), 0.0).astype(bf16)
        plo = jnp.where(at_row, jnp.broadcast_to(p_lo, (RG, nobs)), 0.0).astype(bf16)
        for j in range(LANES // RG):
            abuf[j * RG : (j + 1) * RG, 0:nobs] = ph
            abuf[j * RG : (j + 1) * RG, nobs : 2 * nobs] = plo
        oa = dims(hot2, abuf[...], 1, 1)
        for j in range(gl // LANES):
            obs_a[:, g * gl + j * LANES : g * gl + (j + 1) * LANES] = oa

    pltpu.make_async_copy(fe_recv, fe_recv, fe_rs).wait()
    nt = wide // LANES
    left = jnp.concatenate([fe_recv[0, t : t + 1, :] for t in range(nt)], axis=1)
    right = jnp.concatenate([fe_recv[1, t : t + 1, :] for t in range(nt)], axis=1)
    fb = [fine_bg[b * SUB : (b + 1) * SUB, :] for b in range(ratio)]
    arow = iota((SUB, wide), 0)
    before0 = jnp.where(arow == 0, left, pltpu.roll(fb[ratio - 1], 1, 0))
    after_last = jnp.where(arow == SUB - 1, right, pltpu.roll(fb[0], SUB - 1, 0))
    chain = [before0] + fb + [after_last]
    slope_bg = [0.5 * (chain[b + 2] - chain[b]) for b in range(ratio)]

    def all_of(ref, count, height, sem):
        got = ref.at[pl.ds(0, count), pl.ds(0, height), :]
        pltpu.make_async_copy(got, got, sem).wait()

    all_of(rece, n - 1, packed_rows, rse)
    for side in (0, 1):

        @pl.when(has[side])
        def _():
            i = 0 if xs == 1 else side
            all_of(recc.at[i], n, packed_rows, rsc.at[i])

    prods, plains = [], []
    for i in range(xs):
        prod = rece[0] * recc[i, 0]
        only = recc[i, 0]
        for s in range(1, n):
            prod = prod + rece[s] * recc[i, s]
            only = only + recc[i, s]
        prods.append(prod)
        plains.append(only)
    set_of = (lane8 % half) // levp
    edge_sum = jnp.where(
        set_of < 2, jnp.where(has_up, prods[0], 0.0), jnp.where(has_down, prods[-1], 0.0)
    )
    from_up = jnp.where(has_up, pltpu.roll(plains[0], LANES - 2 * levp, 1), 0.0)
    from_down = jnp.where(has_down, pltpu.roll(plains[-1], 2 * levp, 1), 0.0)
    edge_sum = edge_sum + jnp.where(set_of == 0, from_up, jnp.where(set_of == 3, from_down, 0.0))
    edge_a = pltpu.roll(edge_sum, half, 1)
    edge_b = pltpu.roll(edge_sum, 5, 0)

    all_of(recv1, n // 2, used, rs1)
    total = recv1[0]
    for s in range(1, n // 2):
        total = total + recv1[s]
    m = total[SUB:]
    m_a = pltpu.roll(m, SUB - 2, 0)
    m_b = pltpu.roll(pltpu.roll(m, half, 1), 3, 0)
    x_a = jnp.where(low_half, m_a, edge_a)
    x_b = jnp.where(low_half, m_b, edge_b)
    x = jnp.concatenate([total, jnp.concatenate([jnp.where(row8 < 5, x_a, x_b), x_b], axis=0)], axis=1)
    x_hi, x_lo = split2f(x)
    x2 = jnp.concatenate([x_hi, x_lo], axis=0).astype(bf16)
    y = dims(x2, table_hi[...], 1, 0)
    y = y[0:16] + y[16:32] + dims(x_hi.astype(bf16), table_lo[...], 1, 0)
    taps = [y[0:SUB]] + [pltpu.roll(y, 2 * SUB - d, 0)[0:SUB] for d in (1, 2)]

    us, vs, moved = [], [], []
    for b in range(ratio):
        state = fb[b] + combine(wv[b], taps)
        slope = slope_bg[b] + combine(ws[b], taps)
        factor = 1.0 - advect_rate * slope
        mv = state * factor
        at = slice(b * SUB, (b + 1) * SUB)
        cot = obs_a[at, :] * mv - obs_b[at, :]
        us.append(cot * factor)
        vs.append((-advect_rate) * (state * cot))
        moved.append(mv)
    gl_v = None
    for d in range(3):
        t = combine([wv[b][d] for b in range(ratio)] + [ws[b][d] for b in range(ratio)], us + vs)
        t = jnp.concatenate([t, jnp.zeros_like(t)], axis=0)
        gl_v = t if d == 0 else gl_v + pltpu.roll(t, d, 0)
    g_hi, g_lo = split2f(gl_v)
    g2 = jnp.concatenate([g_hi, g_lo], axis=0).astype(bf16)
    gr = dims(g2, back_hi[...], 1, 0)
    gr = gr[0:16] + gr[16:32] + dims(g_hi.astype(bf16), back_lo[...], 1, 0)
    for g in (0, 1):
        send2[g] = gr[:, g * LANES : (g + 1) * LANES]
    def slot2(src):
        return recv2.at[src, :, pl.ds(0, frame), :]

    def copy2(dst, sem):
        return pltpu.make_async_remote_copy(
            src_ref=send2.at[:, pl.ds(0, frame), :],
            dst_ref=slot2(me),
            send_sem=ss2,
            recv_sem=sem,
            device_id={"mem": dst},
        )

    def forward2(src):
        return pltpu.make_async_remote_copy(
            src_ref=slot2(src),
            dst_ref=slot2(src),
            send_sem=ss2,
            recv_sem=rs2f,
            device_id={"mem": partner},
        )

    def copyx(side, dst):
        i = 0 if xs == 1 else 1 - side
        return pltpu.make_async_remote_copy(
            src_ref=sendx.at[0 if xs == 1 else side, pl.ds(0, packed_rows), :],
            dst_ref=recvx.at[i, core, chip, pl.ds(0, packed_rows), :],
            send_sem=ssx.at[0 if xs == 1 else side],
            recv_sem=rsx.at[i],
            device_id={"mem": dst, "band": side_band[side]},
        )

    def forwardx(i):
        got = recvx.at[i, 1 - core, :, pl.ds(0, packed_rows), :]
        return pltpu.make_async_remote_copy(
            src_ref=got,
            dst_ref=got,
            send_sem=ssx.at[xs + i],
            recv_sem=rsxf.at[i],
            device_id={"mem": partner},
        )

    def send_class(i):
        for step in classes[i]:
            copy2(2 * to_chip(step) + 1 - core, rs2.at[len(classes) - 1 - i]).start()

    for i in range(len(classes) - 1):
        send_class(i)
    v0, v1 = gr[0:SUB, LANES:], gr[SUB:, LANES:]
    quarter = lane8 // (2 * levp)
    v32, v96, w32, w96 = (pltpu.roll(v, r, 1) for v in (v0, v1) for r in (2 * levp, 6 * levp))

    def late(a, b):
        return jnp.where(row8 < 3, pltpu.roll(a, 3, 0), pltpu.roll(b, 3, 0))

    def pack_for(up_there):
        near = jnp.where(up_there, v32, v96)
        rest_cols = late(jnp.where(up_there, v96, v32), jnp.where(up_there, w96, w32))
        q = jnp.where(up_there, quarter - 1, quarter)
        return jnp.where(q == 2, near, jnp.where(q == 0, rest_cols, 0.0))

    if xs == 1:
        sendx[0] = pack_for(has_up)
    else:
        for side in (0, 1):
            sendx[side] = pack_for(side == 0)

    for side in (0, 1):

        @pl.when(has[side])
        def _():
            for step in far_first:
                copyx(side, 2 * to_chip(step) + 1 - core).start()

    send_class(len(classes) - 1)
    copy2(partner, rs2f).start()
    for g in (0, 1):
        recv2[me, g] = send2[g]

    advbuf[...] = jnp.concatenate(moved + [jnp.zeros((SUB, wide), f32)], axis=0)
    pickt = jnp.concatenate([pick, pick], axis=0)
    for g in range(ng):
        hi, lo = split2(advbuf[:, g * gl : g * gl + main])
        e = dims(jnp.concatenate([hi, lo], axis=0), pickt, 0, 0)
        for l in range(lev):
            v = jnp.where(in_row, e[l * RG : (l + 1) * RG], 0.0)
            adv_ref[l, :, g * gcells : (g + 1) * gcells] = jnp.sum(v, axis=0, keepdims=True)

    def sent_edges():
        pre_copy.wait_send()
        all_of(rece, n - 1, packed_rows, in_sem.at[1])
        all_of(recv1, n // 2, used, in_sem.at[4])
        pltpu.make_async_copy(fe_recv, fe_recv, in_sem.at[5]).wait()
        for side in (0, 1):

            @pl.when(has[side])
            def _():
                all_of(recc.at[0], n, packed_rows, in_sem.at[2 + side])
                edge_copy(side).wait_send()
                pltpu.make_async_copy(edge_recv.at[side], edge_recv.at[side], edge_rs.at[0 if xs == 1 else side]).wait()

    sent_edges()
    def all_2(count, sem):
        got = recv2.at[pl.ds(0, count), :, pl.ds(0, frame), :]
        pltpu.make_async_copy(got, got, sem).wait()

    ensr[...] = pltpu.roll(whole(ensf), 1, 1) * scale
    ebuf[...] = jnp.zeros(ebuf.shape, f32)
    edge_ens = [pltpu.roll(row(ensf, k), 1, 1) * scale for k in (0, rows - 1)]
    halo_ens = [pltpu.roll(edge_recv[side, 0:lev, :], 1, 1) * scale for side in (0, 1)]

    def smooth_back(v):
        return 0.25 * v + 0.5 * pltpu.roll(v, lon - 1, 1) + 0.25 * pltpu.roll(v, lon - 2, 1)

    for i, group in enumerate(reversed(classes)):
        all_2(len(group), rs2.at[i])
        for step in group:
            forward2(2 * from_chip(step) + 1 - core).start()
    for side in (0, 1):

        @pl.when(has[side])
        def _():
            i = 0 if xs == 1 else side
            got = recvx.at[i, 1 - core, :, pl.ds(0, packed_rows), :]
            pltpu.make_async_copy(got, got, rsx.at[i]).wait()
            forwardx(i).start()

    all_2(n // 2, rs2f)

    over = iota((SUB, LANES), 0) < frame - block

    def across(parts):
        per_tile = LANES // SUB
        cols = [jnp.concatenate(parts[t * per_tile : (t + 1) * per_tile], axis=0).T for t in range(tiles)]
        return cols[0] if tiles == 1 else jnp.concatenate(cols, axis=1)

    ours = (quarter < 2) | (set_of == 0) | (set_of == 3)
    set_lanes = lane8 >= half

    def edges_at(i, d):
        e = recvx[i, d % 2, d // 2]
        b = pltpu.roll(pltpu.roll(e, half, 1), 5, 0)
        return jnp.where(row8 < 5, e, b), jnp.where(over, b, 0.0)

    def gather(g):
        sides = range(xs) if g else ()
        prev = [edges_at(i, n - 1)[1] for i in sides]
        parts = []
        for d in range(n):
            tile = recv2[d, g, 0:SUB, :] + jnp.where(over, recv2[(d - 1) % n, g, SUB : 2 * SUB, :], 0.0)
            if g:
                theirs = None
                for i in sides:
                    here, tail = edges_at(i, d)
                    v = here + prev[i]
                    if xs == 2:
                        v = jnp.where(has[i], v, 0.0)
                    theirs = v if theirs is None else theirs + v
                    prev[i] = tail
                tile = jnp.where(ours, tile, 0.0) + jnp.where(set_lanes, theirs, 0.0)
            parts.append(tile)
        return across(parts)

    c0 = gather(0)
    for side in (0, 1):

        @pl.when(has[side])
        def _():
            i = 0 if xs == 1 else side
            all_of(recvx.at[i, 0], n // 2, packed_rows, rsxf.at[i])

    c1 = gather(1)
    e0 = main - LANES
    wm = ensr[...] * jnp.concatenate([c0, c1[0:e0]], axis=0)
    w_up = jnp.where(kk == 0, 0.0, pltpu.roll(wm, 1, 0))
    w_dn = jnp.where(kk == rows - 1, 0.0, pltpu.roll(wm, main - 1, 0))
    zz = smooth_back(0.25 * (w_up + w_dn) + 0.5 * wm)
    for t in range(tiles):
        grad_ref[t] = zz[:, t * LANES : (t + 1) * LANES]
    for side, k, k_in in ((0, 0, 1), (1, rows - 1, rows - 2)):
        halo_at, extra_at = (e0, e0 + levp) if side == 0 else (e0 + 3 * levp, e0 + 2 * levp)
        we = edge_ens[side] * c1[extra_at : extra_at + lev]
        wh = halo_ens[side] * c1[halo_at : halo_at + lev]
        z_edge = smooth_back(0.5 * we + 0.25 * wh)
        z_in = smooth_back(0.25 * we)
        for t in range(tiles):
            cut = slice(t * LANES, (t + 1) * LANES)
            grad_ref.at[t][pl.ds(k, lev, stride=rows), :] += z_edge[:, cut]
            grad_ref.at[t][pl.ds(k_in, lev, stride=rows), :] += z_in[:, cut]

    for side in (0, 1):

        @pl.when(has[side])
        def _():
            i = 0 if xs == 1 else side
            all_of(recvx.at[0, 0], n // 2, packed_rows, ssx.at[i])
            all_of(recvx.at[0, 0], n // 2, packed_rows, ssx.at[xs + i])

    all_2(n - 1, ss2)


def writer(adv_ref, grad_ref, adv_out, grad_out, sem):
    copies = [
        pltpu.make_async_copy(grad_ref, grad_out, sem.at[0]),
        pltpu.make_async_copy(adv_ref, adv_out, sem.at[1]),
    ]
    for c in copies:
        c.start()
    for c in copies:
        c.wait()


def up_to(x, m):
    return -(-x // m) * m


def to_tiles(x):
    return x.reshape(-1, x.shape[3] // LANES, LANES).swapaxes(0, 1)


def shards(ensemble, alpha, lat_lower, lat_weight, background, obs_cell, obs_value, obs_precision):
    n, nb = lax.axis_size("mem"), lax.axis_size("band")
    members, lev, rows, lon = ensemble.shape
    fine_rows = lat_lower.shape[0]
    cells = background.shape[2]
    nobs = obs_cell.shape[1]
    fine_cols = cells // fine_rows
    scale = 1.0 / math.sqrt(members * n - 1)
    block = lon // n
    main = lev * rows
    kaps = main + 4 * RG
    assert n % 2 == 0 and members == 1 and block == SUB and rows == RG and lev <= RG and kaps == 2 * LANES
    assert fine_rows % RG == 0 and fine_cols % block == 0 and fine_cols // block == 3
    cfg = (n, nb, lev, rows, lon, fine_rows, fine_cols, scale)
    tiles = lon // LANES
    ng = fine_rows // RG
    gl = RG * RG
    wide = ng * gl
    gcells = RG * fine_cols
    xs = 1 if nb == 2 else 2
    dma = pltpu.SemaphoreType.DMA
    vm = pl.BlockSpec(memory_space=pltpu.VMEM)
    hbm = pl.BlockSpec(memory_space=pltpu.HBM)
    fr = 2 * SUB
    advected, gradient = pl.pallas_call(
        functools.partial(kernel, cfg),
        out_shape=(
            jax.ShapeDtypeStruct(background.shape, f32),
            jax.ShapeDtypeStruct((tiles, main, LANES), f32),
        ),
        in_specs=[hbm] * 8,
        out_specs=(vm, vm),
        scratch_shapes=[
            pltpu.VMEM((tiles, main, LANES), bf16),
            pltpu.VMEM((tiles, main, LANES), f32),
            pltpu.VMEM((1, fine_rows), jnp.int32),
            pltpu.VMEM((1, fine_rows), f32),
            pltpu.VMEM(background.shape, f32),
            pltpu.VMEM((1, nobs), jnp.int32),
            pltpu.VMEM(obs_value.shape, f32),
            pltpu.VMEM((1, nobs), f32),
            pltpu.VMEM((tiles, main, LANES), f32),
            pltpu.VMEM((tiles, main, LANES), f32),
            pltpu.VMEM((kaps, lon), f32),
            pltpu.VMEM((LANES, lon), f32),
            pltpu.VMEM((2, RG, lon), f32),
            pltpu.VMEM((2, RG, lon), f32),
            pltpu.VMEM((3, lon + SUB, LANES), f32),
            pltpu.VMEM((n // 2, 2, fr, LANES), f32),
            pltpu.VMEM((n // 2, fr, LANES), f32),
            pltpu.VMEM((n // 2, fr, LANES), f32),
            pltpu.VMEM((n // 2, fr, LANES), f32),
            pltpu.VMEM((n, SUB, LANES), f32),
            pltpu.VMEM((n, SUB, LANES), f32),
            pltpu.VMEM((xs, n, SUB, LANES), f32),
            pltpu.VMEM((xs, n, SUB, LANES), f32),
            pltpu.VMEM((kaps, wide), bf16),
            pltpu.VMEM((kaps, wide), bf16),
            pltpu.VMEM((wide, kaps), bf16),
            pltpu.VMEM((wide, kaps), bf16),
            pltpu.VMEM((gl, 2 * gcells), bf16),
            pltpu.VMEM((gl, 2 * nobs), bf16),
            pltpu.VMEM((LANES, 2 * nobs), bf16),
            pltpu.VMEM((4 * SUB, wide), f32),
            pltpu.VMEM((4 * SUB, wide), f32),
            pltpu.VMEM((4 * SUB, wide), f32),
            pltpu.VMEM((2, SUB, LANES), f32),
            pltpu.VMEM((2, SUB, LANES), f32),
            pltpu.VMEM((4 * SUB, wide), f32),
            pltpu.VMEM((2, fr, LANES), f32),
            pltpu.VMEM((n, 2, fr, LANES), f32),
            pltpu.VMEM((xs, SUB, LANES), f32),
            pltpu.VMEM((xs, 2, n // 2, SUB, LANES), f32),
            pltpu.VMEM((tiles, main, LANES), f32),
            pltpu.VMEM((main, lon), f32),
            dma((8,)),
            dma((xs,)),
            dma,
            dma,
            dma,
            dma((xs,)),
            dma,
            dma,
            dma((len(chip_order(n // 2)[1]),)),
            dma,
            dma((2 * xs,)),
            dma((xs,)),
            dma((xs,)),
        ],
        compiler_params=pltpu.CompilerParams(collective_id=0, has_side_effects=True, vmem_limit_bytes=48 * 2**20),
    )(
        *(
            pltpu.with_memory_space_constraint(v, pltpu.HBM)
            for v in (
                to_tiles(ensemble),
                to_tiles(alpha),
                lat_lower.reshape(1, fine_rows),
                lat_weight.reshape(1, fine_rows),
                background,
                obs_cell,
                obs_value,
                obs_precision,
            )
        )
    )
    advected, gradient = pl.pallas_call(
        writer,
        out_shape=(
            jax.ShapeDtypeStruct(background.shape, f32),
            jax.ShapeDtypeStruct((tiles, main, LANES), f32),
        ),
        in_specs=[vm, vm],
        out_specs=(hbm, hbm),
        scratch_shapes=[dma((2,))],
        compiler_params=pltpu.CompilerParams(vmem_limit_bytes=2**20),
    )(advected, gradient)
    return advected, gradient.swapaxes(0, 1).reshape(members, lev, rows, lon)


def solution(mesh):
    return jax.shard_map(
        shards,
        mesh=mesh,
        in_specs=(
            P("mem", None, "band", None),
            P("mem", None, "band", None),
            P("band"),
            P("band"),
            P(None, ("band", "mem"), None),
            P(("band", "mem"), None),
            P(None, ("band", "mem"), None),
            P(("band", "mem"), None),
        ),
        out_specs=(P(None, ("band", "mem"), None), P("mem", None, "band", None)),
        check_vma=False,
    )
```

```python
import functools
import math

import jax
import jax.numpy as jnp
from jax import lax
from jax.experimental import pallas as pl
from jax.experimental.pallas import tpu as pltpu
from jax.sharding import PartitionSpec as P

advect_rate = 0.25
LANES = 128
SUB = 8
RG = 16
f32 = jnp.float32
bf16 = jnp.bfloat16


def split2(x):
    hi = x.astype(bf16)
    lo = (x - hi.astype(f32)).astype(bf16)
    return hi, lo


def split2f(x):
    hi = x.astype(bf16).astype(f32)
    return hi, x - hi


def dims(a, b, ca, cb):
    return lax.dot_general(a, b, (((ca,), (cb,)), ((), ())), preferred_element_type=f32)


def iota(shape, d):
    return lax.broadcasted_iota(jnp.int32, shape, d)


def smooth_lon(x):
    n = x.shape[1]
    return 0.25 * pltpu.roll(x, 1, 1) + 0.5 * x + 0.25 * pltpu.roll(x, n - 1, 1)


def lon_weights(ratio):
    def parts(shift):
        num = 2 * shift + 1 + ratio
        return num // (2 * ratio), (num % (2 * ratio)) / (2 * ratio)

    def taps(shift):
        q, f = parts(shift)
        w = [0.0, 0.0, 0.0]
        for at, v in ((q, 1.0 - f), (q + 1, f)):
            if v:
                w[at] += v
        return w

    value = [taps(b) for b in range(ratio)]
    slope = [[0.5 * (p - m) for p, m in zip(taps(b + 1), taps(b - 1))] for b in range(ratio)]
    return value, slope


def combine(weights, parts):
    out = None
    for w, p in zip(weights, parts):
        if w == 0.0:
            continue
        term = p if w == 1.0 else w * p
        out = term if out is None else out + term
    return out


def chip_order(chips):
    ring = 4 if chips % 4 == 0 else chips
    rest = chips // ring

    def hops(step):
        return min(step[0], ring - step[0]) + min(step[1], rest - step[1])

    steps = sorted(((a, b) for a in range(ring) for b in range(rest)), key=lambda s: -hops(s))
    classes = [[s for s in steps if hops(s) == h] for h in sorted({hops(s) for s in steps if hops(s)}, reverse=True)]
    return steps, classes, ring, rest


def kernel(
    cfg,
    ens_hbm,
    alpha_hbm,
    low_hbm,
    wt_hbm,
    bg_hbm,
    cell_hbm,
    val_hbm,
    prec_hbm,
    adv_ref,
    grad_ref,
    ens_in,
    alpha,
    low,
    wt,
    bg,
    cell,
    val,
    prec,
    ensf,
    plain,
    part,
    xpart,
    edge_send,
    edge_recv,
    flat,
    frames,
    pre_recv,
    psum,
    recv1,
    eloc,
    rece,
    ecr,
    recc,
    table_hi,
    table_lo,
    back_hi,
    back_lo,
    zbuf,
    rbuf,
    abuf,
    fine_bg,
    obs_a,
    obs_b,
    fe_send,
    fe_recv,
    advbuf,
    send2,
    recv2,
    sendx,
    recvx,
    ebuf,
    ensr,
    in_sem,
    edge_rs,
    pre_rs,
    rs1,
    rse,
    rsc,
    fe_rs,
    ss2,
    rs2,
    rs2f,
    ssx,
    rsx,
    rsxf,
):
    n, nb, lev, rows, lon, fine_rows, fine_cols, scale = cfg
    block = lon // n
    frame = block + 2
    ratio = fine_cols // block
    main = lev * rows
    tiles = lon // LANES
    ng = fine_rows // RG
    gcells = RG * fine_cols
    gl = RG * RG
    levp = RG
    xs = recvx.shape[0]
    me = lax.axis_index("mem")
    band = lax.axis_index("band")
    has_up = band > 0
    has_down = band < nb - 1
    has = (has_up, has_down)
    wv, ws = lon_weights(ratio)

    barrier = pltpu.get_barrier_semaphore()

    core = lax.rem(me, 2)
    chip = me // 2
    partner = me + 1 - 2 * core
    chips = n // 2
    far_first, classes, ring, rest = chip_order(chips)
    ring_at, rest_at = chip // rest, lax.rem(chip, rest)

    def to_chip(step):
        return lax.rem(ring_at + step[0], ring) * rest + lax.rem(rest_at + step[1], rest)

    def from_chip(step):
        return to_chip(((ring - step[0]) % ring, (rest - step[1]) % rest))

    side_band = (band - 1, band + 1)
    for step in far_first:
        home = step == (0, 0)
        for c in (core, 1 - core):
            if nb == 2:
                pl.semaphore_signal(barrier, inc=1, device_id={"mem": 2 * to_chip(step) + c, "band": 1 - band})
            else:
                for side in (0, 1):

                    @pl.when(has[side])
                    def _():
                        pl.semaphore_signal(
                            barrier, inc=1, device_id={"mem": 2 * to_chip(step) + c, "band": side_band[side]}
                        )

            if not (home and c is core):
                pl.semaphore_signal(barrier, inc=1, device_id={"mem": 2 * to_chip(step) + c})

    loads = [
        pltpu.make_async_copy(src, dst, in_sem.at[i])
        for i, (src, dst) in enumerate(
            (
                (alpha_hbm, alpha),
                (ens_hbm, ens_in),
                (bg_hbm, bg),
                (low_hbm, low),
                (wt_hbm, wt),
                (cell_hbm, cell),
                (val_hbm, val),
                (prec_hbm, prec),
            )
        )
    ]
    for c in loads:
        c.start()

    part[main:, :] = jnp.zeros((part.shape[0] - main, lon), f32)
    xpart[...] = jnp.zeros(xpart.shape, f32)
    edge_send[...] = jnp.zeros(edge_send.shape, f32)
    fe_send[...] = jnp.zeros(fe_send.shape, f32)

    loads[0].wait()
    loads[1].wait()

    def whole(ref):
        parts = [ref[t] for t in range(tiles)]
        return parts[0] if tiles == 1 else jnp.concatenate(parts, axis=1)

    def row(ref, k):
        parts = [ref.at[t][pl.ds(k, lev, stride=rows), :] for t in range(tiles)]
        return parts[0] if tiles == 1 else jnp.concatenate(parts, axis=1)

    for t in range(tiles):
        ensf[t] = ens_in[t].astype(f32)
    al = whole(alpha)
    en = whole(ensf)
    kk = iota((main, lon), 0) % rows
    a_up = jnp.where(kk == 0, 0.0, pltpu.roll(al, 1, 0))
    a_dn = jnp.where(kk == rows - 1, 0.0, pltpu.roll(al, main - 1, 0))
    z = smooth_lon(0.25 * (a_up + a_dn) + 0.5 * al) * en * scale
    for t in range(tiles):
        plain[t] = z[:, t * LANES : (t + 1) * LANES]
    part[0:main, :] = z
    edges = []
    for side, k in ((0, 0), (1, rows - 1)):
        a_edge = smooth_lon(row(alpha, k)) * (0.25 * scale)
        e_edge = row(ensf, k)
        edges.append((a_edge, e_edge, row(plain, k)))
        edge_send[side, 0:lev, :] = e_edge
        at = main + side * 2 * levp
        for i, v in enumerate((a_edge, e_edge) if side == 0 else (e_edge, a_edge)):
            part[at + i * levp : at + i * levp + lev, :] = v
    (a_0, e_0, p_0), (a_1, e_1, p_1) = edges
    zero = jnp.zeros_like(a_0)
    sets_up = [zero, p_0, a_0, e_0]
    sets_down = [e_1, a_1, p_1, zero]
    if xs == 1:
        sets = [jnp.where(has_up, u, d) for u, d in zip(sets_up, sets_down)]
    else:
        sets = sets_up + sets_down
    for i, v in enumerate(sets):
        xpart[i * levp : i * levp + lev, :] = v

    def lay(g, rows_of):
        rows_of = pltpu.roll(rows_of, 1, 1)
        for t in range(tiles):
            flat[g, t * LANES : (t + 1) * LANES, :] = rows_of[:, t * LANES : (t + 1) * LANES].T
        flat[g, lon : lon + SUB, :] = flat[g, 0:SUB, :]

    lay(0, part[0:LANES, :])
    lay(1, part[LANES : 2 * LANES, :])
    lay(2, xpart[...])

    lane8 = iota((SUB, LANES), 1)
    row8 = iota((SUB, LANES), 0)
    low_half = lane8 < LANES // 2
    half = LANES // 2

    def tile_of(g, d):
        return flat[g, d * SUB : (d + 1) * SUB, :]

    def views(d):
        v, x = tile_of(1, d), tile_of(2, d)
        flip, flipx = pltpu.roll(v, half, 1), pltpu.roll(x, half, 1)
        return v, flip, x, flipx, pltpu.roll(flip, 5, 0), pltpu.roll(v, 3, 0), pltpu.roll(flipx, 3, 0), pltpu.roll(x, 3, 0)

    cur = views(0)
    for d in range(n):
        nxt = views(d + 1)
        v, flip, x, flipx, r5, v3, fx3, x3 = cur
        packed = jnp.where(low_half, pltpu.roll(v, 2, 0), jnp.where(row8 < 5, r5, nxt[4]))
        frames[d // 2, d % 2, 0:SUB, :] = tile_of(0, d)
        frames[d // 2, d % 2, SUB : 2 * SUB, :] = jnp.where(row8 < 2, tile_of(0, d + 1), packed)
        eloc[d] = jnp.where(low_half, flip, jnp.where(row8 < 3, v3, nxt[5]))
        ecr[0, d] = jnp.where(low_half, x, jnp.where(row8 < 3, fx3, nxt[6]))
        if xs == 2:
            ecr[1, d] = jnp.where(low_half, flipx, jnp.where(row8 < 3, x3, nxt[7]))
        cur = nxt

    loads[2].wait()
    row32 = iota((4 * SUB, gcells), 0)
    col_of = jnp.where(row32 < ratio * SUB, (row32 % SUB) * ratio + row32 // SUB, -1)
    pick = (iota((4 * SUB, gcells), 1) % fine_cols == col_of).astype(f32).astype(bf16)
    pick2 = jnp.concatenate([pick, pick], axis=1)
    in_row = iota((RG, gcells), 1) // fine_cols == iota((RG, gcells), 0)
    zbuf[main:, :] = jnp.zeros((gl - main, 2 * gcells), bf16)
    back = bg[:, 0, :]
    for g in range(ng):
        hi, lo = split2f(back[:, g * gcells : (g + 1) * gcells])
        for l in range(lev):
            at = slice(l * RG, (l + 1) * RG)
            zbuf[at, 0:gcells] = jnp.where(in_row, jnp.broadcast_to(hi[l : l + 1], (RG, gcells)), 0.0).astype(bf16)
            zbuf[at, gcells : 2 * gcells] = jnp.where(in_row, jnp.broadcast_to(lo[l : l + 1], (RG, gcells)), 0.0).astype(bf16)
        fine_bg[:, g * gl : (g + 1) * gl] = dims(pick2, zbuf[...], 1, 1)
    for c in loads[3:]:
        c.wait()

    if nb == 2:
        pl.semaphore_wait(barrier, 2 * n - 1)
    else:
        pl.semaphore_wait(barrier, n - 1 + n * (has_up.astype(jnp.int32) + has_down.astype(jnp.int32)))

    pre_copy = pltpu.make_async_remote_copy(
        src_ref=frames.at[:, core],
        dst_ref=pre_recv,
        send_sem=in_sem.at[0],
        recv_sem=pre_rs,
        device_id={"mem": partner},
    )
    pre_copy.start()
    packed_rows = frame // 2

    def copyc(side, dst):
        i = 0 if xs == 1 else 1 - side
        return pltpu.make_async_remote_copy(
            src_ref=ecr.at[0 if xs == 1 else side, dst, pl.ds(0, packed_rows), :],
            dst_ref=recc.at[i, me, pl.ds(0, packed_rows), :],
            send_sem=in_sem.at[2 + side],
            recv_sem=rsc.at[i],
            device_id={"mem": dst, "band": side_band[side]},
        )

    def copye(dst):
        return pltpu.make_async_remote_copy(
            src_ref=eloc.at[dst, pl.ds(0, packed_rows), :],
            dst_ref=rece.at[me, pl.ds(0, packed_rows), :],
            send_sem=in_sem.at[1],
            recv_sem=rse,
            device_id={"mem": dst},
        )

    def edge_copy(side):
        return pltpu.make_async_remote_copy(
            src_ref=edge_send.at[side],
            dst_ref=edge_recv.at[1 - side],
            send_sem=in_sem.at[6 + side],
            recv_sem=edge_rs.at[0 if xs == 1 else 1 - side],
            device_id={"band": side_band[side]},
        )

    for side in (0, 1):

        @pl.when(has[side])
        def _():
            for step in far_first:
                for c in (core, 1 - core):
                    copyc(side, 2 * to_chip(step) + c).start()

        @pl.when(jnp.logical_not(has[side]))
        def _():
            edge_recv[side] = jnp.zeros(edge_recv.shape[1:], f32)

    for step in far_first:
        for c in (core, 1 - core):
            if step != (0, 0) or c is not core:
                copye(2 * to_chip(step) + c).start()
    for side in (0, 1):

        @pl.when(has[side])
        def _():
            edge_copy(side).start()

    rece[me] = eloc[me]

    first = fine_bg[0:1, :]
    last = fine_bg[ratio * SUB - 1 : ratio * SUB, :]
    for t in range(ng * gl // LANES):
        fe_send[0, t : t + 1, :] = first[:, t * LANES : (t + 1) * LANES]
        fe_send[1, t : t + 1, :] = last[:, t * LANES : (t + 1) * LANES]

    def fe_copy(side):
        return pltpu.make_async_remote_copy(
            src_ref=fe_send.at[side],
            dst_ref=fe_recv.at[1 - side],
            send_sem=in_sem.at[5],
            recv_sem=fe_rs,
            device_id={"mem": lax.rem(me + (n - 1 if side == 0 else 1), n)},
        )

    fe_copy(0).start()
    fe_copy(1).start()

    lane = iota((SUB, LANES), 1)
    wide = ng * gl

    def per_row(v):
        v = jnp.concatenate([v, jnp.zeros((1, LANES - fine_rows), f32)], axis=1)
        return jnp.broadcast_to(v, (SUB, LANES))

    def tiled(v, g):
        r = v if g == 0 else pltpu.roll(v, LANES - g * RG, 1)
        r = jnp.where(lane < RG, r, 0.0)
        for s in (RG, 2 * RG, 4 * RG):
            r = r + pltpu.roll(r, s, 1)
        return jnp.concatenate([r, r], axis=0)

    low_rows, wt_rows = per_row(low[...].astype(f32)), per_row(wt[...])
    down = lambda v: jnp.concatenate([v] * (LANES // SUB), axis=0).T
    low_col, wt_col = down(low_rows), down(wt_rows)
    lane16 = iota((RG, LANES), 1)
    row16 = iota((RG, LANES), 0)
    lev_of = lane16 // RG
    set_rows = (-1, 0, rows - 1, rows)
    table_hi[...] = jnp.zeros(table_hi.shape, bf16)
    table_lo[...] = jnp.zeros(table_lo.shape, bf16)
    back_hi[...] = jnp.zeros(back_hi.shape, bf16)
    back_lo[...] = jnp.zeros(back_lo.shape, bf16)
    halves = gl // LANES
    per = LANES // RG

    def weigh(k, lo_k, w):
        w_hi, w_lo = split2f(w)
        o_hi, o_lo = split2f(1.0 - w)
        m0, m1 = k == lo_k, k == lo_k + 1.0
        return (
            jnp.where(m0, o_hi, jnp.where(m1, w_hi, 0.0)),
            jnp.where(m0, o_lo, jnp.where(m1, w_lo, 0.0)),
        )

    def put(ref, r, c, v, keep):
        ref[r : r + RG, c : c + LANES] = jnp.where(keep, v, 0.0).astype(bf16)

    for g in range(ng):
        lo_t, w_t = tiled(low_rows, g), tiled(wt_rows, g)
        main_t = weigh(row16.astype(f32), lo_t, w_t)
        set_t = [weigh(jnp.full((RG, LANES), float(k), f32), lo_t, w_t) for k in set_rows]
        for ref, which in ((table_hi, 0), (table_lo, 1)):
            for l in range(lev):
                put(ref, l * RG, g * gl + l // per * LANES, main_t[which], lev_of == l % per)
            for s in range(4):
                for h in range(halves):
                    put(ref, main + s * levp, g * gl + h * LANES, set_t[s][which], (row16 == lev_of + h * per) & (row16 < lev))
        lo_c, w_c = low_col[g * RG : (g + 1) * RG], wt_col[g * RG : (g + 1) * RG]
        for h in range(halves):
            kap = lane16 + h * LANES
            e = kap - main
            es = e // levp
            ek = jnp.where(es == 0, -1, jnp.where(es == 1, 0, jnp.where(es == 2, rows - 1, rows)))
            k_of = jnp.where(e < 0, kap % rows, ek).astype(f32)
            l_of = jnp.where(e < 0, kap // rows, e % levp)
            back_t = weigh(k_of, lo_c, w_c)
            for ref, which in ((back_hi, 0), (back_lo, 1)):
                for l in range(lev):
                    if (h + 1) * LANES > main or l // per == h:
                        put(ref, g * gl + l * RG, h * LANES, back_t[which], l_of == l)

    pre_copy.wait_recv()
    for j in range(n // 2):
        psum[j] = frames[j, 1 - core] + pre_recv[j]

    used = frame + packed_rows

    def copy1(dst):
        return pltpu.make_async_remote_copy(
            src_ref=psum.at[dst, pl.ds(0, used), :],
            dst_ref=recv1.at[chip, pl.ds(0, used), :],
            send_sem=in_sem.at[4],
            recv_sem=rs1,
            device_id={"mem": 2 * dst + 1 - core},
        )

    for step in far_first:
        copy1(to_chip(step)).start()

    nobs = cell.shape[1]
    crow = cell[...] // fine_cols
    ccol = cell[...] % fine_cols
    r32 = iota((4 * SUB, nobs), 0)
    col_o = jnp.where(r32 < ratio * SUB, (r32 % SUB) * ratio + r32 // SUB, -1)
    hot = (col_o == ccol).astype(f32).astype(bf16)
    hot2 = jnp.concatenate([hot, hot], axis=1)
    pr = prec[...]
    p_hi, p_lo = split2f(pr)
    v_hi, v_lo = split2f(val[:, 0, :] * pr)
    rbuf[main:, :] = jnp.zeros((gl - main, 2 * nobs), bf16)
    for g in range(ng):
        at_row = iota((RG, nobs), 0) + g * RG == crow
        for l in range(lev):
            at = slice(l * RG, (l + 1) * RG)
            rbuf[at, 0:nobs] = jnp.where(at_row, jnp.broadcast_to(v_hi[l : l + 1], (RG, nobs)), 0.0).astype(bf16)
            rbuf[at, nobs : 2 * nobs] = jnp.where(at_row, jnp.broadcast_to(v_lo[l : l + 1], (RG, nobs)), 0.0).astype(bf16)
        obs_b[:, g * gl : (g + 1) * gl] = dims(hot2, rbuf[...], 1, 1)
        ph = jnp.where(at_row, jnp.broadcast_to(p_hi, (RG, nobs)), 0.0).astype(bf16)
        plo = jnp.where(at_row, jnp.broadcast_to(p_lo, (RG, nobs)), 0.0).astype(bf16)
        for j in range(LANES // RG):
            abuf[j * RG : (j + 1) * RG, 0:nobs] = ph
            abuf[j * RG : (j + 1) * RG, nobs : 2 * nobs] = plo
        oa = dims(hot2, abuf[...], 1, 1)
        for j in range(gl // LANES):
            obs_a[:, g * gl + j * LANES : g * gl + (j + 1) * LANES] = oa

    pltpu.make_async_copy(fe_recv, fe_recv, fe_rs).wait()
    nt = wide // LANES
    left = jnp.concatenate([fe_recv[0, t : t + 1, :] for t in range(nt)], axis=1)
    right = jnp.concatenate([fe_recv[1, t : t + 1, :] for t in range(nt)], axis=1)
    fb = [fine_bg[b * SUB : (b + 1) * SUB, :] for b in range(ratio)]
    arow = iota((SUB, wide), 0)
    before0 = jnp.where(arow == 0, left, pltpu.roll(fb[ratio - 1], 1, 0))
    after_last = jnp.where(arow == SUB - 1, right, pltpu.roll(fb[0], SUB - 1, 0))
    chain = [before0] + fb + [after_last]
    slope_bg = [0.5 * (chain[b + 2] - chain[b]) for b in range(ratio)]

    def all_of(ref, count, height, sem):
        got = ref.at[pl.ds(0, count), pl.ds(0, height), :]
        pltpu.make_async_copy(got, got, sem).wait()

    all_of(rece, n - 1, packed_rows, rse)
    for side in (0, 1):

        @pl.when(has[side])
        def _():
            i = 0 if xs == 1 else side
            all_of(recc.at[i], n, packed_rows, rsc.at[i])

    prods, plains = [], []
    for i in range(xs):
        prod = rece[0] * recc[i, 0]
        only = recc[i, 0]
        for s in range(1, n):
            prod = prod + rece[s] * recc[i, s]
            only = only + recc[i, s]
        prods.append(prod)
        plains.append(only)
    set_of = (lane8 % half) // levp
    edge_sum = jnp.where(
        set_of < 2, jnp.where(has_up, prods[0], 0.0), jnp.where(has_down, prods[-1], 0.0)
    )
    from_up = jnp.where(has_up, pltpu.roll(plains[0], LANES - 2 * levp, 1), 0.0)
    from_down = jnp.where(has_down, pltpu.roll(plains[-1], 2 * levp, 1), 0.0)
    edge_sum = edge_sum + jnp.where(set_of == 0, from_up, jnp.where(set_of == 3, from_down, 0.0))
    edge_a = pltpu.roll(edge_sum, half, 1)
    edge_b = pltpu.roll(edge_sum, 5, 0)

    all_of(recv1, n // 2, used, rs1)
    total = recv1[0]
    for s in range(1, n // 2):
        total = total + recv1[s]
    m = total[SUB:]
    m_a = pltpu.roll(m, SUB - 2, 0)
    m_b = pltpu.roll(pltpu.roll(m, half, 1), 3, 0)
    x_a = jnp.where(low_half, m_a, edge_a)
    x_b = jnp.where(low_half, m_b, edge_b)
    x = jnp.concatenate([total, jnp.concatenate([jnp.where(row8 < 5, x_a, x_b), x_b], axis=0)], axis=1)
    x_hi, x_lo = split2f(x)
    x2 = jnp.concatenate([x_hi, x_lo], axis=0).astype(bf16)
    y = dims(x2, table_hi[...], 1, 0)
    y = y[0:16] + y[16:32] + dims(x_hi.astype(bf16), table_lo[...], 1, 0)
    taps = [y[0:SUB]] + [pltpu.roll(y, 2 * SUB - d, 0)[0:SUB] for d in (1, 2)]

    us, vs, moved = [], [], []
    for b in range(ratio):
        state = fb[b] + combine(wv[b], taps)
        slope = slope_bg[b] + combine(ws[b], taps)
        factor = 1.0 - advect_rate * slope
        mv = state * factor
        at = slice(b * SUB, (b + 1) * SUB)
        cot = obs_a[at, :] * mv - obs_b[at, :]
        us.append(cot * factor)
        vs.append((-advect_rate) * (state * cot))
        moved.append(mv)
    gl_v = None
    for d in range(3):
        t = combine([wv[b][d] for b in range(ratio)] + [ws[b][d] for b in range(ratio)], us + vs)
        t = jnp.concatenate([t, jnp.zeros_like(t)], axis=0)
        gl_v = t if d == 0 else gl_v + pltpu.roll(t, d, 0)
    g_hi, g_lo = split2f(gl_v)
    g2 = jnp.concatenate([g_hi, g_lo], axis=0).astype(bf16)
    gr = dims(g2, back_hi[...], 1, 0)
    gr = gr[0:16] + gr[16:32] + dims(g_hi.astype(bf16), back_lo[...], 1, 0)
    for g in (0, 1):
        send2[g] = gr[:, g * LANES : (g + 1) * LANES]
    def slot2(src):
        return recv2.at[src, :, pl.ds(0, frame), :]

    def copy2(dst, sem):
        return pltpu.make_async_remote_copy(
            src_ref=send2.at[:, pl.ds(0, frame), :],
            dst_ref=slot2(me),
            send_sem=ss2,
            recv_sem=sem,
            device_id={"mem": dst},
        )

    def forward2(src):
        return pltpu.make_async_remote_copy(
            src_ref=slot2(src),
            dst_ref=slot2(src),
            send_sem=ss2,
            recv_sem=rs2f,
            device_id={"mem": partner},
        )

    def copyx(side, dst):
        i = 0 if xs == 1 else 1 - side
        return pltpu.make_async_remote_copy(
            src_ref=sendx.at[0 if xs == 1 else side, pl.ds(0, packed_rows), :],
            dst_ref=recvx.at[i, core, chip, pl.ds(0, packed_rows), :],
            send_sem=ssx.at[0 if xs == 1 else side],
            recv_sem=rsx.at[i],
            device_id={"mem": dst, "band": side_band[side]},
        )

    def forwardx(i):
        got = recvx.at[i, 1 - core, :, pl.ds(0, packed_rows), :]
        return pltpu.make_async_remote_copy(
            src_ref=got,
            dst_ref=got,
            send_sem=ssx.at[xs + i],
            recv_sem=rsxf.at[i],
            device_id={"mem": partner},
        )

    def send_class(i):
        for step in classes[i]:
            copy2(2 * to_chip(step) + 1 - core, rs2.at[len(classes) - 1 - i]).start()

    v0, v1 = gr[0:SUB, LANES:], gr[SUB:, LANES:]
    quarter = lane8 // (2 * levp)
    v32, v96, w32, w96 = (pltpu.roll(v, r, 1) for v in (v0, v1) for r in (2 * levp, 6 * levp))

    def late(a, b):
        return jnp.where(row8 < 3, pltpu.roll(a, 3, 0), pltpu.roll(b, 3, 0))

    def pack_for(up_there):
        near = jnp.where(up_there, v32, v96)
        rest_cols = late(jnp.where(up_there, v96, v32), jnp.where(up_there, w96, w32))
        q = jnp.where(up_there, quarter - 1, quarter)
        return jnp.where(q == 2, near, jnp.where(q == 0, rest_cols, 0.0))

    if xs == 1:
        sendx[0] = pack_for(has_up)
    else:
        for side in (0, 1):
            sendx[side] = pack_for(side == 0)

    for side in (0, 1):

        @pl.when(has[side])
        def _():
            for step in far_first:
                copyx(side, 2 * to_chip(step) + 1 - core).start()

    for i in range(len(classes)):
        send_class(i)
    copy2(partner, rs2f).start()
    for g in (0, 1):
        recv2[me, g] = send2[g]

    advbuf[...] = jnp.concatenate(moved + [jnp.zeros((SUB, wide), f32)], axis=0)
    pickt = jnp.concatenate([pick, pick], axis=0)
    for g in range(ng):
        hi, lo = split2(advbuf[:, g * gl : g * gl + main])
        e = dims(jnp.concatenate([hi, lo], axis=0), pickt, 0, 0)
        for l in range(lev):
            v = jnp.where(in_row, e[l * RG : (l + 1) * RG], 0.0)
            adv_ref[l, :, g * gcells : (g + 1) * gcells] = jnp.sum(v, axis=0, keepdims=True)

    def sent_edges():
        pre_copy.wait_send()
        all_of(rece, n - 1, packed_rows, in_sem.at[1])
        all_of(recv1, n // 2, used, in_sem.at[4])
        pltpu.make_async_copy(fe_recv, fe_recv, in_sem.at[5]).wait()
        for side in (0, 1):

            @pl.when(has[side])
            def _():
                all_of(recc.at[0], n, packed_rows, in_sem.at[2 + side])
                edge_copy(side).wait_send()
                pltpu.make_async_copy(edge_recv.at[side], edge_recv.at[side], edge_rs.at[0 if xs == 1 else side]).wait()

    sent_edges()
    def all_2(count, sem):
        got = recv2.at[pl.ds(0, count), :, pl.ds(0, frame), :]
        pltpu.make_async_copy(got, got, sem).wait()

    ensr[...] = pltpu.roll(whole(ensf), 1, 1) * scale
    ebuf[...] = jnp.zeros(ebuf.shape, f32)
    edge_ens = [pltpu.roll(row(ensf, k), 1, 1) * scale for k in (0, rows - 1)]
    halo_ens = [pltpu.roll(edge_recv[side, 0:lev, :], 1, 1) * scale for side in (0, 1)]

    def smooth_back(v):
        return 0.25 * v + 0.5 * pltpu.roll(v, lon - 1, 1) + 0.25 * pltpu.roll(v, lon - 2, 1)

    for i, group in enumerate(reversed(classes)):
        all_2(len(group), rs2.at[i])
        for step in group:
            forward2(2 * from_chip(step) + 1 - core).start()
    for side in (0, 1):

        @pl.when(has[side])
        def _():
            i = 0 if xs == 1 else side
            got = recvx.at[i, 1 - core, :, pl.ds(0, packed_rows), :]
            pltpu.make_async_copy(got, got, rsx.at[i]).wait()
            forwardx(i).start()

    all_2(n // 2, rs2f)

    over = iota((SUB, LANES), 0) < frame - block

    def across(parts):
        per_tile = LANES // SUB
        cols = [jnp.concatenate(parts[t * per_tile : (t + 1) * per_tile], axis=0).T for t in range(tiles)]
        return cols[0] if tiles == 1 else jnp.concatenate(cols, axis=1)

    ours = (quarter < 2) | (set_of == 0) | (set_of == 3)
    set_lanes = lane8 >= half

    def edges_at(i, d):
        e = recvx[i, d % 2, d // 2]
        b = pltpu.roll(pltpu.roll(e, half, 1), 5, 0)
        return jnp.where(row8 < 5, e, b), jnp.where(over, b, 0.0)

    def gather(g):
        sides = range(xs) if g else ()
        prev = [edges_at(i, n - 1)[1] for i in sides]
        parts = []
        for d in range(n):
            tile = recv2[d, g, 0:SUB, :] + jnp.where(over, recv2[(d - 1) % n, g, SUB : 2 * SUB, :], 0.0)
            if g:
                theirs = None
                for i in sides:
                    here, tail = edges_at(i, d)
                    v = here + prev[i]
                    if xs == 2:
                        v = jnp.where(has[i], v, 0.0)
                    theirs = v if theirs is None else theirs + v
                    prev[i] = tail
                tile = jnp.where(ours, tile, 0.0) + jnp.where(set_lanes, theirs, 0.0)
            parts.append(tile)
        return across(parts)

    c0 = gather(0)
    for side in (0, 1):

        @pl.when(has[side])
        def _():
            i = 0 if xs == 1 else side
            all_of(recvx.at[i, 0], n // 2, packed_rows, rsxf.at[i])

    c1 = gather(1)
    e0 = main - LANES
    wm = ensr[...] * jnp.concatenate([c0, c1[0:e0]], axis=0)
    w_up = jnp.where(kk == 0, 0.0, pltpu.roll(wm, 1, 0))
    w_dn = jnp.where(kk == rows - 1, 0.0, pltpu.roll(wm, main - 1, 0))
    zz = smooth_back(0.25 * (w_up + w_dn) + 0.5 * wm)
    for t in range(tiles):
        grad_ref[t] = zz[:, t * LANES : (t + 1) * LANES]
    for side, k, k_in in ((0, 0, 1), (1, rows - 1, rows - 2)):
        halo_at, extra_at = (e0, e0 + levp) if side == 0 else (e0 + 3 * levp, e0 + 2 * levp)
        we = edge_ens[side] * c1[extra_at : extra_at + lev]
        wh = halo_ens[side] * c1[halo_at : halo_at + lev]
        z_edge = smooth_back(0.5 * we + 0.25 * wh)
        z_in = smooth_back(0.25 * we)
        for t in range(tiles):
            cut = slice(t * LANES, (t + 1) * LANES)
            grad_ref.at[t][pl.ds(k, lev, stride=rows), :] += z_edge[:, cut]
            grad_ref.at[t][pl.ds(k_in, lev, stride=rows), :] += z_in[:, cut]

    for side in (0, 1):

        @pl.when(has[side])
        def _():
            i = 0 if xs == 1 else side
            all_of(recvx.at[0, 0], n // 2, packed_rows, ssx.at[i])
            all_of(recvx.at[0, 0], n // 2, packed_rows, ssx.at[xs + i])

    all_2(n - 1, ss2)


def writer(adv_ref, grad_ref, adv_out, grad_out, sem):
    copies = [
        pltpu.make_async_copy(grad_ref, grad_out, sem.at[0]),
        pltpu.make_async_copy(adv_ref, adv_out, sem.at[1]),
    ]
    for c in copies:
        c.start()
    for c in copies:
        c.wait()


def up_to(x, m):
    return -(-x // m) * m


def to_tiles(x):
    return x.reshape(-1, x.shape[3] // LANES, LANES).swapaxes(0, 1)


def shards(ensemble, alpha, lat_lower, lat_weight, background, obs_cell, obs_value, obs_precision):
    n, nb = lax.axis_size("mem"), lax.axis_size("band")
    members, lev, rows, lon = ensemble.shape
    fine_rows = lat_lower.shape[0]
    cells = background.shape[2]
    nobs = obs_cell.shape[1]
    fine_cols = cells // fine_rows
    scale = 1.0 / math.sqrt(members * n - 1)
    block = lon // n
    main = lev * rows
    kaps = main + 4 * RG
    assert n % 2 == 0 and members == 1 and block == SUB and rows == RG and lev <= RG and kaps == 2 * LANES
    assert fine_rows % RG == 0 and fine_cols % block == 0 and fine_cols // block == 3
    cfg = (n, nb, lev, rows, lon, fine_rows, fine_cols, scale)
    tiles = lon // LANES
    ng = fine_rows // RG
    gl = RG * RG
    wide = ng * gl
    gcells = RG * fine_cols
    xs = 1 if nb == 2 else 2
    dma = pltpu.SemaphoreType.DMA
    vm = pl.BlockSpec(memory_space=pltpu.VMEM)
    hbm = pl.BlockSpec(memory_space=pltpu.HBM)
    fr = 2 * SUB
    advected, gradient = pl.pallas_call(
        functools.partial(kernel, cfg),
        out_shape=(
            jax.ShapeDtypeStruct(background.shape, f32),
            jax.ShapeDtypeStruct((tiles, main, LANES), f32),
        ),
        in_specs=[hbm] * 8,
        out_specs=(vm, vm),
        scratch_shapes=[
            pltpu.VMEM((tiles, main, LANES), bf16),
            pltpu.VMEM((tiles, main, LANES), f32),
            pltpu.VMEM((1, fine_rows), jnp.int32),
            pltpu.VMEM((1, fine_rows), f32),
            pltpu.VMEM(background.shape, f32),
            pltpu.VMEM((1, nobs), jnp.int32),
            pltpu.VMEM(obs_value.shape, f32),
            pltpu.VMEM((1, nobs), f32),
            pltpu.VMEM((tiles, main, LANES), f32),
            pltpu.VMEM((tiles, main, LANES), f32),
            pltpu.VMEM((kaps, lon), f32),
            pltpu.VMEM((LANES, lon), f32),
            pltpu.VMEM((2, RG, lon), f32),
            pltpu.VMEM((2, RG, lon), f32),
            pltpu.VMEM((3, lon + SUB, LANES), f32),
            pltpu.VMEM((n // 2, 2, fr, LANES), f32),
            pltpu.VMEM((n // 2, fr, LANES), f32),
            pltpu.VMEM((n // 2, fr, LANES), f32),
            pltpu.VMEM((n // 2, fr, LANES), f32),
            pltpu.VMEM((n, SUB, LANES), f32),
            pltpu.VMEM((n, SUB, LANES), f32),
            pltpu.VMEM((xs, n, SUB, LANES), f32),
            pltpu.VMEM((xs, n, SUB, LANES), f32),
            pltpu.VMEM((kaps, wide), bf16),
            pltpu.VMEM((kaps, wide), bf16),
            pltpu.VMEM((wide, kaps), bf16),
            pltpu.VMEM((wide, kaps), bf16),
            pltpu.VMEM((gl, 2 * gcells), bf16),
            pltpu.VMEM((gl, 2 * nobs), bf16),
            pltpu.VMEM((LANES, 2 * nobs), bf16),
            pltpu.VMEM((4 * SUB, wide), f32),
            pltpu.VMEM((4 * SUB, wide), f32),
            pltpu.VMEM((4 * SUB, wide), f32),
            pltpu.VMEM((2, SUB, LANES), f32),
            pltpu.VMEM((2, SUB, LANES), f32),
            pltpu.VMEM((4 * SUB, wide), f32),
            pltpu.VMEM((2, fr, LANES), f32),
            pltpu.VMEM((n, 2, fr, LANES), f32),
            pltpu.VMEM((xs, SUB, LANES), f32),
            pltpu.VMEM((xs, 2, n // 2, SUB, LANES), f32),
            pltpu.VMEM((tiles, main, LANES), f32),
            pltpu.VMEM((main, lon), f32),
            dma((8,)),
            dma((xs,)),
            dma,
            dma,
            dma,
            dma((xs,)),
            dma,
            dma,
            dma((len(chip_order(n // 2)[1]),)),
            dma,
            dma((2 * xs,)),
            dma((xs,)),
            dma((xs,)),
        ],
        compiler_params=pltpu.CompilerParams(collective_id=0, has_side_effects=True, vmem_limit_bytes=48 * 2**20),
    )(
        *(
            pltpu.with_memory_space_constraint(v, pltpu.HBM)
            for v in (
                to_tiles(ensemble),
                to_tiles(alpha),
                lat_lower.reshape(1, fine_rows),
                lat_weight.reshape(1, fine_rows),
                background,
                obs_cell,
                obs_value,
                obs_precision,
            )
        )
    )
    advected, gradient = pl.pallas_call(
        writer,
        out_shape=(
            jax.ShapeDtypeStruct(background.shape, f32),
            jax.ShapeDtypeStruct((tiles, main, LANES), f32),
        ),
        in_specs=[vm, vm],
        out_specs=(hbm, hbm),
        scratch_shapes=[dma((2,))],
        compiler_params=pltpu.CompilerParams(vmem_limit_bytes=2**20),
    )(advected, gradient)
    return advected, gradient.swapaxes(0, 1).reshape(members, lev, rows, lon)


def solution(mesh):
    return jax.shard_map(
        shards,
        mesh=mesh,
        in_specs=(
            P("mem", None, "band", None),
            P("mem", None, "band", None),
            P("band"),
            P("band"),
            P(None, ("band", "mem"), None),
            P(("band", "mem"), None),
            P(None, ("band", "mem"), None),
            P(("band", "mem"), None),
        ),
        out_specs=(P(None, ("band", "mem"), None), P("mem", None, "band", None)),
        check_vma=False,
    )
```

```python
import functools
import math

import jax
import jax.numpy as jnp
from jax import lax
from jax.experimental import pallas as pl
from jax.experimental.pallas import tpu as pltpu
from jax.sharding import PartitionSpec as P

advect_rate = 0.25
LANES = 128
SUB = 8
RG = 16
f32 = jnp.float32
bf16 = jnp.bfloat16


def split2(x):
    hi = x.astype(bf16)
    lo = (x - hi.astype(f32)).astype(bf16)
    return hi, lo


def split2f(x):
    hi = x.astype(bf16).astype(f32)
    return hi, x - hi


def split3f(x):
    hi, rest = split2f(x)
    mid, lo = split2f(rest)
    return hi, mid, lo


def dims(a, b, ca, cb):
    return lax.dot_general(a, b, (((ca,), (cb,)), ((), ())), preferred_element_type=f32)


def iota(shape, d):
    return lax.broadcasted_iota(jnp.int32, shape, d)


def smooth_lon(x):
    n = x.shape[1]
    return 0.25 * pltpu.roll(x, 1, 1) + 0.5 * x + 0.25 * pltpu.roll(x, n - 1, 1)


def lon_weights(ratio):
    def parts(shift):
        num = 2 * shift + 1 + ratio
        return num // (2 * ratio), (num % (2 * ratio)) / (2 * ratio)

    def taps(shift):
        q, f = parts(shift)
        w = [0.0, 0.0, 0.0]
        for at, v in ((q, 1.0 - f), (q + 1, f)):
            if v:
                w[at] += v
        return w

    value = [taps(b) for b in range(ratio)]
    slope = [[0.5 * (p - m) for p, m in zip(taps(b + 1), taps(b - 1))] for b in range(ratio)]
    return value, slope


def combine(weights, parts):
    out = None
    for w, p in zip(weights, parts):
        if w == 0.0:
            continue
        term = p if w == 1.0 else w * p
        out = term if out is None else out + term
    return out


def chip_order(chips):
    ring = 4 if chips % 4 == 0 else chips
    rest = chips // ring

    def hops(step):
        return min(step[0], ring - step[0]) + min(step[1], rest - step[1])

    steps = sorted(((a, b) for a in range(ring) for b in range(rest)), key=lambda s: -hops(s))
    classes = [[s for s in steps if hops(s) == h] for h in sorted({hops(s) for s in steps if hops(s)}, reverse=True)]
    return steps, classes, ring, rest


def kernel(
    cfg,
    ens_hbm,
    alpha_hbm,
    low_hbm,
    wt_hbm,
    bg_hbm,
    cell_hbm,
    val_hbm,
    prec_hbm,
    adv_ref,
    grad_ref,
    ens_in,
    alpha,
    low,
    wt,
    bg,
    cell,
    val,
    prec,
    ensf,
    plain,
    part,
    xpart,
    edge_send,
    edge_recv,
    flat,
    frames,
    pre_recv,
    psum,
    recv1,
    eloc,
    rece,
    ecr,
    recc,
    table_hi,
    table_lo,
    back_hi,
    back_lo,
    zbuf,
    rbuf,
    abuf,
    fine_bg,
    obs_a,
    obs_b,
    fe_send,
    fe_recv,
    advbuf,
    send2,
    recv2,
    sendx,
    recvx,
    ebuf,
    ensr,
    in_sem,
    edge_rs,
    pre_rs,
    rs1,
    rse,
    rsc,
    fe_rs,
    ss2,
    rs2,
    rs2f,
    ssx,
    rsx,
    rsxf,
):
    n, nb, lev, rows, lon, fine_rows, fine_cols, scale = cfg
    block = lon // n
    frame = block + 2
    ratio = fine_cols // block
    main = lev * rows
    tiles = lon // LANES
    ng = fine_rows // RG
    gcells = RG * fine_cols
    gl = RG * RG
    levp = RG
    xs = recvx.shape[0]
    me = lax.axis_index("mem")
    band = lax.axis_index("band")
    has_up = band > 0
    has_down = band < nb - 1
    has = (has_up, has_down)
    wv, ws = lon_weights(ratio)

    barrier = pltpu.get_barrier_semaphore()

    core = lax.rem(me, 2)
    chip = me // 2
    partner = me + 1 - 2 * core
    chips = n // 2
    far_first, classes, ring, rest = chip_order(chips)
    ring_at, rest_at = chip // rest, lax.rem(chip, rest)

    def to_chip(step):
        return lax.rem(ring_at + step[0], ring) * rest + lax.rem(rest_at + step[1], rest)

    def from_chip(step):
        return to_chip(((ring - step[0]) % ring, (rest - step[1]) % rest))

    side_band = (band - 1, band + 1)
    for step in far_first:
        home = step == (0, 0)
        for c in (core, 1 - core):
            if nb == 2:
                pl.semaphore_signal(barrier, inc=1, device_id={"mem": 2 * to_chip(step) + c, "band": 1 - band})
            else:
                for side in (0, 1):

                    @pl.when(has[side])
                    def _():
                        pl.semaphore_signal(
                            barrier, inc=1, device_id={"mem": 2 * to_chip(step) + c, "band": side_band[side]}
                        )

            if not (home and c is core):
                pl.semaphore_signal(barrier, inc=1, device_id={"mem": 2 * to_chip(step) + c})

    loads = [
        pltpu.make_async_copy(src, dst, in_sem.at[i])
        for i, (src, dst) in enumerate(
            (
                (alpha_hbm, alpha),
                (ens_hbm, ens_in),
                (bg_hbm, bg),
                (low_hbm, low),
                (wt_hbm, wt),
                (cell_hbm, cell),
                (val_hbm, val),
                (prec_hbm, prec),
            )
        )
    ]
    for c in loads:
        c.start()

    part[main:, :] = jnp.zeros((part.shape[0] - main, lon), f32)
    xpart[...] = jnp.zeros(xpart.shape, f32)
    edge_send[...] = jnp.zeros(edge_send.shape, f32)
    fe_send[...] = jnp.zeros(fe_send.shape, f32)

    loads[0].wait()
    loads[1].wait()

    def whole(ref):
        parts = [ref[t] for t in range(tiles)]
        return parts[0] if tiles == 1 else jnp.concatenate(parts, axis=1)

    def row(ref, k):
        parts = [ref.at[t][pl.ds(k, lev, stride=rows), :] for t in range(tiles)]
        return parts[0] if tiles == 1 else jnp.concatenate(parts, axis=1)

    for t in range(tiles):
        ensf[t] = ens_in[t].astype(f32)
    al = whole(alpha)
    en = whole(ensf)
    kk = iota((main, lon), 0) % rows
    a_up = jnp.where(kk == 0, 0.0, pltpu.roll(al, 1, 0))
    a_dn = jnp.where(kk == rows - 1, 0.0, pltpu.roll(al, main - 1, 0))
    z = smooth_lon(0.25 * (a_up + a_dn) + 0.5 * al) * en * scale
    for t in range(tiles):
        plain[t] = z[:, t * LANES : (t + 1) * LANES]
    part[0:main, :] = z
    edges = []
    for side, k in ((0, 0), (1, rows - 1)):
        a_edge = smooth_lon(row(alpha, k)) * (0.25 * scale)
        e_edge = row(ensf, k)
        edges.append((a_edge, e_edge, row(plain, k)))
        edge_send[side, 0:lev, :] = e_edge
        at = main + side * 2 * levp
        for i, v in enumerate((a_edge, e_edge) if side == 0 else (e_edge, a_edge)):
            part[at + i * levp : at + i * levp + lev, :] = v
    (a_0, e_0, p_0), (a_1, e_1, p_1) = edges
    zero = jnp.zeros_like(a_0)
    sets_up = [zero, p_0, a_0, e_0]
    sets_down = [e_1, a_1, p_1, zero]
    if xs == 1:
        sets = [jnp.where(has_up, u, d) for u, d in zip(sets_up, sets_down)]
    else:
        sets = sets_up + sets_down
    for i, v in enumerate(sets):
        xpart[i * levp : i * levp + lev, :] = v

    def lay(g, rows_of):
        rows_of = pltpu.roll(rows_of, 1, 1)
        for t in range(tiles):
            flat[g, t * LANES : (t + 1) * LANES, :] = rows_of[:, t * LANES : (t + 1) * LANES].T
        flat[g, lon : lon + SUB, :] = flat[g, 0:SUB, :]

    lay(0, part[0:LANES, :])
    lay(1, part[LANES : 2 * LANES, :])
    lay(2, xpart[...])

    lane8 = iota((SUB, LANES), 1)
    row8 = iota((SUB, LANES), 0)
    low_half = lane8 < LANES // 2
    half = LANES // 2

    def tile_of(g, d):
        return flat[g, d * SUB : (d + 1) * SUB, :]

    def views(d):
        v, x = tile_of(1, d), tile_of(2, d)
        flip, flipx = pltpu.roll(v, half, 1), pltpu.roll(x, half, 1)
        return v, flip, x, flipx, pltpu.roll(flip, 5, 0), pltpu.roll(v, 3, 0), pltpu.roll(flipx, 3, 0), pltpu.roll(x, 3, 0)

    cur = views(0)
    for d in range(n):
        nxt = views(d + 1)
        v, flip, x, flipx, r5, v3, fx3, x3 = cur
        packed = jnp.where(low_half, pltpu.roll(v, 2, 0), jnp.where(row8 < 5, r5, nxt[4]))
        frames[d // 2, d % 2, 0:SUB, :] = tile_of(0, d)
        frames[d // 2, d % 2, SUB : 2 * SUB, :] = jnp.where(row8 < 2, tile_of(0, d + 1), packed)
        eloc[d] = jnp.where(low_half, flip, jnp.where(row8 < 3, v3, nxt[5]))
        ecr[0, d] = jnp.where(low_half, x, jnp.where(row8 < 3, fx3, nxt[6]))
        if xs == 2:
            ecr[1, d] = jnp.where(low_half, flipx, jnp.where(row8 < 3, x3, nxt[7]))
        cur = nxt

    loads[2].wait()
    row32 = iota((4 * SUB, gcells), 0)
    col_of = jnp.where(row32 < ratio * SUB, (row32 % SUB) * ratio + row32 // SUB, -1)
    pick = (iota((4 * SUB, gcells), 1) % fine_cols == col_of).astype(f32).astype(bf16)
    pick3 = jnp.concatenate([pick] * 3, axis=1)
    in_row = iota((RG, gcells), 1) // fine_cols == iota((RG, gcells), 0)
    zbuf[main:, :] = jnp.zeros((gl - main, 3 * gcells), bf16)
    back = bg[:, 0, :]
    for g in range(ng):
        terms = split3f(back[:, g * gcells : (g + 1) * gcells])
        for l in range(lev):
            at = slice(l * RG, (l + 1) * RG)
            for i, v in enumerate(terms):
                spread = jnp.where(in_row, jnp.broadcast_to(v[l : l + 1], (RG, gcells)), 0.0)
                zbuf[at, i * gcells : (i + 1) * gcells] = spread.astype(bf16)
        fine_bg[:, g * gl : (g + 1) * gl] = dims(pick3, zbuf[...], 1, 1)
    for c in loads[3:]:
        c.wait()

    if nb == 2:
        pl.semaphore_wait(barrier, 2 * n - 1)
    else:
        pl.semaphore_wait(barrier, n - 1 + n * (has_up.astype(jnp.int32) + has_down.astype(jnp.int32)))

    pre_copy = pltpu.make_async_remote_copy(
        src_ref=frames.at[:, core],
        dst_ref=pre_recv,
        send_sem=in_sem.at[0],
        recv_sem=pre_rs,
        device_id={"mem": partner},
    )
    pre_copy.start()
    packed_rows = frame // 2

    def copyc(side, dst):
        i = 0 if xs == 1 else 1 - side
        return pltpu.make_async_remote_copy(
            src_ref=ecr.at[0 if xs == 1 else side, dst, pl.ds(0, packed_rows), :],
            dst_ref=recc.at[i, me, pl.ds(0, packed_rows), :],
            send_sem=in_sem.at[2 + side],
            recv_sem=rsc.at[i],
            device_id={"mem": dst, "band": side_band[side]},
        )

    def copye(dst):
        return pltpu.make_async_remote_copy(
            src_ref=eloc.at[dst, pl.ds(0, packed_rows), :],
            dst_ref=rece.at[me, pl.ds(0, packed_rows), :],
            send_sem=in_sem.at[1],
            recv_sem=rse,
            device_id={"mem": dst},
        )

    def edge_copy(side):
        return pltpu.make_async_remote_copy(
            src_ref=edge_send.at[side],
            dst_ref=edge_recv.at[1 - side],
            send_sem=in_sem.at[6 + side],
            recv_sem=edge_rs.at[0 if xs == 1 else 1 - side],
            device_id={"band": side_band[side]},
        )

    for side in (0, 1):

        @pl.when(has[side])
        def _():
            for step in far_first:
                for c in (core, 1 - core):
                    copyc(side, 2 * to_chip(step) + c).start()

        @pl.when(jnp.logical_not(has[side]))
        def _():
            edge_recv[side] = jnp.zeros(edge_recv.shape[1:], f32)

    for step in far_first:
        for c in (core, 1 - core):
            if step != (0, 0) or c is not core:
                copye(2 * to_chip(step) + c).start()
    for side in (0, 1):

        @pl.when(has[side])
        def _():
            edge_copy(side).start()

    rece[me] = eloc[me]

    first = fine_bg[0:1, :]
    last = fine_bg[ratio * SUB - 1 : ratio * SUB, :]
    for t in range(ng * gl // LANES):
        fe_send[0, t : t + 1, :] = first[:, t * LANES : (t + 1) * LANES]
        fe_send[1, t : t + 1, :] = last[:, t * LANES : (t + 1) * LANES]

    def fe_copy(side):
        return pltpu.make_async_remote_copy(
            src_ref=fe_send.at[side],
            dst_ref=fe_recv.at[1 - side],
            send_sem=in_sem.at[5],
            recv_sem=fe_rs,
            device_id={"mem": lax.rem(me + (n - 1 if side == 0 else 1), n)},
        )

    fe_copy(0).start()
    fe_copy(1).start()

    lane = iota((SUB, LANES), 1)
    wide = ng * gl

    def per_row(v):
        v = jnp.concatenate([v, jnp.zeros((1, LANES - fine_rows), f32)], axis=1)
        return jnp.broadcast_to(v, (SUB, LANES))

    def tiled(v, g):
        r = v if g == 0 else pltpu.roll(v, LANES - g * RG, 1)
        r = jnp.where(lane < RG, r, 0.0)
        for s in (RG, 2 * RG, 4 * RG):
            r = r + pltpu.roll(r, s, 1)
        return jnp.concatenate([r, r], axis=0)

    low_rows, wt_rows = per_row(low[...].astype(f32)), per_row(wt[...])
    down = lambda v: jnp.concatenate([v] * (LANES // SUB), axis=0).T
    low_col, wt_col = down(low_rows), down(wt_rows)
    lane16 = iota((RG, LANES), 1)
    row16 = iota((RG, LANES), 0)
    lev_of = lane16 // RG
    set_rows = (-1, 0, rows - 1, rows)
    table_hi[...] = jnp.zeros(table_hi.shape, bf16)
    table_lo[...] = jnp.zeros(table_lo.shape, bf16)
    back_hi[...] = jnp.zeros(back_hi.shape, bf16)
    back_lo[...] = jnp.zeros(back_lo.shape, bf16)
    halves = gl // LANES
    per = LANES // RG

    def weigh(k, lo_k, w):
        w_hi, w_lo = split2f(w)
        o_hi, o_lo = split2f(1.0 - w)
        m0, m1 = k == lo_k, k == lo_k + 1.0
        return (
            jnp.where(m0, o_hi, jnp.where(m1, w_hi, 0.0)),
            jnp.where(m0, o_lo, jnp.where(m1, w_lo, 0.0)),
        )

    def put(ref, r, c, v, keep):
        ref[r : r + RG, c : c + LANES] = jnp.where(keep, v, 0.0).astype(bf16)

    for g in range(ng):
        lo_t, w_t = tiled(low_rows, g), tiled(wt_rows, g)
        main_t = weigh(row16.astype(f32), lo_t, w_t)
        set_t = [weigh(jnp.full((RG, LANES), float(k), f32), lo_t, w_t) for k in set_rows]
        for ref, which in ((table_hi, 0), (table_lo, 1)):
            for l in range(lev):
                put(ref, l * RG, g * gl + l // per * LANES, main_t[which], lev_of == l % per)
            for s in range(4):
                for h in range(halves):
                    put(ref, main + s * levp, g * gl + h * LANES, set_t[s][which], (row16 == lev_of + h * per) & (row16 < lev))
        lo_c, w_c = low_col[g * RG : (g + 1) * RG], wt_col[g * RG : (g + 1) * RG]
        for h in range(halves):
            kap = lane16 + h * LANES
            e = kap - main
            es = e // levp
            ek = jnp.where(es == 0, -1, jnp.where(es == 1, 0, jnp.where(es == 2, rows - 1, rows)))
            k_of = jnp.where(e < 0, kap % rows, ek).astype(f32)
            l_of = jnp.where(e < 0, kap // rows, e % levp)
            back_t = weigh(k_of, lo_c, w_c)
            for ref, which in ((back_hi, 0), (back_lo, 1)):
                for l in range(lev):
                    if (h + 1) * LANES > main or l // per == h:
                        put(ref, g * gl + l * RG, h * LANES, back_t[which], l_of == l)

    pre_copy.wait_recv()
    for j in range(n // 2):
        psum[j] = frames[j, 1 - core] + pre_recv[j]

    used = frame + packed_rows

    def copy1(dst):
        return pltpu.make_async_remote_copy(
            src_ref=psum.at[dst, pl.ds(0, used), :],
            dst_ref=recv1.at[chip, pl.ds(0, used), :],
            send_sem=in_sem.at[4],
            recv_sem=rs1,
            device_id={"mem": 2 * dst + 1 - core},
        )

    for step in far_first:
        copy1(to_chip(step)).start()

    nobs = cell.shape[1]
    crow = cell[...] // fine_cols
    ccol = cell[...] % fine_cols
    r32 = iota((4 * SUB, nobs), 0)
    col_o = jnp.where(r32 < ratio * SUB, (r32 % SUB) * ratio + r32 // SUB, -1)
    hot = (col_o == ccol).astype(f32).astype(bf16)
    hot3 = jnp.concatenate([hot] * 3, axis=1)
    pr = prec[...]
    p_terms = split3f(pr)
    v_terms = split3f(val[:, 0, :] * pr)
    rbuf[main:, :] = jnp.zeros((gl - main, 3 * nobs), bf16)
    for g in range(ng):
        at_row = iota((RG, nobs), 0) + g * RG == crow
        for i in range(3):
            cut = slice(i * nobs, (i + 1) * nobs)
            for l in range(lev):
                v = jnp.broadcast_to(v_terms[i][l : l + 1], (RG, nobs))
                rbuf[l * RG : (l + 1) * RG, cut] = jnp.where(at_row, v, 0.0).astype(bf16)
            p = jnp.where(at_row, jnp.broadcast_to(p_terms[i], (RG, nobs)), 0.0).astype(bf16)
            for j in range(LANES // RG):
                abuf[j * RG : (j + 1) * RG, cut] = p
        obs_b[:, g * gl : (g + 1) * gl] = dims(hot3, rbuf[...], 1, 1)
        oa = dims(hot3, abuf[...], 1, 1)
        for j in range(gl // LANES):
            obs_a[:, g * gl + j * LANES : g * gl + (j + 1) * LANES] = oa

    pltpu.make_async_copy(fe_recv, fe_recv, fe_rs).wait()
    nt = wide // LANES
    left = jnp.concatenate([fe_recv[0, t : t + 1, :] for t in range(nt)], axis=1)
    right = jnp.concatenate([fe_recv[1, t : t + 1, :] for t in range(nt)], axis=1)
    fb = [fine_bg[b * SUB : (b + 1) * SUB, :] for b in range(ratio)]
    arow = iota((SUB, wide), 0)
    before0 = jnp.where(arow == 0, left, pltpu.roll(fb[ratio - 1], 1, 0))
    after_last = jnp.where(arow == SUB - 1, right, pltpu.roll(fb[0], SUB - 1, 0))
    chain = [before0] + fb + [after_last]
    slope_bg = [0.5 * (chain[b + 2] - chain[b]) for b in range(ratio)]

    def all_of(ref, count, height, sem):
        got = ref.at[pl.ds(0, count), pl.ds(0, height), :]
        pltpu.make_async_copy(got, got, sem).wait()

    all_of(rece, n - 1, packed_rows, rse)
    for side in (0, 1):

        @pl.when(has[side])
        def _():
            i = 0 if xs == 1 else side
            all_of(recc.at[i], n, packed_rows, rsc.at[i])

    prods, plains = [], []
    for i in range(xs):
        prod = rece[0] * recc[i, 0]
        only = recc[i, 0]
        for s in range(1, n):
            prod = prod + rece[s] * recc[i, s]
            only = only + recc[i, s]
        prods.append(prod)
        plains.append(only)
    set_of = (lane8 % half) // levp
    edge_sum = jnp.where(
        set_of < 2, jnp.where(has_up, prods[0], 0.0), jnp.where(has_down, prods[-1], 0.0)
    )
    from_up = jnp.where(has_up, pltpu.roll(plains[0], LANES - 2 * levp, 1), 0.0)
    from_down = jnp.where(has_down, pltpu.roll(plains[-1], 2 * levp, 1), 0.0)
    edge_sum = edge_sum + jnp.where(set_of == 0, from_up, jnp.where(set_of == 3, from_down, 0.0))
    edge_a = pltpu.roll(edge_sum, half, 1)
    edge_b = pltpu.roll(edge_sum, 5, 0)

    all_of(recv1, n // 2, used, rs1)
    total = recv1[0]
    for s in range(1, n // 2):
        total = total + recv1[s]
    m = total[SUB:]
    m_a = pltpu.roll(m, SUB - 2, 0)
    m_b = pltpu.roll(pltpu.roll(m, half, 1), 3, 0)
    x_a = jnp.where(low_half, m_a, edge_a)
    x_b = jnp.where(low_half, m_b, edge_b)
    x = jnp.concatenate([total, jnp.concatenate([jnp.where(row8 < 5, x_a, x_b), x_b], axis=0)], axis=1)
    x_hi, x_lo = split2f(x)
    x2 = jnp.concatenate([x_hi, x_lo], axis=0).astype(bf16)
    y = dims(x2, table_hi[...], 1, 0)
    y = y[0:16] + y[16:32] + dims(x_hi.astype(bf16), table_lo[...], 1, 0)
    taps = [y[0:SUB]] + [pltpu.roll(y, 2 * SUB - d, 0)[0:SUB] for d in (1, 2)]

    us, vs, moved = [], [], []
    for b in range(ratio):
        state = fb[b] + combine(wv[b], taps)
        slope = slope_bg[b] + combine(ws[b], taps)
        factor = 1.0 - advect_rate * slope
        mv = state * factor
        at = slice(b * SUB, (b + 1) * SUB)
        cot = obs_a[at, :] * mv - obs_b[at, :]
        us.append(cot * factor)
        vs.append((-advect_rate) * (state * cot))
        moved.append(mv)
    gl_v = None
    for d in range(3):
        t = combine([wv[b][d] for b in range(ratio)] + [ws[b][d] for b in range(ratio)], us + vs)
        t = jnp.concatenate([t, jnp.zeros_like(t)], axis=0)
        gl_v = t if d == 0 else gl_v + pltpu.roll(t, d, 0)
    g_hi, g_lo = split2f(gl_v)
    g2 = jnp.concatenate([g_hi, g_lo], axis=0).astype(bf16)
    gr = dims(g2, back_hi[...], 1, 0)
    gr = gr[0:16] + gr[16:32] + dims(g_hi.astype(bf16), back_lo[...], 1, 0)
    for g in (0, 1):
        send2[g] = gr[:, g * LANES : (g + 1) * LANES]
    def slot2(src):
        return recv2.at[src, :, pl.ds(0, frame), :]

    def copy2(dst, sem):
        return pltpu.make_async_remote_copy(
            src_ref=send2.at[:, pl.ds(0, frame), :],
            dst_ref=slot2(me),
            send_sem=ss2,
            recv_sem=sem,
            device_id={"mem": dst},
        )

    def forward2(src):
        return pltpu.make_async_remote_copy(
            src_ref=slot2(src),
            dst_ref=slot2(src),
            send_sem=ss2,
            recv_sem=rs2f,
            device_id={"mem": partner},
        )

    def copyx(side, dst):
        i = 0 if xs == 1 else 1 - side
        return pltpu.make_async_remote_copy(
            src_ref=sendx.at[0 if xs == 1 else side, pl.ds(0, packed_rows), :],
            dst_ref=recvx.at[i, core, chip, pl.ds(0, packed_rows), :],
            send_sem=ssx.at[0 if xs == 1 else side],
            recv_sem=rsx.at[i],
            device_id={"mem": dst, "band": side_band[side]},
        )

    def forwardx(i):
        got = recvx.at[i, 1 - core, :, pl.ds(0, packed_rows), :]
        return pltpu.make_async_remote_copy(
            src_ref=got,
            dst_ref=got,
            send_sem=ssx.at[xs + i],
            recv_sem=rsxf.at[i],
            device_id={"mem": partner},
        )

    def send_class(i):
        for step in classes[i]:
            copy2(2 * to_chip(step) + 1 - core, rs2.at[len(classes) - 1 - i]).start()

    v0, v1 = gr[0:SUB, LANES:], gr[SUB:, LANES:]
    quarter = lane8 // (2 * levp)
    v32, v96, w32, w96 = (pltpu.roll(v, r, 1) for v in (v0, v1) for r in (2 * levp, 6 * levp))

    def late(a, b):
        return jnp.where(row8 < 3, pltpu.roll(a, 3, 0), pltpu.roll(b, 3, 0))

    def pack_for(up_there):
        near = jnp.where(up_there, v32, v96)
        rest_cols = late(jnp.where(up_there, v96, v32), jnp.where(up_there, w96, w32))
        q = jnp.where(up_there, quarter - 1, quarter)
        return jnp.where(q == 2, near, jnp.where(q == 0, rest_cols, 0.0))

    if xs == 1:
        sendx[0] = pack_for(has_up)
    else:
        for side in (0, 1):
            sendx[side] = pack_for(side == 0)

    for side in (0, 1):

        @pl.when(has[side])
        def _():
            for step in far_first:
                copyx(side, 2 * to_chip(step) + 1 - core).start()

    for i in range(len(classes)):
        send_class(i)
    copy2(partner, rs2f).start()
    for g in (0, 1):
        recv2[me, g] = send2[g]

    advbuf[...] = jnp.concatenate(moved + [jnp.zeros((SUB, wide), f32)], axis=0)
    pickt = jnp.concatenate([pick, pick], axis=0)
    for g in range(ng):
        hi, lo = split2(advbuf[:, g * gl : g * gl + main])
        e = dims(jnp.concatenate([hi, lo], axis=0), pickt, 0, 0)
        for l in range(lev):
            v = jnp.where(in_row, e[l * RG : (l + 1) * RG], 0.0)
            adv_ref[l, :, g * gcells : (g + 1) * gcells] = jnp.sum(v, axis=0, keepdims=True)

    def sent_edges():
        pre_copy.wait_send()
        all_of(rece, n - 1, packed_rows, in_sem.at[1])
        all_of(recv1, n // 2, used, in_sem.at[4])
        pltpu.make_async_copy(fe_recv, fe_recv, in_sem.at[5]).wait()
        for side in (0, 1):

            @pl.when(has[side])
            def _():
                all_of(recc.at[0], n, packed_rows, in_sem.at[2 + side])
                edge_copy(side).wait_send()
                pltpu.make_async_copy(edge_recv.at[side], edge_recv.at[side], edge_rs.at[0 if xs == 1 else side]).wait()

    sent_edges()
    def all_2(count, sem):
        got = recv2.at[pl.ds(0, count), :, pl.ds(0, frame), :]
        pltpu.make_async_copy(got, got, sem).wait()

    ensr[...] = pltpu.roll(whole(ensf), 1, 1) * scale
    ebuf[...] = jnp.zeros(ebuf.shape, f32)
    edge_ens = [pltpu.roll(row(ensf, k), 1, 1) * scale for k in (0, rows - 1)]
    halo_ens = [pltpu.roll(edge_recv[side, 0:lev, :], 1, 1) * scale for side in (0, 1)]

    def smooth_back(v):
        return 0.25 * v + 0.5 * pltpu.roll(v, lon - 1, 1) + 0.25 * pltpu.roll(v, lon - 2, 1)

    for i, group in enumerate(reversed(classes)):
        all_2(len(group), rs2.at[i])
        for step in group:
            forward2(2 * from_chip(step) + 1 - core).start()
    for side in (0, 1):

        @pl.when(has[side])
        def _():
            i = 0 if xs == 1 else side
            got = recvx.at[i, 1 - core, :, pl.ds(0, packed_rows), :]
            pltpu.make_async_copy(got, got, rsx.at[i]).wait()
            forwardx(i).start()

    all_2(n // 2, rs2f)

    over = iota((SUB, LANES), 0) < frame - block

    def across(parts):
        per_tile = LANES // SUB
        cols = [jnp.concatenate(parts[t * per_tile : (t + 1) * per_tile], axis=0).T for t in range(tiles)]
        return cols[0] if tiles == 1 else jnp.concatenate(cols, axis=1)

    ours = (quarter < 2) | (set_of == 0) | (set_of == 3)
    set_lanes = lane8 >= half

    def edges_at(i, d):
        e = recvx[i, d % 2, d // 2]
        b = pltpu.roll(pltpu.roll(e, half, 1), 5, 0)
        return jnp.where(row8 < 5, e, b), jnp.where(over, b, 0.0)

    def gather(g):
        sides = range(xs) if g else ()
        prev = [edges_at(i, n - 1)[1] for i in sides]
        parts = []
        for d in range(n):
            tile = recv2[d, g, 0:SUB, :] + jnp.where(over, recv2[(d - 1) % n, g, SUB : 2 * SUB, :], 0.0)
            if g:
                theirs = None
                for i in sides:
                    here, tail = edges_at(i, d)
                    v = here + prev[i]
                    if xs == 2:
                        v = jnp.where(has[i], v, 0.0)
                    theirs = v if theirs is None else theirs + v
                    prev[i] = tail
                tile = jnp.where(ours, tile, 0.0) + jnp.where(set_lanes, theirs, 0.0)
            parts.append(tile)
        return across(parts)

    c0 = gather(0)
    for side in (0, 1):

        @pl.when(has[side])
        def _():
            i = 0 if xs == 1 else side
            all_of(recvx.at[i, 0], n // 2, packed_rows, rsxf.at[i])

    c1 = gather(1)
    e0 = main - LANES
    wm = ensr[...] * jnp.concatenate([c0, c1[0:e0]], axis=0)
    w_up = jnp.where(kk == 0, 0.0, pltpu.roll(wm, 1, 0))
    w_dn = jnp.where(kk == rows - 1, 0.0, pltpu.roll(wm, main - 1, 0))
    zz = smooth_back(0.25 * (w_up + w_dn) + 0.5 * wm)
    for t in range(tiles):
        grad_ref[t] = zz[:, t * LANES : (t + 1) * LANES]
    for side, k, k_in in ((0, 0, 1), (1, rows - 1, rows - 2)):
        halo_at, extra_at = (e0, e0 + levp) if side == 0 else (e0 + 3 * levp, e0 + 2 * levp)
        we = edge_ens[side] * c1[extra_at : extra_at + lev]
        wh = halo_ens[side] * c1[halo_at : halo_at + lev]
        z_edge = smooth_back(0.5 * we + 0.25 * wh)
        z_in = smooth_back(0.25 * we)
        for t in range(tiles):
            cut = slice(t * LANES, (t + 1) * LANES)
            grad_ref.at[t][pl.ds(k, lev, stride=rows), :] += z_edge[:, cut]
            grad_ref.at[t][pl.ds(k_in, lev, stride=rows), :] += z_in[:, cut]

    for side in (0, 1):

        @pl.when(has[side])
        def _():
            i = 0 if xs == 1 else side
            all_of(recvx.at[0, 0], n // 2, packed_rows, ssx.at[i])
            all_of(recvx.at[0, 0], n // 2, packed_rows, ssx.at[xs + i])

    all_2(n - 1, ss2)


def writer(adv_ref, grad_ref, adv_out, grad_out, sem):
    copies = [
        pltpu.make_async_copy(grad_ref, grad_out, sem.at[0]),
        pltpu.make_async_copy(adv_ref, adv_out, sem.at[1]),
    ]
    for c in copies:
        c.start()
    for c in copies:
        c.wait()


def up_to(x, m):
    return -(-x // m) * m


def to_tiles(x):
    return x.reshape(-1, x.shape[3] // LANES, LANES).swapaxes(0, 1)


def shards(ensemble, alpha, lat_lower, lat_weight, background, obs_cell, obs_value, obs_precision):
    n, nb = lax.axis_size("mem"), lax.axis_size("band")
    members, lev, rows, lon = ensemble.shape
    fine_rows = lat_lower.shape[0]
    cells = background.shape[2]
    nobs = obs_cell.shape[1]
    fine_cols = cells // fine_rows
    scale = 1.0 / math.sqrt(members * n - 1)
    block = lon // n
    main = lev * rows
    kaps = main + 4 * RG
    assert n % 2 == 0 and members == 1 and block == SUB and rows == RG and lev <= RG and kaps == 2 * LANES
    assert fine_rows % RG == 0 and fine_cols % block == 0 and fine_cols // block == 3
    cfg = (n, nb, lev, rows, lon, fine_rows, fine_cols, scale)
    tiles = lon // LANES
    ng = fine_rows // RG
    gl = RG * RG
    wide = ng * gl
    gcells = RG * fine_cols
    xs = 1 if nb == 2 else 2
    dma = pltpu.SemaphoreType.DMA
    vm = pl.BlockSpec(memory_space=pltpu.VMEM)
    hbm = pl.BlockSpec(memory_space=pltpu.HBM)
    fr = 2 * SUB
    advected, gradient = pl.pallas_call(
        functools.partial(kernel, cfg),
        out_shape=(
            jax.ShapeDtypeStruct(background.shape, f32),
            jax.ShapeDtypeStruct((tiles, main, LANES), f32),
        ),
        in_specs=[hbm] * 8,
        out_specs=(vm, vm),
        scratch_shapes=[
            pltpu.VMEM((tiles, main, LANES), bf16),
            pltpu.VMEM((tiles, main, LANES), f32),
            pltpu.VMEM((1, fine_rows), jnp.int32),
            pltpu.VMEM((1, fine_rows), f32),
            pltpu.VMEM(background.shape, f32),
            pltpu.VMEM((1, nobs), jnp.int32),
            pltpu.VMEM(obs_value.shape, f32),
            pltpu.VMEM((1, nobs), f32),
            pltpu.VMEM((tiles, main, LANES), f32),
            pltpu.VMEM((tiles, main, LANES), f32),
            pltpu.VMEM((kaps, lon), f32),
            pltpu.VMEM((LANES, lon), f32),
            pltpu.VMEM((2, RG, lon), f32),
            pltpu.VMEM((2, RG, lon), f32),
            pltpu.VMEM((3, lon + SUB, LANES), f32),
            pltpu.VMEM((n // 2, 2, fr, LANES), f32),
            pltpu.VMEM((n // 2, fr, LANES), f32),
            pltpu.VMEM((n // 2, fr, LANES), f32),
            pltpu.VMEM((n // 2, fr, LANES), f32),
            pltpu.VMEM((n, SUB, LANES), f32),
            pltpu.VMEM((n, SUB, LANES), f32),
            pltpu.VMEM((xs, n, SUB, LANES), f32),
            pltpu.VMEM((xs, n, SUB, LANES), f32),
            pltpu.VMEM((kaps, wide), bf16),
            pltpu.VMEM((kaps, wide), bf16),
            pltpu.VMEM((wide, kaps), bf16),
            pltpu.VMEM((wide, kaps), bf16),
            pltpu.VMEM((gl, 3 * gcells), bf16),
            pltpu.VMEM((gl, 3 * nobs), bf16),
            pltpu.VMEM((LANES, 3 * nobs), bf16),
            pltpu.VMEM((4 * SUB, wide), f32),
            pltpu.VMEM((4 * SUB, wide), f32),
            pltpu.VMEM((4 * SUB, wide), f32),
            pltpu.VMEM((2, SUB, LANES), f32),
            pltpu.VMEM((2, SUB, LANES), f32),
            pltpu.VMEM((4 * SUB, wide), f32),
            pltpu.VMEM((2, fr, LANES), f32),
            pltpu.VMEM((n, 2, fr, LANES), f32),
            pltpu.VMEM((xs, SUB, LANES), f32),
            pltpu.VMEM((xs, 2, n // 2, SUB, LANES), f32),
            pltpu.VMEM((tiles, main, LANES), f32),
            pltpu.VMEM((main, lon), f32),
            dma((8,)),
            dma((xs,)),
            dma,
            dma,
            dma,
            dma((xs,)),
            dma,
            dma,
            dma((len(chip_order(n // 2)[1]),)),
            dma,
            dma((2 * xs,)),
            dma((xs,)),
            dma((xs,)),
        ],
        compiler_params=pltpu.CompilerParams(collective_id=0, has_side_effects=True, vmem_limit_bytes=48 * 2**20),
    )(
        *(
            pltpu.with_memory_space_constraint(v, pltpu.HBM)
            for v in (
                to_tiles(ensemble),
                to_tiles(alpha),
                lat_lower.reshape(1, fine_rows),
                lat_weight.reshape(1, fine_rows),
                background,
                obs_cell,
                obs_value,
                obs_precision,
            )
        )
    )
    advected, gradient = pl.pallas_call(
        writer,
        out_shape=(
            jax.ShapeDtypeStruct(background.shape, f32),
            jax.ShapeDtypeStruct((tiles, main, LANES), f32),
        ),
        in_specs=[vm, vm],
        out_specs=(hbm, hbm),
        scratch_shapes=[dma((2,))],
        compiler_params=pltpu.CompilerParams(vmem_limit_bytes=2**20),
    )(advected, gradient)
    return advected, gradient.swapaxes(0, 1).reshape(members, lev, rows, lon)


def solution(mesh):
    return jax.shard_map(
        shards,
        mesh=mesh,
        in_specs=(
            P("mem", None, "band", None),
            P("mem", None, "band", None),
            P("band"),
            P("band"),
            P(None, ("band", "mem"), None),
            P(("band", "mem"), None),
            P(None, ("band", "mem"), None),
            P(("band", "mem"), None),
        ),
        out_specs=(P(None, ("band", "mem"), None), P("mem", None, "band", None)),
        check_vma=False,
    )
```
